16 devices in a mesh: dap: 2 (over z), dp: 8 (over y, x, core).
Axes of the slice: x: 2, y: 2, z: 2, core: 2. Of those that a mesh axis runs over, the one named last changes fastest.
Arguments:
- pair_z: bfloat16 [24, 64, 64, 128], P('dp', 'dap')
- single_s: bfloat16 [24, 64, 384], P('dp', 'dap')
- token_mask: int32 [24, 64], P('dp')
- dz_out: bfloat16 [24, 64, 64, 128], P('dp', 'dap')
- ds_out: bfloat16 [24, 64, 384], P('dp', 'dap')
- w_pa: bfloat16 [128, 512], replicated
- w_pb: bfloat16 [128, 512], replicated
- w_po: bfloat16 [512, 128], replicated
- w_bias: bfloat16 [128, 16], replicated
- w_q: bfloat16 [384, 384], replicated
- q_bias: bfloat16 [384], replicated
- w_kv: bfloat16 [384, 768], replicated
- w_g: bfloat16 [384, 384], replicated
- w_o: bfloat16 [384, 384], replicated
- w_sa: bfloat16 [384, 1536], replicated
- w_sb: bfloat16 [384, 1536], replicated
- w_so: bfloat16 [1536, 384], replicated
Outputs:
- output 1: bfloat16 [24, 64, 64, 128], P('dp', 'dap')
- output 2: bfloat16 [24, 64, 384], P('dp', 'dap')
- output 3: float32 [128, 512], replicated
- output 4: float32 [128, 512], replicated
- output 5: float32 [512, 128], replicated
- output 6: float32 [128, 16], replicated
- output 7: float32 [384, 384], replicated
- output 8: float32 [384], replicated
- output 9: float32 [384, 768], replicated
- output 10: float32 [384, 384], replicated
- output 11: float32 [384, 384], replicated
- output 12: float32 [384, 1536], replicated
- output 13: float32 [384, 1536], replicated
- output 14: float32 [1536, 384], replicated
All inputs are finite; a program needn't handle non-finite values.
Results may differ from the reference program's by a relative error of at most 0.0171153.
Values are sent between devices in bfloat16 or wider.
A program may use at most 1 GiB of HBM per device.

```python
import jax
import jax.numpy as jnp
from jax import lax

C_S = 384
C_Z = 128
HEADS = 16
HEAD = 24
TRANS = 4
TOKENS = 64
COMPLEXES = 24


def snap_bf16(values):
    return values + lax.stop_gradient(values.astype(jnp.bfloat16).astype(jnp.float32) - values)


def layer_norm(values):
    centred = values - jnp.mean(values, axis=-1, keepdims=True)
    return centred * lax.rsqrt(jnp.mean(centred * centred, axis=-1, keepdims=True) + 1e-5)


def pair_rows(z_rows, w_pa, w_pb, w_po):
    normed = snap_bf16(layer_norm(z_rows))
    hid_a = jnp.einsum('rjc,cf->rjf', normed, w_pa)
    hid_b = jnp.einsum('rjc,cf->rjf', normed, w_pb)
    hidden = snap_bf16(jax.nn.silu(hid_a) * hid_b)
    return snap_bf16(z_rows + jnp.einsum('rjf,fc->rjc', hidden, w_po))


def block_forward(pair_z, single_s, mask_row, w_pa, w_pb, w_po, w_bias, w_q, q_bias, w_kv, w_g, w_o, w_sa, w_sb, w_so):
    attn_width = HEADS * HEAD
    checked_rows = jax.checkpoint(pair_rows)

    def row_step(z_rows):
        return checked_rows(z_rows, w_pa, w_pb, w_po)

    z_new = lax.map(row_step, pair_z.reshape(TOKENS // 16, 16, TOKENS, C_Z)).reshape(TOKENS, TOKENS, C_Z)
    pair_bias = jnp.einsum('ijc,ch->hij', snap_bf16(layer_norm(z_new)), w_bias)
    act_norm = snap_bf16(layer_norm(single_s))
    queries = snap_bf16(jnp.dot(act_norm, w_q, preferred_element_type=jnp.float32) + q_bias).reshape(TOKENS, HEADS, HEAD)
    key_val = snap_bf16(jnp.dot(act_norm, w_kv, preferred_element_type=jnp.float32))
    key_heads = key_val[:, :attn_width].reshape(TOKENS, HEADS, HEAD)
    value_heads = key_val[:, attn_width:].reshape(TOKENS, HEADS, HEAD)
    gate_vals = jax.nn.sigmoid(jnp.dot(act_norm, w_g, preferred_element_type=jnp.float32))
    key_mask = 1e9 * (mask_row.astype(jnp.float32) - 1.0)
    logits = jnp.einsum('ihd,jhd->hij', queries, key_heads) * (HEAD ** -0.5) + pair_bias + key_mask[None, None, :]
    attn_prob = snap_bf16(jax.nn.softmax(logits, axis=-1))
    attended = jnp.einsum('hij,jhd->ihd', attn_prob, value_heads).reshape(TOKENS, attn_width)
    gated = snap_bf16(gate_vals * attended)
    s_mid = snap_bf16(single_s + jnp.dot(gated, w_o, preferred_element_type=jnp.float32))
    mid_act = snap_bf16(layer_norm(s_mid))
    trans_a = jnp.dot(mid_act, w_sa, preferred_element_type=jnp.float32)
    trans_b = jnp.dot(mid_act, w_sb, preferred_element_type=jnp.float32)
    trans_hidden = snap_bf16(jax.nn.silu(trans_a) * trans_b)
    return z_new, s_mid + jnp.dot(trans_hidden, w_so, preferred_element_type=jnp.float32)


def draw_mask(mask_key):
    len_key, full_key = jax.random.split(mask_key)
    lengths = jax.random.randint(len_key, (COMPLEXES,), TOKENS // 4, TOKENS + 1)
    full_at = jax.random.randint(full_key, (), 0, COMPLEXES)
    lengths = jnp.where(jnp.arange(COMPLEXES) == full_at, TOKENS, lengths)
    return (jnp.arange(TOKENS)[None, :] < lengths[:, None]).astype(jnp.int32)


def setup_inputs(seed: int = 0) -> dict:
    sub_keys = jax.random.split(jax.random.key(seed), 17)
    attn_width = HEADS * HEAD

    def draw_normal(key_index, arr_shape, std_scale):
        return (jax.random.normal(sub_keys[key_index], arr_shape, jnp.float32) * std_scale).astype(jnp.bfloat16)

    return {
        'pair_z': draw_normal(0, (COMPLEXES, TOKENS, TOKENS, C_Z), 1.0),
        'single_s': draw_normal(1, (COMPLEXES, TOKENS, C_S), 1.0),
        'token_mask': draw_mask(sub_keys[2]),
        'dz_out': draw_normal(3, (COMPLEXES, TOKENS, TOKENS, C_Z), 1.0),
        'ds_out': draw_normal(4, (COMPLEXES, TOKENS, C_S), 1.0),
        'w_pa': draw_normal(5, (C_Z, TRANS * C_Z), C_Z ** -0.5),
        'w_pb': draw_normal(6, (C_Z, TRANS * C_Z), C_Z ** -0.5),
        'w_po': draw_normal(7, (TRANS * C_Z, C_Z), (TRANS * C_Z) ** -0.5),
        'w_bias': draw_normal(8, (C_Z, HEADS), C_Z ** -0.5),
        'w_q': draw_normal(9, (C_S, attn_width), C_S ** -0.5),
        'q_bias': draw_normal(10, (attn_width,), 0.5),
        'w_kv': draw_normal(11, (C_S, 2 * attn_width), C_S ** -0.5),
        'w_g': draw_normal(12, (C_S, attn_width), C_S ** -0.5),
        'w_o': draw_normal(13, (attn_width, C_S), attn_width ** -0.5),
        'w_sa': draw_normal(14, (C_S, TRANS * C_S), C_S ** -0.5),
        'w_sb': draw_normal(15, (C_S, TRANS * C_S), C_S ** -0.5),
        'w_so': draw_normal(16, (TRANS * C_S, C_S), (TRANS * C_S) ** -0.5),
    }


def reference(pair_z, single_s, token_mask, dz_out, ds_out, w_pa, w_pb, w_po, w_bias, w_q, q_bias, w_kv, w_g, w_o, w_sa, w_sb, w_so):
    weights = tuple(weight.astype(jnp.float32) for weight in (w_pa, w_pb, w_po, w_bias, w_q, q_bias, w_kv, w_g, w_o, w_sa, w_sb, w_so))

    def scan_step(running, per_complex):
        z_one, s_one, mask_one, dz_one, ds_one = per_complex

        def run_block(z_in, s_in, *params):
            return block_forward(z_in, s_in, mask_one, *params)

        _, pullback = jax.vjp(run_block, z_one.astype(jnp.float32), s_one.astype(jnp.float32), *weights)
        all_grads = pullback((dz_one.astype(jnp.float32), ds_one.astype(jnp.float32)))
        summed = tuple(acc_sum + update for acc_sum, update in zip(running, all_grads[2:]))
        return summed, (all_grads[0].astype(jnp.bfloat16), all_grads[1].astype(jnp.bfloat16))

    zero_sums = tuple(jnp.zeros_like(weight) for weight in weights)
    grad_sums, (dz_in, ds_in) = lax.scan(scan_step, zero_sums, (pair_z, single_s, token_mask, dz_out, ds_out))
    return (dz_in, ds_in, grad_sums[0], grad_sums[1], grad_sums[2], grad_sums[3], grad_sums[4], grad_sums[5], grad_sums[6], grad_sums[7], grad_sums[8], grad_sums[9], grad_sums[10], grad_sums[11])
```

```python
import jax
import jax.numpy as jnp
from jax import lax
from jax.experimental import pallas as pl
from jax.experimental.pallas import tpu as pltpu
from jax.sharding import PartitionSpec as P

HEADS = 16
HEAD_DIM = 24
EPSILON = 1e-5
MASK_BIG = 1e9
BF = jnp.bfloat16
F32 = jnp.float32
ROWS_S, ROWS_A, ROWS_P = 4608, 2048, 768
LANES = 128


def nn(a, b):
    return lax.dot_general(a, b, (((1,), (0,)), ((), ())), preferred_element_type=F32)


def nt(a, b):
    return lax.dot_general(a, b, (((1,), (1,)), ((), ())), preferred_element_type=F32)


def tn(a, b):
    return lax.dot_general(a, b, (((0,), (0,)), ((), ())), preferred_element_type=F32)


def sigmoid(x):
    return 0.5 * jnp.tanh(0.5 * x) + 0.5


def layer_norm(vals):
    centred = vals - jnp.mean(vals, axis=-1, keepdims=True)
    inv = lax.rsqrt(jnp.mean(centred * centred, axis=-1, keepdims=True) + EPSILON)
    return centred * inv, inv


def norm_grad(normed, inv, grad):
    mean_grad = jnp.mean(grad, axis=-1, keepdims=True)
    mean_proj = jnp.mean(grad * normed, axis=-1, keepdims=True)
    return inv * (grad - mean_grad - normed * mean_proj)


def swiglu_grad(ha, hb, dh):
    sig = sigmoid(ha)
    silu = ha * sig
    hidden = silu * hb
    grad_a = dh * hb * (sig * (1.0 + (ha - silu)))
    return hidden.astype(BF), grad_a.astype(BF), (dh * silu).astype(BF)


class Reducer:
    def __init__(self, place, rows, grads, recvs, final, send_sem, recv_sem):
        self.place, self.rows, self.grads, self.recvs, self.final = place, rows, grads, recvs, final
        self.send_sem, self.recv_sem = send_sem, recv_sem
        coords = place["coords"]
        self.order = [("x", "y", "z"), ("y", "z", "x"), ("z", "x", "y")]
        self.base = []
        for third in range(3):
            base = [coords["core"] * (rows // 2)]
            for depth, axis in enumerate(self.order[third]):
                base.append(base[-1] + coords[axis] * (rows >> (depth + 2)))
            self.base.append(base)

    def copy(self, stage, third):
        rows, base, order = self.rows, self.base[third], self.order[third]
        coords = self.place["coords"]
        step = rows // 16
        if stage < 4:
            size = rows >> (stage + 1)
            axis = "core" if stage == 0 else order[stage - 1]
            low = 0 if stage == 0 else base[stage - 1]
            start = pl.multiple_of(low + (1 - coords[axis]) * size, step)
            src = self.grads.at[third, pl.ds(start, size)]
            dst = self.recvs[stage].at[third]
        else:
            size = rows >> (8 - stage)
            axis = "core" if stage == 7 else order[6 - stage]
            start = pl.multiple_of(base[7 - stage], step)
            src = self.final.at[third, pl.ds(start, size)]
            dst = src
        return pltpu.make_async_remote_copy(
            src_ref=src, dst_ref=dst,
            send_sem=self.send_sem.at[stage, third], recv_sem=self.recv_sem.at[stage, third],
            device_id=self.place["peers"][axis], device_id_type=pl.DeviceIdType.MESH)

    def start(self, stage):
        for third in range(3):
            self.copy(stage, third).start()

    def step(self, stage):
        for third in range(3):
            done = stage - 1
            self.copy(done, third).wait()
            if done < 4:
                size = self.rows >> (done + 1)
                chunk = self.rows // 16
                low = self.base[third][done]
                dest = self.final if done == 3 else self.grads
                recv = self.recvs[done]

                def add(k, carry):
                    at = pl.ds(pl.multiple_of(low + k * chunk, chunk), chunk)
                    off = pl.ds(pl.multiple_of(k * chunk, chunk), chunk)
                    dest[third, at, :] = (self.grads[third, at, :].astype(F32) + recv[third, off, :].astype(F32)).astype(BF)
                    return carry

                lax.fori_loop(0, size // chunk, add, 0)
            if stage < 8:
                self.copy(stage, third).start()


def body_kernel(
        z_hbm, dz_hbm, wpa_hbm, wpb_hbm, wpo_hbm, wq_hbm, wkv_hbm, wg_hbm, wo_hbm, wsa_hbm, wsb_hbm, wso_hbm,
        s_ref, ds_ref, mask_ref, qb_ref, wbias_ref,
        dzin_ref, dsin_ref, fs_ref, fa_ref, fp_ref,
        z_v, dz_v, wpa, wpb, wpo, wq, wkv, wg, wo, wsa, wsb, wso,
        z1_v, w8, bias_v, prob_v, act_v, q_v, gate_v, att_v, gated_v, gatt_v, gmid_v, kv_v, gkv_v, gkvr_v,
        dwpa, dwpb, dwpo, m8,
        gs, gs0, gs1, gs2, gs3, ga_, ga0, ga1, ga2, ga3, gp, gp0, gp1, gp2, gp3,
        in_sem, kv_sem, send_sem, recv_sem):
    dap = lax.axis_index("dap")
    dp = lax.axis_index("dp")
    core = lax.rem(dp, 2)
    cx = lax.rem(dp // 2, 2)
    cy = dp // 4
    peers = {
        "core": (dap, dp + 1 - 2 * core),
        "x": (dap, dp + 2 - 4 * cx),
        "y": (dap, dp + 4 - 8 * cy),
        "z": (1 - dap, dp),
    }
    place = {"coords": {"core": core, "x": cx, "y": cy, "z": dap}, "peers": peers}
    num_cplx, num_tok = mask_ref.shape
    half = num_tok // 2
    width = HEADS * HEAD_DIM

    loads = [(wkv_hbm, wkv), (wq_hbm, wq), (wg_hbm, wg), (wpa_hbm, wpa), (wpb_hbm, wpb), (wpo_hbm, wpo), (z_hbm, z_v),
             (wo_hbm, wo), (wsa_hbm, wsa), (wsb_hbm, wsb), (wso_hbm, wso), (dz_hbm, dz_v)]
    copies = [pltpu.make_async_copy(src, dst, in_sem.at[k]) for k, (src, dst) in enumerate(loads)]
    for item in copies:
        item.start()

    barrier = pltpu.get_barrier_semaphore()
    for peer in peers.values():
        pl.semaphore_signal(barrier, inc=1, device_id=peer, device_id_type=pl.DeviceIdType.MESH)
    pl.semaphore_wait(barrier, 4)

    red_s = Reducer(place, ROWS_S, gs, (gs0, gs1, gs2, gs3), fs_ref, send_sem.at[0], recv_sem.at[0])
    red_a = Reducer(place, ROWS_A, ga_, (ga0, ga1, ga2, ga3), fa_ref, send_sem.at[1], recv_sem.at[1])
    red_p = Reducer(place, ROWS_P, gp, (gp0, gp1, gp2, gp3), fp_ref, send_sem.at[2], recv_sem.at[2])

    s_f = s_ref[...].astype(F32)
    s_norm, s_inv = layer_norm(s_f)
    act = s_norm.astype(BF)
    act_v[...] = act
    copies[0].wait()
    kv_v[dap] = nn(act, wkv[...]).astype(BF)

    def kv_copy():
        return pltpu.make_async_remote_copy(
            src_ref=kv_v.at[dap], dst_ref=kv_v.at[dap], send_sem=kv_sem.at[0], recv_sem=kv_sem.at[1],
            device_id=peers["z"], device_id_type=pl.DeviceIdType.MESH)

    def gkv_copy():
        return pltpu.make_async_remote_copy(
            src_ref=gkv_v.at[1 - dap], dst_ref=gkvr_v, send_sem=kv_sem.at[2], recv_sem=kv_sem.at[3],
            device_id=peers["z"], device_id_type=pl.DeviceIdType.MESH)

    kv_copy().start()
    copies[1].wait()
    copies[2].wait()
    q_v[...] = (nn(act, wq[...]) + qb_ref[...].astype(F32)).astype(BF)
    gate_v[...] = sigmoid(nn(act, wg[...]))

    row_head = lax.broadcasted_iota(jnp.int32, (128, HEADS), 0)
    col_head = lax.broadcasted_iota(jnp.int32, (128, HEADS), 1)
    pick = jnp.where((row_head >= col_head * 8) & (row_head < col_head * 8 + 8), 1.0, 0.0).astype(BF)
    spread = nt(pick, wbias_ref[...])
    row8 = lax.rem(lax.broadcasted_iota(jnp.int32, (128, LANES), 0), 8)
    for k in range(8):
        w8[:, k * LANES:(k + 1) * LANES] = jnp.where(row8 == k, spread, 0.0).astype(BF)

    for k in range(3, 7):
        copies[k].wait()

    blk = 8 * num_tok
    per_cplx = half // 8
    num_blk = num_cplx * per_cplx

    def side_by_side(tokens):
        return jnp.concatenate([tokens[k * num_tok:(k + 1) * num_tok] for k in range(8)], axis=1)

    def pair_forward(b, carry):
        at = pl.ds(pl.multiple_of(b * blk, blk), blk)
        z_f = z_v[at, :].astype(F32)
        normed, _ = layer_norm(z_f)
        u = normed.astype(BF)
        total = z_f
        for f in range(0, 512, 256):
            ha = nn(u, wpa[:, f:f + 256])
            hb = nn(u, wpb[:, f:f + 256])
            hidden = (ha * sigmoid(ha) * hb).astype(BF)
            total = total + nn(hidden, wpo[f:f + 256, :])
        z1 = total.astype(BF)
        z1_v[at, :] = z1
        bias_norm, _ = layer_norm(z1.astype(F32))
        bias8 = nt(w8[...], side_by_side(bias_norm.astype(BF)))
        c, i0 = b // per_cplx, pl.multiple_of(lax.rem(b, per_cplx) * 8, 8)
        bias_v[c, :, pl.ds(i0, 8), :] = bias8.reshape(HEADS, 8, num_tok)
        return carry

    lax.fori_loop(0, num_blk, pair_forward, 0)

    scale = HEAD_DIM ** -0.5
    grow = lax.broadcasted_iota(jnp.int32, (HEADS, 1, width), 0) * HEAD_DIM
    gcol = lax.broadcasted_iota(jnp.int32, (HEADS, 1, width), 2)
    head_mask = (gcol >= grow) & (gcol < grow + HEAD_DIM)

    def expand(rows):
        wide = jnp.where(head_mask, rows.astype(F32)[None], 0.0)
        return wide.reshape(HEADS * half, width).astype(BF)

    def gather_heads(wide):
        return jnp.sum(jnp.where(head_mask, wide.reshape(HEADS, half, width), 0.0), axis=0)

    def tokens_of(c, lo):
        rows = slice(c * half, (c + 1) * half)
        return jnp.concatenate([kv_v[0, rows, lo:lo + width], kv_v[1, rows, lo:lo + width]], axis=0)

    kv_copy().wait()
    for c in range(num_cplx):
        rows = slice(c * half, (c + 1) * half)
        key_mask = MASK_BIG * (mask_ref[c:c + 1, :].astype(F32) - 1.0)
        logits = nt(expand(q_v[rows, :]), tokens_of(c, 0)) * scale + bias_v[c].reshape(HEADS * half, num_tok) + key_mask
        ex = jnp.exp(logits - jnp.max(logits, axis=-1, keepdims=True))
        prob = ex / jnp.sum(ex, axis=-1, keepdims=True)
        prob_v[c] = prob
        att_v[rows, :] = gather_heads(nn(prob.astype(BF), tokens_of(c, width)))
    gated = (gate_v[...] * att_v[...]).astype(BF)
    gated_v[...] = gated
    copies[7].wait()
    s_mid = (s_ref[...].astype(F32) + nn(gated, wo[...])).astype(BF)
    mid_norm, mid_inv = layer_norm(s_mid.astype(F32))
    mid_act = mid_norm.astype(BF)
    mid_t = mid_act.T

    for k in range(8, 11):
        copies[k].wait()
    ds_b = ds_ref[...]
    grad_mid_norm = None
    for t in range(3):
        cols = slice(t * 512, (t + 1) * 512)
        ta = nn(mid_act, wsa[:, cols])
        tb = nn(mid_act, wsb[:, cols])
        dh = nt(ds_b, wso[cols, :])
        hidden, grad_a, grad_b = swiglu_grad(ta, tb, dh)
        part = nt(grad_a, wsa[:, cols]) + nt(grad_b, wsb[:, cols])
        grad_mid_norm = part if grad_mid_norm is None else grad_mid_norm + part
        d_sa = nn(mid_t, grad_a).astype(BF)
        d_sb = nn(mid_t, grad_b).astype(BF)
        for k in range(4):
            gs[t, k * 384:(k + 1) * 384, :] = d_sa[:, k * LANES:(k + 1) * LANES]
            gs[t, 1536 + k * 384:1536 + (k + 1) * 384, :] = d_sb[:, k * LANES:(k + 1) * LANES]
        d_so = tn(hidden, ds_b).astype(BF)
        for k in range(3):
            gs[k, 3072 + t * 512:3072 + (t + 1) * 512, :] = d_so[:, k * LANES:(k + 1) * LANES]
    red_s.start(0)
    grad_mid = ds_b.astype(F32) + norm_grad(mid_norm, mid_inv, grad_mid_norm)
    gmid_v[...] = grad_mid
    grad_mid_bf = grad_mid.astype(BF)
    grad_gated = nt(grad_mid_bf, wo[...])
    gate = gate_v[...]
    gatt_v[...] = (grad_gated * gate).astype(BF)
    grad_gate_pre = (grad_gated * att_v[...] * gate * (1.0 - gate)).astype(BF)

    def put_attn(name_row, value):
        val = value.astype(BF)
        for k in range(val.shape[1] // LANES):
            per = val.shape[1] // width
            lo = name_row + (k % per) * 384
            ga_[k // per, lo:lo + 384, :] = val[:, k * LANES:(k + 1) * LANES]

    act_t = act_v[...].T
    put_attn(1152, nn(act_t, grad_gate_pre))
    put_attn(1536, tn(gated_v[...], grad_mid_bf))

    grad_q_parts = []
    for c in range(num_cplx):
        rows = slice(c * half, (c + 1) * half)
        keys, vals = tokens_of(c, 0), tokens_of(c, width)
        gatt = expand(gatt_v[rows, :])
        prob = prob_v[c]
        grad_prob = nt(gatt, vals)
        grad_vals = tn(prob.astype(BF), gatt)
        grad_logits = prob * (grad_prob - jnp.sum(prob * grad_prob, axis=-1, keepdims=True))
        bias_v[c] = grad_logits.reshape(HEADS, half, num_tok)
        gl_b = grad_logits.astype(BF)
        grad_q_parts.append(gather_heads(nn(gl_b, keys)) * scale)
        grad_keys = tn(gl_b, expand(q_v[rows, :])) * scale
        for d in range(2):
            gkv_v[d, rows, 0:width] = grad_keys[d * half:(d + 1) * half].astype(BF)
            gkv_v[d, rows, width:2 * width] = grad_vals[d * half:(d + 1) * half].astype(BF)
        if c == 1:
            red_s.step(1)
    gkv_copy().start()
    grad_q = jnp.concatenate(grad_q_parts, axis=0)
    grad_q_bf = grad_q.astype(BF)
    put_attn(0, nn(act_t, grad_q_bf))
    row16 = lax.broadcasted_iota(jnp.int32, (16, width), 0)
    bias_tile = jnp.where(row16 == 0, jnp.sum(grad_q, axis=0, keepdims=True), 0.0).astype(BF)
    for t in range(3):
        ga_[t, 1920:1936, :] = bias_tile[:, t * LANES:(t + 1) * LANES]
        ga_[t, 1936:2048, :] = jnp.zeros((112, LANES), BF)
    grad_act = nt(grad_q_bf, wq[...]) + nt(grad_gate_pre, wg[...])
    gkv_copy().wait()
    grad_kv = (gkv_v[dap].astype(F32) + gkvr_v[...].astype(F32)).astype(BF)
    put_attn(384, nn(act_t, grad_kv))
    red_a.start(0)
    grad_act = grad_act + nt(grad_kv, wkv[...])
    s_norm2, s_inv2 = layer_norm(s_ref[...].astype(F32))
    dsin_ref[...] = (gmid_v[...] + norm_grad(s_norm2, s_inv2, grad_act)).astype(BF)

    copies[11].wait()
    for ref in (dwpa, dwpb, dwpo, m8):
        ref[...] = jnp.zeros(ref.shape, F32)

    hooks = {0: [(red_a, 1)], 2: [(red_s, 2)], 3: [(red_a, 2)], 5: [(red_s, 3), (red_a, 3)], 7: [(red_s, 4), (red_a, 4)],
             9: [(red_s, 5), (red_a, 5)], 11: [(red_s, 6), (red_a, 6)]}

    def pair_backward(b, carry):
        at = pl.ds(pl.multiple_of(b * blk, blk), blk)
        c, i0 = b // per_cplx, pl.multiple_of(lax.rem(b, per_cplx) * 8, 8)
        gl = bias_v[c, :, pl.ds(i0, 8), :].reshape(8 * HEADS, num_tok).astype(BF)
        wide = tn(gl, w8[...])
        grad_norm = jnp.concatenate([wide[:, k * LANES:(k + 1) * LANES] for k in range(8)], axis=0)
        bias_norm, bias_inv = layer_norm(z1_v[at, :].astype(F32))
        m8[...] += nn(gl, side_by_side(bias_norm.astype(BF)))
        grad_new = dz_v[at, :].astype(F32) + norm_grad(bias_norm, bias_inv, grad_norm)
        gnb = grad_new.astype(BF)
        gnb_t = gnb.T
        normed, inv = layer_norm(z_v[at, :].astype(F32))
        u = normed.astype(BF)
        u_t = u.T
        grad_normed = None
        for f in range(0, 512, 256):
            cols = slice(f, f + 256)
            hidden, grad_a, grad_b = swiglu_grad(nn(u, wpa[:, cols]), nn(u, wpb[:, cols]), nt(gnb, wpo[cols, :]))
            dwpo[:, cols] += nn(gnb_t, hidden)
            dwpa[:, cols] += nn(u_t, grad_a)
            dwpb[:, cols] += nn(u_t, grad_b)
            part = nt(grad_a, wpa[:, cols]) + nt(grad_b, wpb[:, cols])
            grad_normed = part if grad_normed is None else grad_normed + part
        dzin_ref[at, :] = (grad_new + norm_grad(normed, inv, grad_normed)).astype(BF)
        for when, todo in hooks.items():
            @pl.when(b == when)
            def _():
                for red, stage in todo:
                    red.step(stage)
        return carry

    lax.fori_loop(0, num_blk, pair_backward, 0)

    for t, ref in enumerate((dwpa, dwpb, dwpo)):
        for k in range(4):
            gp[t, k * 128:(k + 1) * 128, :] = ref[:, k * LANES:(k + 1) * LANES].astype(BF)
        gp[t, 528:768, :] = jnp.zeros((240, LANES), BF)
    diag = jnp.zeros((128, LANES), F32)
    for k in range(8):
        diag = diag + jnp.where(row8 == k, m8[:, k * LANES:(k + 1) * LANES], 0.0)
    gp[0, 512:528, :] = jnp.sum(diag.reshape(HEADS, 8, LANES), axis=1).astype(BF)
    for t in range(1, 3):
        gp[t, 512:528, :] = jnp.zeros((16, LANES), BF)
    red_p.start(0)
    red_p.step(1)
    red_p.step(2)
    red_s.step(7)
    red_a.step(7)
    red_p.step(3)
    red_p.step(4)
    red_p.step(5)
    red_p.step(6)
    red_s.step(8)
    red_a.step(8)
    red_p.step(7)
    red_p.step(8)


def unpack_kernel(fs, fa, fp, pa_o, pb_o, po_o, bias_o, q_o, qb_o, kv_o, g_o, o_o, sa_o, sb_o, so_o,
                  pa, pb, po, bias, q, qb, kv, g, o, sa, sb, so, sem):
    outs = [(sa, sa_o), (sb, sb_o), (so, so_o), (q, q_o), (kv, kv_o), (g, g_o), (o, o_o), (qb, qb_o), (pa, pa_o), (pb, pb_o),
            (po, po_o), (bias, bias_o)]
    copies = [pltpu.make_async_copy(src, dst, sem.at[k]) for k, (src, dst) in enumerate(outs)]
    for t in range(3):
        for k in range(4):
            cols = slice(t * 512 + k * LANES, t * 512 + (k + 1) * LANES)
            sa[:, cols] = fs[t, k * 384:(k + 1) * 384, :].astype(F32)
    copies[0].start()
    for t in range(3):
        for k in range(4):
            cols = slice(t * 512 + k * LANES, t * 512 + (k + 1) * LANES)
            sb[:, cols] = fs[t, 1536 + k * 384:1536 + (k + 1) * 384, :].astype(F32)
    copies[1].start()
    for k in range(3):
        so[:, k * LANES:(k + 1) * LANES] = fs[k, 3072:4608, :].astype(F32)
    copies[2].start()
    for index, (ref, row) in enumerate(((q, 0), (kv, 384), (g, 1152), (o, 1536))):
        per = ref.shape[1] // 384
        for k in range(3 * per):
            lo = row + (k % per) * 384
            ref[:, k * LANES:(k + 1) * LANES] = fa[k // per, lo:lo + 384, :].astype(F32)
        copies[3 + index].start()
    for t in range(3):
        qb[:, t * LANES:(t + 1) * LANES] = fa[t, 1920:1936, :].astype(F32)[0:1]
    copies[7].start()
    for t, ref in enumerate((pa, pb)):
        for k in range(4):
            ref[:, k * LANES:(k + 1) * LANES] = fp[t, k * 128:(k + 1) * 128, :].astype(F32)
        copies[8 + t].start()
    for k in range(4):
        po[k * 128:(k + 1) * 128, :] = fp[2, k * 128:(k + 1) * 128, :].astype(F32).T
    copies[10].start()
    bias[...] = fp[0, 512:640, :].astype(F32).T[:, 0:HEADS]
    copies[11].start()
    for item in copies:
        item.wait()


def solution(mesh):
    pair_spec = P('dp', 'dap', None, None)
    single_spec = P('dp', 'dap', None)
    hbm = pl.BlockSpec(memory_space=pl.ANY)
    vmem = pl.BlockSpec(memory_space=pltpu.VMEM)

    def body(pair_z, single_s, token_mask, dz_out, ds_out, w_pa, w_pb, w_po, w_bias, w_q, q_bias, w_kv, w_g, w_o, w_sa, w_sb, w_so):
        num_cplx, half, num_tok, dim = pair_z.shape
        toks = num_cplx * half * num_tok
        rows = num_cplx * half
        width = w_q.shape[1]
        big = (pair_z.reshape(toks, dim), dz_out.reshape(toks, dim), w_pa, w_pb, w_po, w_q, w_kv, w_g, w_o, w_sa, w_sb, w_so)
        small = (single_s.reshape(rows, width), ds_out.reshape(rows, width), token_mask, q_bias.reshape(1, width), w_bias)
        scratch = [pltpu.VMEM(a.shape, a.dtype) for a in big]
        scratch += [
            pltpu.VMEM((toks, dim), BF), pltpu.VMEM((128, 1024), BF),
            pltpu.VMEM((num_cplx, HEADS, half, num_tok), F32), pltpu.VMEM((num_cplx, HEADS * half, num_tok), F32),
            pltpu.VMEM((rows, width), BF), pltpu.VMEM((rows, width), BF), pltpu.VMEM((rows, width), F32),
            pltpu.VMEM((rows, width), F32), pltpu.VMEM((rows, width), BF), pltpu.VMEM((rows, width), BF),
            pltpu.VMEM((rows, width), F32),
            pltpu.VMEM((2, rows, 2 * width), BF), pltpu.VMEM((2, rows, 2 * width), BF), pltpu.VMEM((rows, 2 * width), BF),
            pltpu.VMEM((128, 512), F32), pltpu.VMEM((128, 512), F32), pltpu.VMEM((128, 512), F32), pltpu.VMEM((128, 1024), F32),
        ]
        for total in (ROWS_S, ROWS_A, ROWS_P):
            scratch += [pltpu.VMEM((3, total >> k, LANES), BF) for k in range(5)]
        scratch += [pltpu.SemaphoreType.DMA((12,)), pltpu.SemaphoreType.DMA((4,)),
                    pltpu.SemaphoreType.DMA((3, 8, 3)), pltpu.SemaphoreType.DMA((3, 8, 3))]
        dz_in, ds_in, fs, fa, fp = pl.pallas_call(
            body_kernel,
            out_shape=[jax.ShapeDtypeStruct((toks, dim), BF), jax.ShapeDtypeStruct((rows, width), BF)] + [
                jax.ShapeDtypeStruct((3, total, LANES), BF) for total in (ROWS_S, ROWS_A, ROWS_P)],
            in_specs=[hbm] * 12 + [vmem] * 5,
            out_specs=[vmem] * 5,
            scratch_shapes=scratch,
            compiler_params=pltpu.CompilerParams(collective_id=0, has_side_effects=True, vmem_limit_bytes=60 * 2 ** 20),
            name="block",
        )(*big, *small)
        shapes = [w_pa.shape, w_pb.shape, w_po.shape, w_bias.shape, w_q.shape, (1, width), w_kv.shape, w_g.shape, w_o.shape,
                  w_sa.shape, w_sb.shape, w_so.shape]
        grads = pl.pallas_call(
            unpack_kernel,
            out_shape=[jax.ShapeDtypeStruct(shape, F32) for shape in shapes],
            in_specs=[vmem] * 3,
            out_specs=[hbm] * 12,
            scratch_shapes=[pltpu.VMEM(shape, F32) for shape in shapes] + [pltpu.SemaphoreType.DMA((12,))],
            compiler_params=pltpu.CompilerParams(vmem_limit_bytes=40 * 2 ** 20),
            name="unpack",
        )(fs, fa, fp)
        grads = list(grads)
        grads[5] = grads[5].reshape(width)
        return (dz_in.reshape(pair_z.shape), ds_in.reshape(single_s.shape)) + tuple(grads)

    in_specs = (pair_spec, single_spec, P('dp', None), pair_spec, single_spec) + (P(),) * 12
    out_specs = (pair_spec, single_spec) + (P(),) * 12
    return jax.shard_map(body, mesh=mesh, in_specs=in_specs, out_specs=out_specs, check_vma=False)
```

```python
import jax
import jax.numpy as jnp
from jax import lax
from jax.experimental import pallas as pl
from jax.experimental.pallas import tpu as pltpu
from jax.sharding import PartitionSpec as P

HEADS = 16
HEAD_DIM = 24
EPSILON = 1e-5
MASK_BIG = 1e9
BF = jnp.bfloat16
F32 = jnp.float32
ROWS_A, ROWS_P = 2048, 544
LANES = 128


def nn(a, b):
    return lax.dot_general(a, b, (((1,), (0,)), ((), ())), preferred_element_type=F32)


def nt(a, b):
    return lax.dot_general(a, b, (((1,), (1,)), ((), ())), preferred_element_type=F32)


def tn(a, b):
    return lax.dot_general(a, b, (((0,), (0,)), ((), ())), preferred_element_type=F32)


def sigmoid(x):
    return 0.5 * jnp.tanh(0.5 * x) + 0.5


def layer_norm(vals):
    centred = vals - jnp.mean(vals, axis=-1, keepdims=True)
    inv = lax.rsqrt(jnp.mean(centred * centred, axis=-1, keepdims=True) + EPSILON)
    return centred * inv, inv


def norm_grad(normed, inv, grad):
    mean_grad = jnp.mean(grad, axis=-1, keepdims=True)
    mean_proj = jnp.mean(grad * normed, axis=-1, keepdims=True)
    return inv * (grad - mean_grad - normed * mean_proj)


def swiglu_grad(ha, hb, dh):
    sig = sigmoid(ha)
    silu = ha * sig
    hidden = silu * hb
    grad_a = dh * hb * (sig * (1.0 + (ha - silu)))
    return hidden.astype(BF), grad_a.astype(BF), (dh * silu).astype(BF)


AXES = ("x", "y", "z")
ORDER = (("x", "y", "z"), ("y", "z", "x"), ("z", "x", "y"))
ORDER_YZ = (("y", "z"), ("z", "y"), ("y", "z"))


def remote(place, src, dst, send_sem, recv_sem, axis):
    return pltpu.make_async_remote_copy(
        src_ref=src, dst_ref=dst, send_sem=send_sem, recv_sem=recv_sem,
        device_id=place["peers"][axis], device_id_type=pl.DeviceIdType.MESH)


class Reducer:
    last = 8

    def __init__(self, place, rows, grads, recvs, final, send_sem, recv_sem):
        self.place, self.rows, self.grads, self.recvs, self.final = place, rows, grads, recvs, final
        self.send_sem, self.recv_sem = send_sem, recv_sem
        coords = place["coords"]
        self.base = []
        for third in range(3):
            base = [coords["core"] * (rows // 2)]
            for depth, axis in enumerate(ORDER[third]):
                base.append(base[-1] + coords[axis] * (rows >> (depth + 2)))
            self.base.append(base)

    def copy(self, stage, third):
        rows, base, order = self.rows, self.base[third], ORDER[third]
        coords = self.place["coords"]
        step = rows // 16
        if stage < 4:
            size = rows >> (stage + 1)
            axis = "core" if stage == 0 else order[stage - 1]
            low = 0 if stage == 0 else base[stage - 1]
            start = pl.multiple_of(low + (1 - coords[axis]) * size, step)
            src = self.grads.at[third, pl.ds(start, size)]
            dst = self.recvs[stage].at[third]
        else:
            size = rows >> (8 - stage)
            axis = "core" if stage == 7 else order[6 - stage]
            start = pl.multiple_of(base[7 - stage], step)
            src = self.final.at[third, pl.ds(start, size)]
            dst = src
        return remote(self.place, src, dst, self.send_sem.at[stage, third], self.recv_sem.at[stage, third], axis)

    def add(self, third, low, size, chunk, recv, dest):
        def run(k, carry):
            at = pl.ds(pl.multiple_of(low + k * chunk, chunk), chunk)
            off = pl.ds(pl.multiple_of(k * chunk, chunk), chunk)
            dest[third, at, :] = (self.grads[third, at, :].astype(F32) + recv[third, off, :].astype(F32)).astype(BF)
            return carry

        lax.fori_loop(0, size // chunk, run, 0)

    def start(self):
        for third in range(3):
            self.copy(0, third).start()

    def step(self, stage):
        for third in range(3):
            done = stage - 1
            self.copy(done, third).wait()
            if done < 4:
                self.add(third, self.base[third][done], self.rows >> (done + 1), self.rows // 16, self.recvs[done],
                         self.final if done == 3 else self.grads)
            if stage < self.last:
                self.copy(stage, third).start()


class Doubler(Reducer):
    last = 5

    def copy(self, stage, third):
        half = self.rows // 2
        core = self.place["coords"]["core"]
        mine = pl.ds(pl.multiple_of(core * half, 16), half)
        if stage == 0:
            src = self.grads.at[third, pl.ds(pl.multiple_of((1 - core) * half, 16), half)]
            dst, axis = self.recvs[0].at[third], "core"
        elif stage < 4:
            src, dst, axis = self.grads.at[third, mine], self.recvs[stage].at[third], ORDER[third][stage - 1]
        else:
            src, dst, axis = self.final.at[third, mine], self.final.at[third, mine], "core"
        return remote(self.place, src, dst, self.send_sem.at[stage, third], self.recv_sem.at[stage, third], axis)

    def step(self, stage):
        half = self.rows // 2
        for third in range(3):
            done = stage - 1
            self.copy(done, third).wait()
            if done < 4:
                self.add(third, self.base[third][0], half, half, self.recvs[done], self.final if done == 3 else self.grads)
            if stage < self.last:
                self.copy(stage, third).start()


class Gatherer:
    def __init__(self, place, buf, send_sem, recv_sem):
        self.place, self.buf, self.send_sem, self.recv_sem = place, buf, send_sem, recv_sem

    def copy(self, stage, third):
        coords, order = self.place["coords"], ORDER[third]
        got = order[:stage - 1]
        index = [third, coords["core"]] + [slice(None) if axis in got else coords[axis] for axis in AXES]
        ref = self.buf.at[tuple(index)]
        axis = order[stage - 1] if stage < 4 else "core"
        return remote(self.place, ref, ref, self.send_sem.at[stage, third], self.recv_sem.at[stage, third], axis)

    def step(self, stage):
        for third in range(3):
            if stage > 1:
                self.copy(stage - 1, third).wait()
            if stage < 5:
                self.copy(stage, third).start()


class Tiles:
    def __init__(self, place, buf0, buf1, send_sem, recv_sem):
        self.place, self.bufs, self.send_sem, self.recv_sem = place, (buf0, buf1), send_sem, recv_sem

    def copy(self, core, stage, third):
        coords = self.place["coords"]
        order = ORDER[third] if core == 0 else ORDER_YZ[third]
        axes = AXES if core == 0 else AXES[1:]
        if stage > len(order):
            ref, axis, slot = self.bufs[core].at[third], "core", 4 + core
        else:
            got = order[:stage - 1]
            ref = self.bufs[core].at[tuple([third] + [slice(None) if axis in got else coords[axis] for axis in axes])]
            axis, slot = order[stage - 1], stage
        return remote(self.place, ref, ref, self.send_sem.at[slot, third], self.recv_sem.at[slot, third], axis)

    def step(self, stage):
        for core in range(2):
            last = 4 - core

            @pl.when(self.place["coords"]["core"] == core)
            def _():
                for third in range(3):
                    if 1 < stage <= last:
                        self.copy(core, stage - 1, third).wait()
                    if stage <= last:
                        self.copy(core, stage, third).start()
                    if stage == 5:
                        self.copy(core, last, third).wait_send()
                        self.copy(1 - core, 3 + core, third).wait_recv()


def body_kernel(
        z_hbm, dz_hbm, wpa_hbm, wpb_hbm, wpo_hbm, wq_hbm, wkv_hbm, wg_hbm, wo_hbm, wsa_hbm, wsb_hbm, wso_hbm,
        s_ref, ds_ref, mask_ref, qb_ref, wbias_ref,
        dzin_hbm, dsin_hbm, fs0_hbm, fs1_hbm, fa_hbm, fp_hbm,
        z_v, dz_v, wpa, wpb, wpo, wq, wkv, wg, wo, wsa, wsb, wso,
        z1_v, w8, bias_v, prob_v, act_v, q_v, gate_v, att_v, gated_v, gatt_v, gmid_v, kv_v, gkv_v, gkvr_v,
        dwpa, dwpb, dwpo, m8, dzin_ref, dsin_ref, c_all, ds_all, d_ab, d_so, fs0, fs1, fa_ref, fp_ref,
        ga_, ga0, ga1, ga2, ga3, gp, gp0, gp1, gp2, gp3,
        in_sem, out_sem, dz_sem, kv_sem, send_sem, recv_sem):
    dap = lax.axis_index("dap")
    dp = lax.axis_index("dp")
    core = lax.rem(dp, 2)
    cx = lax.rem(dp // 2, 2)
    cy = dp // 4
    peers = {
        "core": (dap, dp + 1 - 2 * core),
        "x": (dap, dp + 2 - 4 * cx),
        "y": (dap, dp + 4 - 8 * cy),
        "z": (1 - dap, dp),
    }
    place = {"coords": {"core": core, "x": cx, "y": cy, "z": dap}, "peers": peers}
    num_cplx, num_tok = mask_ref.shape
    half = num_tok // 2
    width = HEADS * HEAD_DIM

    loads = [(wkv_hbm, wkv), (wq_hbm, wq), (wg_hbm, wg), (wpa_hbm, wpa), (wpb_hbm, wpb), (wpo_hbm, wpo), (z_hbm, z_v),
             (wo_hbm, wo), (wsa_hbm, wsa), (wsb_hbm, wsb), (wso_hbm, wso), (dz_hbm, dz_v)]
    copies = [pltpu.make_async_copy(src, dst, in_sem.at[k]) for k, (src, dst) in enumerate(loads)]
    for item in copies:
        item.start()

    barrier = pltpu.get_barrier_semaphore()
    for peer in peers.values():
        pl.semaphore_signal(barrier, inc=1, device_id=peer, device_id_type=pl.DeviceIdType.MESH)
    pl.semaphore_wait(barrier, 4)

    red_a = Reducer(place, ROWS_A, ga_, (ga0, ga1, ga2, ga3), fa_ref, send_sem.at[0], recv_sem.at[0])
    red_p = Doubler(place, ROWS_P, gp, (gp0, gp1, gp2, gp3), fp_ref, send_sem.at[1], recv_sem.at[1])
    gat_ds = Gatherer(place, ds_all, send_sem.at[2], recv_sem.at[2])
    gat_c = Gatherer(place, c_all, send_sem.at[3], recv_sem.at[3])
    tiles = Tiles(place, fs0, fs1, send_sem.at[4], recv_sem.at[4])

    def own_block(buf, value):
        for t in range(3):
            buf[t, core, cx, cy, dap] = value[:, t * LANES:(t + 1) * LANES]

    own_block(ds_all, ds_ref[...])
    gat_ds.step(1)

    s_f = s_ref[...].astype(F32)
    s_norm, s_inv = layer_norm(s_f)
    act = s_norm.astype(BF)
    act_v[...] = act
    copies[0].wait()
    kv_v[dap] = nn(act, wkv[...]).astype(BF)

    def kv_copy():
        return pltpu.make_async_remote_copy(
            src_ref=kv_v.at[dap], dst_ref=kv_v.at[dap], send_sem=kv_sem.at[0], recv_sem=kv_sem.at[1],
            device_id=peers["z"], device_id_type=pl.DeviceIdType.MESH)

    def gkv_copy():
        return pltpu.make_async_remote_copy(
            src_ref=gkv_v.at[1 - dap], dst_ref=gkvr_v, send_sem=kv_sem.at[2], recv_sem=kv_sem.at[3],
            device_id=peers["z"], device_id_type=pl.DeviceIdType.MESH)

    kv_copy().start()
    copies[1].wait()
    copies[2].wait()
    q_v[...] = (nn(act, wq[...]) + qb_ref[...].astype(F32).reshape(1, width)).astype(BF)
    gate_v[...] = sigmoid(nn(act, wg[...]))

    row_head = lax.broadcasted_iota(jnp.int32, (128, HEADS), 0)
    col_head = lax.broadcasted_iota(jnp.int32, (128, HEADS), 1)
    pick = jnp.where((row_head >= col_head * 8) & (row_head < col_head * 8 + 8), 1.0, 0.0).astype(BF)
    spread = nn(pick, wbias_ref[...])
    row8 = lax.rem(lax.broadcasted_iota(jnp.int32, (128, LANES), 0), 8)
    for k in range(8):
        w8[:, k * LANES:(k + 1) * LANES] = jnp.where(row8 == k, spread, 0.0).astype(BF)

    for k in range(3, 7):
        copies[k].wait()

    blk = 8 * num_tok
    per_cplx = half // 8
    num_blk = num_cplx * per_cplx

    def side_by_side(tokens):
        return jnp.concatenate([tokens[k * num_tok:(k + 1) * num_tok] for k in range(8)], axis=1)

    def pair_forward(b, carry):
        at = pl.ds(pl.multiple_of(b * blk, blk), blk)
        z_f = z_v[at, :].astype(F32)
        normed, _ = layer_norm(z_f)
        u = normed.astype(BF)
        total = z_f
        for f in range(0, 512, 256):
            ha = nn(u, wpa[:, f:f + 256])
            hb = nn(u, wpb[:, f:f + 256])
            hidden = (ha * sigmoid(ha) * hb).astype(BF)
            total = total + nn(hidden, wpo[f:f + 256, :])
        z1 = total.astype(BF)
        z1_v[at, :] = z1
        bias_norm, _ = layer_norm(z1.astype(F32))
        bias8 = nt(w8[...], side_by_side(bias_norm.astype(BF)))
        c, i0 = b // per_cplx, pl.multiple_of(lax.rem(b, per_cplx) * 8, 8)
        bias_v[c, :, pl.ds(i0, 8), :] = bias8.reshape(HEADS, 8, num_tok)
        for when, stage in ((2, 2), (5, 3), (9, 4)):
            @pl.when(b == when)
            def _():
                gat_ds.step(stage)
        return carry

    lax.fori_loop(0, num_blk, pair_forward, 0)

    scale = HEAD_DIM ** -0.5
    grow = lax.broadcasted_iota(jnp.int32, (HEADS, 1, width), 0) * HEAD_DIM
    gcol = lax.broadcasted_iota(jnp.int32, (HEADS, 1, width), 2)
    head_mask = (gcol >= grow) & (gcol < grow + HEAD_DIM)

    def expand(rows):
        wide = jnp.where(head_mask, rows.astype(F32)[None], 0.0)
        return wide.reshape(HEADS * half, width).astype(BF)

    def gather_heads(wide):
        return jnp.sum(jnp.where(head_mask, wide.reshape(HEADS, half, width), 0.0), axis=0)

    def tokens_of(c, lo):
        rows = slice(c * half, (c + 1) * half)
        return jnp.concatenate([kv_v[0, rows, lo:lo + width], kv_v[1, rows, lo:lo + width]], axis=0)

    kv_copy().wait()
    for c in range(num_cplx):
        rows = slice(c * half, (c + 1) * half)
        key_mask = MASK_BIG * (mask_ref[c:c + 1, :].astype(F32) - 1.0)
        logits = nt(expand(q_v[rows, :]), tokens_of(c, 0)) * scale + bias_v[c].reshape(HEADS * half, num_tok) + key_mask
        ex = jnp.exp(logits - jnp.max(logits, axis=-1, keepdims=True))
        prob = ex / jnp.sum(ex, axis=-1, keepdims=True)
        prob_v[c] = prob
        att_v[rows, :] = gather_heads(nn(prob.astype(BF), tokens_of(c, width)))
    gated = (gate_v[...] * att_v[...]).astype(BF)
    gated_v[...] = gated
    copies[7].wait()
    s_mid = (s_ref[...].astype(F32) + nn(gated, wo[...])).astype(BF)
    mid_norm, mid_inv = layer_norm(s_mid.astype(F32))
    mid_act = mid_norm.astype(BF)
    own_block(c_all, mid_act)
    gat_c.step(1)
    gat_ds.step(5)

    for k in range(8, 11):
        copies[k].wait()
    ds_b = ds_ref[...]
    grad_mid_norm = None
    for t in range(3):
        cols = slice(t * 512, (t + 1) * 512)
        ta = nn(mid_act, wsa[:, cols])
        tb = nn(mid_act, wsb[:, cols])
        dh = nt(ds_b, wso[cols, :])
        _, grad_a, grad_b = swiglu_grad(ta, tb, dh)
        part = nt(grad_a, wsa[:, cols]) + nt(grad_b, wsb[:, cols])
        grad_mid_norm = part if grad_mid_norm is None else grad_mid_norm + part
    grad_mid = ds_b.astype(F32) + norm_grad(mid_norm, mid_inv, grad_mid_norm)
    gmid_v[...] = grad_mid
    grad_mid_bf = grad_mid.astype(BF)
    grad_gated = nt(grad_mid_bf, wo[...])
    gate = gate_v[...]
    gatt_v[...] = (grad_gated * gate).astype(BF)
    grad_gate_pre = (grad_gated * att_v[...] * gate * (1.0 - gate)).astype(BF)

    def put_attn(name_row, value):
        val = value.astype(BF)
        for k in range(val.shape[1] // LANES):
            per = val.shape[1] // width
            lo = name_row + (k % per) * 384
            ga_[k // per, lo:lo + 384, :] = val[:, k * LANES:(k + 1) * LANES]

    gat_c.step(2)
    act_t = act_v[...].T
    put_attn(1152, nn(act_t, grad_gate_pre))
    put_attn(1536, tn(gated_v[...], grad_mid_bf))

    grad_q_parts = []
    for c in range(num_cplx):
        rows = slice(c * half, (c + 1) * half)
        keys, vals = tokens_of(c, 0), tokens_of(c, width)
        gatt = expand(gatt_v[rows, :])
        prob = prob_v[c]
        grad_prob = nt(gatt, vals)
        grad_vals = tn(prob.astype(BF), gatt)
        grad_logits = prob * (grad_prob - jnp.sum(prob * grad_prob, axis=-1, keepdims=True))
        bias_v[c] = grad_logits.reshape(HEADS, half, num_tok)
        gl_b = grad_logits.astype(BF)
        grad_q_parts.append(gather_heads(nn(gl_b, keys)) * scale)
        grad_keys = tn(gl_b, expand(q_v[rows, :])) * scale
        for d in range(2):
            gkv_v[d, rows, 0:width] = grad_keys[d * half:(d + 1) * half].astype(BF)
            gkv_v[d, rows, width:2 * width] = grad_vals[d * half:(d + 1) * half].astype(BF)
    gkv_copy().start()
    grad_q = jnp.concatenate(grad_q_parts, axis=0)
    grad_q_bf = grad_q.astype(BF)
    put_attn(0, nn(act_t, grad_q_bf))
    row16 = lax.broadcasted_iota(jnp.int32, (16, width), 0)
    bias_tile = jnp.where(row16 == 0, jnp.sum(grad_q, axis=0, keepdims=True), 0.0).astype(BF)
    for t in range(3):
        ga_[t, 1920:1936, :] = bias_tile[:, t * LANES:(t + 1) * LANES]
        ga_[t, 1936:2048, :] = jnp.zeros((112, LANES), BF)
    grad_act = nt(grad_q_bf, wq[...]) + nt(grad_gate_pre, wg[...])
    gkv_copy().wait()
    grad_kv = (gkv_v[dap].astype(F32) + gkvr_v[...].astype(F32)).astype(BF)
    put_attn(384, nn(act_t, grad_kv))
    red_a.start()
    gat_c.step(3)
    grad_act = grad_act + nt(grad_kv, wkv[...])
    s_norm2, s_inv2 = layer_norm(s_ref[...].astype(F32))
    dsin_ref[...] = (gmid_v[...] + norm_grad(s_norm2, s_inv2, grad_act)).astype(BF)
    outs = [(dsin_ref, dsin_hbm), (fs0, fs0_hbm), (fs1, fs1_hbm), (fa_ref, fa_hbm), (fp_ref, fp_hbm)]
    out_copies = [pltpu.make_async_copy(src, dst, out_sem.at[k]) for k, (src, dst) in enumerate(outs)]
    out_copies[0].start()

    def tile_grads():
        tile = jnp.where(core == 0, 3 * (2 * cy + dap) + 2 * cx, 3 * (2 * cy + dap) + 1)
        at = pl.ds(pl.multiple_of(tile * LANES, LANES), LANES)
        w_ab = jnp.concatenate([wsa[:, at], wsb[:, at]], axis=1)
        w_o_tile = wso[at, :]
        d_ab[...] = jnp.zeros(d_ab.shape, F32)
        d_so[...] = jnp.zeros(d_so.shape, F32)

        def quarter(k, carry):
            def rows_of(buf):
                return jnp.concatenate([buf[t, k // 2, lax.rem(k, 2)].reshape(4 * 96, LANES) for t in range(3)], axis=1)

            acts, cots = rows_of(c_all), rows_of(ds_all)
            both = nn(acts, w_ab)
            hidden, grad_a, grad_b = swiglu_grad(both[:, :LANES], both[:, LANES:], nt(cots, w_o_tile))
            d_ab[...] += tn(acts, jnp.concatenate([grad_a, grad_b], axis=1))
            d_so[...] += tn(hidden, cots)
            return carry

        lax.fori_loop(0, 4, quarter, 0)
        for k in range(2):
            @pl.when(core == k)
            def _():
                slot = (cx, cy, dap) if k == 0 else (cy, dap)
                buf = fs0 if k == 0 else fs1
                buf[(0,) + slot] = d_ab[:, :LANES].astype(BF)
                buf[(1,) + slot] = d_ab[:, LANES:].astype(BF)
                so_b = d_so[...].astype(BF)
                buf[(2,) + slot] = jnp.concatenate([so_b[:, t * LANES:(t + 1) * LANES] for t in range(3)], axis=0)

    copies[11].wait()
    for ref in (dwpa, dwpb, dwpo, m8):
        ref[...] = jnp.zeros(ref.shape, F32)

    def hook(*calls):
        def run():
            for call in calls:
                call()
        return run

    def dz_copy(k):
        at = pl.ds(pl.multiple_of(k * blk, blk), blk)
        return pltpu.make_async_copy(dzin_ref.at[at, :], dzin_hbm.at[at, :], dz_sem.at[k])

    hooks = {
        0: hook(lambda: red_a.step(1)),
        2: hook(lambda: gat_c.step(4), lambda: red_a.step(2)),
        3: hook(lambda: gat_c.step(5), tile_grads, lambda: tiles.step(1)),
        4: hook(lambda: red_a.step(3)),
        5: hook(lambda: tiles.step(2)),
        6: hook(lambda: red_a.step(4)),
        7: hook(lambda: tiles.step(3)),
        8: hook(lambda: red_a.step(5)),
        10: hook(lambda: red_a.step(6)),
        11: hook(lambda: tiles.step(4)),
    }

    def pair_backward(b, carry):
        at = pl.ds(pl.multiple_of(b * blk, blk), blk)
        c, i0 = b // per_cplx, pl.multiple_of(lax.rem(b, per_cplx) * 8, 8)
        gl = bias_v[c, :, pl.ds(i0, 8), :].reshape(8 * HEADS, num_tok).astype(BF)
        wide = tn(gl, w8[...])
        grad_norm = jnp.concatenate([wide[:, k * LANES:(k + 1) * LANES] for k in range(8)], axis=0)
        bias_norm, bias_inv = layer_norm(z1_v[at, :].astype(F32))
        m8[...] += nn(gl, side_by_side(bias_norm.astype(BF)))
        grad_new = dz_v[at, :].astype(F32) + norm_grad(bias_norm, bias_inv, grad_norm)
        gnb = grad_new.astype(BF)
        gnb_t = gnb.T
        normed, inv = layer_norm(z_v[at, :].astype(F32))
        u = normed.astype(BF)
        u_t = u.T
        grad_normed = None
        for f in range(0, 512, 256):
            cols = slice(f, f + 256)
            hidden, grad_a, grad_b = swiglu_grad(nn(u, wpa[:, cols]), nn(u, wpb[:, cols]), nt(gnb, wpo[cols, :]))
            dwpo[:, cols] += nn(gnb_t, hidden)
            dwpa[:, cols] += nn(u_t, grad_a)
            dwpb[:, cols] += nn(u_t, grad_b)
            part = nt(grad_a, wpa[:, cols]) + nt(grad_b, wpb[:, cols])
            grad_normed = part if grad_normed is None else grad_normed + part
        dzin_ref[at, :] = (grad_new + norm_grad(normed, inv, grad_normed)).astype(BF)
        dz_copy(b).start()
        for when, todo in hooks.items():
            pl.when(b == when)(todo)
        return carry

    lax.fori_loop(0, num_blk, pair_backward, 0)

    for t, ref in enumerate((dwpa, dwpb, dwpo)):
        for k in range(4):
            gp[t, k * 128:(k + 1) * 128, :] = ref[:, k * LANES:(k + 1) * LANES].astype(BF)
        gp[t, 528:544, :] = jnp.zeros((16, LANES), BF)
    diag = jnp.zeros((128, LANES), F32)
    for k in range(8):
        diag = diag + jnp.where(row8 == k, m8[:, k * LANES:(k + 1) * LANES], 0.0)
    gp[0, 512:528, :] = jnp.sum(diag.reshape(HEADS, 8, LANES), axis=1).astype(BF)
    for t in range(1, 3):
        gp[t, 512:528, :] = jnp.zeros((16, LANES), BF)
    red_p.start()
    red_p.step(1)
    red_a.step(7)
    red_p.step(2)
    tiles.step(5)
    out_copies[1].start()
    out_copies[2].start()
    red_a.step(8)
    out_copies[3].start()
    red_p.step(3)
    red_p.step(4)
    red_p.step(5)
    out_copies[4].start()

    def drain(k, carry):
        dz_copy(k).wait()
        return carry

    lax.fori_loop(0, num_blk, drain, 0)
    for item in out_copies:
        item.wait()


def unpack_kernel(dz_i, ds_i, fs0_i, fs1_i, fa_i, fp_i,
                  dz_o, ds_o, pa_o, pb_o, po_o, bias_o, q_o, qb_o, kv_o, g_o, o_o, sa_o, sb_o, so_o,
                  dz, ds, fs0, fs1, fa, fp, pa, pb, po, bias, q, qb, kv, g, o, sa, sb, so, in_sem, sem):
    ins = [(fs0_i, fs0), (fs1_i, fs1), (fa_i, fa), (fp_i, fp), (dz_i, dz), (ds_i, ds)]
    reads = [pltpu.make_async_copy(src, dst, in_sem.at[k]) for k, (src, dst) in enumerate(ins)]
    for item in reads:
        item.start()
    outs = [(sa, sa_o), (sb, sb_o), (so, so_o), (q, q_o), (kv, kv_o), (g, g_o), (o, o_o), (qb, qb_o), (pa, pa_o), (pb, pb_o),
            (po, po_o), (bias, bias_o), (dz, dz_o), (ds, ds_o)]
    copies = [pltpu.make_async_copy(src, dst, sem.at[k]) for k, (src, dst) in enumerate(outs)]

    reads[0].wait()
    reads[1].wait()
    for kind in range(3):
        for pair in range(4):
            cy, cz = pair // 2, pair % 2
            for j in range(3):
                lo = (3 * pair + j) * LANES
                tile = fs1[kind, cy, cz] if j == 1 else fs0[kind, j // 2, cy, cz]
                wide = tile.astype(F32)
                if kind < 2:
                    (sa, sb)[kind][:, lo:lo + LANES] = wide
                else:
                    for k in range(3):
                        so[lo:lo + LANES, k * LANES:(k + 1) * LANES] = wide[k * LANES:(k + 1) * LANES]
        copies[kind].start()
    reads[2].wait()
    for index, (ref, row) in enumerate(((q, 0), (kv, 384), (g, 1152), (o, 1536))):
        per = ref.shape[1] // 384
        for k in range(3 * per):
            lo = row + (k % per) * 384
            ref[:, k * LANES:(k + 1) * LANES] = fa[k // per, lo:lo + 384, :].astype(F32)
        copies[3 + index].start()
    for t in range(3):
        qb[t * LANES:(t + 1) * LANES] = fa[t, 1920:1936, :].astype(F32)[0]
    copies[7].start()
    reads[3].wait()
    for t, ref in enumerate((pa, pb)):
        for k in range(4):
            ref[:, k * LANES:(k + 1) * LANES] = fp[t, k * 128:(k + 1) * 128, :].astype(F32)
        copies[8 + t].start()
    for k in range(4):
        po[k * 128:(k + 1) * 128, :] = fp[2, k * 128:(k + 1) * 128, :].astype(F32).T
    copies[10].start()
    bias[...] = fp[0, 512:528, :].astype(F32)
    copies[11].start()
    for k in range(2):
        reads[4 + k].wait()
        copies[12 + k].start()
    for item in copies:
        item.wait()


def solution(mesh):
    pair_spec = P('dp', 'dap', None, None)
    single_spec = P('dp', 'dap', None)
    hbm = pl.BlockSpec(memory_space=pl.ANY)
    vmem = pl.BlockSpec(memory_space=pltpu.VMEM)

    def body(pair_z, single_s, token_mask, dz_out, ds_out, w_pa, w_pb, w_po, w_bias, w_q, q_bias, w_kv, w_g, w_o, w_sa, w_sb, w_so):
        num_cplx, half, num_tok, dim = pair_z.shape
        toks = num_cplx * half * num_tok
        rows = num_cplx * half
        width = w_q.shape[1]
        big = (pair_z.reshape(toks, dim), dz_out.reshape(toks, dim), w_pa, w_pb, w_po, w_q, w_kv, w_g, w_o, w_sa, w_sb, w_so)
        small = (single_s.reshape(rows, width), ds_out.reshape(rows, width), token_mask, q_bias, w_bias.T)
        scratch = [pltpu.VMEM(a.shape, a.dtype) for a in big]
        finals = [(toks, dim), (rows, width), (3, 2, 2, 2, width, LANES), (3, 2, 2, width, LANES), (3, ROWS_A, LANES), (3, ROWS_P, LANES)]
        scratch += [
            pltpu.VMEM((toks, dim), BF), pltpu.VMEM((128, 1024), BF),
            pltpu.VMEM((num_cplx, HEADS, half, num_tok), F32), pltpu.VMEM((num_cplx, HEADS * half, num_tok), F32),
            pltpu.VMEM((rows, width), BF), pltpu.VMEM((rows, width), BF), pltpu.VMEM((rows, width), F32),
            pltpu.VMEM((rows, width), F32), pltpu.VMEM((rows, width), BF), pltpu.VMEM((rows, width), BF),
            pltpu.VMEM((rows, width), F32),
            pltpu.VMEM((2, rows, 2 * width), BF), pltpu.VMEM((2, rows, 2 * width), BF), pltpu.VMEM((rows, 2 * width), BF),
            pltpu.VMEM((128, 512), F32), pltpu.VMEM((128, 512), F32), pltpu.VMEM((128, 512), F32), pltpu.VMEM((128, 1024), F32),
            pltpu.VMEM(finals[0], BF), pltpu.VMEM(finals[1], BF),
            pltpu.VMEM((3, 2, 2, 2, 2, rows, LANES), BF), pltpu.VMEM((3, 2, 2, 2, 2, rows, LANES), BF),
            pltpu.VMEM((width, 2 * LANES), F32), pltpu.VMEM((LANES, width), F32),
        ]
        scratch += [pltpu.VMEM(shape, BF) for shape in finals[2:]]
        scratch += [pltpu.VMEM((3, ROWS_A >> k, LANES), BF) for k in range(5)]
        scratch += [pltpu.VMEM((3, ROWS_P, LANES), BF)] + [pltpu.VMEM((3, ROWS_P // 2, LANES), BF) for _ in range(4)]
        scratch += [pltpu.SemaphoreType.DMA((12,)), pltpu.SemaphoreType.DMA((5,)), pltpu.SemaphoreType.DMA((toks // (8 * num_tok),)),
                    pltpu.SemaphoreType.DMA((4,)), pltpu.SemaphoreType.DMA((5, 8, 3)), pltpu.SemaphoreType.DMA((5, 8, 3))]
        packed = pl.pallas_call(
            body_kernel,
            out_shape=[jax.ShapeDtypeStruct(shape, BF) for shape in finals],
            in_specs=[hbm] * 12 + [vmem] * 5,
            out_specs=[hbm] * 6,
            scratch_shapes=scratch,
            compiler_params=pltpu.CompilerParams(collective_id=0, has_side_effects=True, vmem_limit_bytes=60 * 2 ** 20),
            name="block",
        )(*big, *small)
        shapes = [w_pa.shape, w_pb.shape, w_po.shape, (HEADS, dim), w_q.shape, (width,), w_kv.shape, w_g.shape, w_o.shape,
                  w_sa.shape, w_sb.shape, w_so.shape]
        done = pl.pallas_call(
            unpack_kernel,
            out_shape=[jax.ShapeDtypeStruct(shape, BF) for shape in finals[:2]] + [jax.ShapeDtypeStruct(shape, F32) for shape in shapes],
            in_specs=[hbm] * 6,
            out_specs=[hbm] * 14,
            scratch_shapes=[pltpu.VMEM(shape, BF) for shape in finals] + [pltpu.VMEM(shape, F32) for shape in shapes] + [
                pltpu.SemaphoreType.DMA((6,)), pltpu.SemaphoreType.DMA((14,))],
            compiler_params=pltpu.CompilerParams(vmem_limit_bytes=56 * 2 ** 20),
            name="unpack",
        )(*packed)
        grads = list(done[2:])
        grads[3] = grads[3].T
        return (done[0].reshape(pair_z.shape), done[1].reshape(single_s.shape)) + tuple(grads)

    in_specs = (pair_spec, single_spec, P('dp', None), pair_spec, single_spec) + (P(),) * 12
    out_specs = (pair_spec, single_spec) + (P(),) * 12
    return jax.shard_map(body, mesh=mesh, in_specs=in_specs, out_specs=out_specs, check_vma=False)
```

```python
import jax
import jax.numpy as jnp
from jax import lax
from jax.experimental import pallas as pl
from jax.experimental.pallas import tpu as pltpu
from jax.sharding import PartitionSpec as P

HEADS = 16
HEAD_DIM = 24
EPSILON = 1e-5
MASK_BIG = 1e9
BF = jnp.bfloat16
F32 = jnp.float32
ROWS_A, ROWS_K, ROWS_P = 1280, 768, 544
LANES = 128


def nn(a, b):
    return lax.dot_general(a, b, (((1,), (0,)), ((), ())), preferred_element_type=F32)


def nt(a, b):
    return lax.dot_general(a, b, (((1,), (1,)), ((), ())), preferred_element_type=F32)


def tn(a, b):
    return lax.dot_general(a, b, (((0,), (0,)), ((), ())), preferred_element_type=F32)


def sigmoid(x):
    return 0.5 * jnp.tanh(0.5 * x) + 0.5


def layer_norm(vals):
    centred = vals - jnp.mean(vals, axis=-1, keepdims=True)
    inv = lax.rsqrt(jnp.mean(centred * centred, axis=-1, keepdims=True) + EPSILON)
    return centred * inv, inv


def norm_grad(normed, inv, grad):
    mean_grad = jnp.mean(grad, axis=-1, keepdims=True)
    mean_proj = jnp.mean(grad * normed, axis=-1, keepdims=True)
    return inv * (grad - mean_grad - normed * mean_proj)


def swiglu_grad(ha, hb, dh):
    sig = sigmoid(ha)
    silu = ha * sig
    hidden = silu * hb
    grad_a = dh * hb * (sig * (1.0 + (ha - silu)))
    return hidden.astype(BF), grad_a.astype(BF), (dh * silu).astype(BF)


AXES = ("x", "y", "z")
ORDER = (("x", "y", "z"), ("y", "z", "x"), ("z", "x", "y"))
ORDER_XY = (("x", "y"), ("y", "x"), ("x", "y"))


def remote(place, src, dst, send_sem, recv_sem, axis):
    return pltpu.make_async_remote_copy(
        src_ref=src, dst_ref=dst, send_sem=send_sem, recv_sem=recv_sem,
        device_id=place["peers"][axis], device_id_type=pl.DeviceIdType.MESH)


class Reducer:
    last = 8

    def __init__(self, place, rows, grads, recvs, final, send_sem, recv_sem):
        self.place, self.rows, self.grads, self.recvs, self.final = place, rows, grads, recvs, final
        self.send_sem, self.recv_sem = send_sem, recv_sem
        coords = place["coords"]
        self.base = []
        for third in range(3):
            base = [coords["core"] * (rows // 2)]
            for depth, axis in enumerate(ORDER[third]):
                base.append(base[-1] + coords[axis] * (rows >> (depth + 2)))
            self.base.append(base)

    def copy(self, stage, third):
        rows, base, order = self.rows, self.base[third], ORDER[third]
        coords = self.place["coords"]
        step = rows // 16
        if stage < 4:
            size = rows >> (stage + 1)
            axis = "core" if stage == 0 else order[stage - 1]
            low = 0 if stage == 0 else base[stage - 1]
            start = pl.multiple_of(low + (1 - coords[axis]) * size, step)
            src = self.grads.at[third, pl.ds(start, size)]
            dst = self.recvs[stage].at[third]
        else:
            size = rows >> (8 - stage)
            axis = "core" if stage == 7 else order[6 - stage]
            start = pl.multiple_of(base[7 - stage], step)
            src = self.final.at[third, pl.ds(start, size)]
            dst = src
        return remote(self.place, src, dst, self.send_sem.at[stage, third], self.recv_sem.at[stage, third], axis)

    def add(self, third, low, size, chunk, recv, dest):
        def run(k, carry):
            at = pl.ds(pl.multiple_of(low + k * chunk, chunk), chunk)
            off = pl.ds(pl.multiple_of(k * chunk, chunk), chunk)
            dest[third, at, :] = (self.grads[third, at, :].astype(F32) + recv[third, off, :].astype(F32)).astype(BF)
            return carry

        lax.fori_loop(0, size // chunk, run, 0)

    def start(self):
        for third in range(3):
            self.copy(0, third).start()

    def step(self, stage):
        for third in range(3):
            done = stage - 1
            self.copy(done, third).wait()
            if done < 4:
                self.add(third, self.base[third][done], self.rows >> (done + 1), self.rows // 16, self.recvs[done],
                         self.final if done == 3 else self.grads)
            if stage < self.last:
                self.copy(stage, third).start()


class Doubler(Reducer):
    last = 5

    def copy(self, stage, third):
        half = self.rows // 2
        core = self.place["coords"]["core"]
        mine = pl.ds(pl.multiple_of(core * half, 16), half)
        if stage == 0:
            src = self.grads.at[third, pl.ds(pl.multiple_of((1 - core) * half, 16), half)]
            dst, axis = self.recvs[0].at[third], "core"
        elif stage < 4:
            src, dst, axis = self.grads.at[third, mine], self.recvs[stage].at[third], ORDER[third][stage - 1]
        else:
            src, dst, axis = self.final.at[third, mine], self.final.at[third, mine], "core"
        return remote(self.place, src, dst, self.send_sem.at[stage, third], self.recv_sem.at[stage, third], axis)

    def step(self, stage):
        half = self.rows // 2
        for third in range(3):
            done = stage - 1
            self.copy(done, third).wait()
            if done < 4:
                self.add(third, self.base[third][0], half, half, self.recvs[done], self.final if done == 3 else self.grads)
            if stage < self.last:
                self.copy(stage, third).start()


class Gatherer:
    def __init__(self, place, buf, send_sem, recv_sem):
        self.place, self.buf, self.send_sem, self.recv_sem = place, buf, send_sem, recv_sem

    def copy(self, stage, third):
        coords, order = self.place["coords"], ORDER[third]
        got = order[:stage - 1]
        index = [third, coords["core"]] + [slice(None) if axis in got else coords[axis] for axis in AXES]
        ref = self.buf.at[tuple(index)]
        axis = order[stage - 1] if stage < 4 else "core"
        return remote(self.place, ref, ref, self.send_sem.at[stage, third], self.recv_sem.at[stage, third], axis)

    def step(self, stage):
        for third in range(3):
            if stage > 1:
                self.copy(stage - 1, third).wait()
            if stage < 5:
                self.copy(stage, third).start()


class Tiles:
    def __init__(self, place, buf0, buf1, send_sem, recv_sem):
        self.place, self.bufs, self.send_sem, self.recv_sem = place, (buf0, buf1), send_sem, recv_sem

    def copy(self, core, stage, third):
        coords = self.place["coords"]
        order = ORDER[third] if core == 0 else ORDER_XY[third]
        axes = AXES if core == 0 else AXES[:2]
        if stage > len(order):
            ref, axis, slot = self.bufs[core].at[third], "core", 4 + core
        else:
            got = order[:stage - 1]
            ref = self.bufs[core].at[tuple([third] + [slice(None) if axis in got else coords[axis] for axis in axes])]
            axis, slot = order[stage - 1], stage
        return remote(self.place, ref, ref, self.send_sem.at[slot, third], self.recv_sem.at[slot, third], axis)

    def step(self, stage):
        for core in range(2):
            last = 4 - core

            @pl.when(self.place["coords"]["core"] == core)
            def _():
                for third in range(3):
                    if 1 < stage <= last:
                        self.copy(core, stage - 1, third).wait()
                    if stage <= last:
                        self.copy(core, stage, third).start()
                    if stage == 5:
                        self.copy(core, last, third).wait_send()
                        self.copy(1 - core, 3 + core, third).wait_recv()


def body_kernel(
        z_hbm, dz_hbm, wpa_hbm, wpb_hbm, wpo_hbm, wq_hbm, wkv_hbm, wg_hbm, wo_hbm, wsa_hbm, wsb_hbm, wso_hbm,
        s_ref, ds_ref, mask_ref, qb_ref, wbias_ref,
        dzin_hbm, dsin_hbm, fs0_hbm, fs1_hbm, fa_hbm, fk_hbm, fp_hbm,
        z_v, dz_v, wpa, wpb, wpo, wq, wkv, wg, wo, wsa, wsb, wso,
        z1_v, w8, bias_v, prob_v, act_v, q_v, gate_v, att_v, gated_v, gatt_v, gmid_v, gact_v, kv_v, gkv_v, gkvr_v,
        dwpa, dwpb, dwpo, m8, dzin_ref, dsin_ref, c_all, ds_all, d_ab, d_so, gnew_v, gab_v,
        u0, u1, ut0, ut1, gn0, gn1, gnt0, gnt1, fs0, fs1, fa_ref, fk_ref, fp_ref,
        ga_, ga0, ga1, ga2, ga3, gk, gk0, gk1, gk2, gk3, gp, gp0, gp1, gp2, gp3,
        in_sem, out_sem, dz_sem, kv_sem, send_sem, recv_sem):
    dap = lax.axis_index("dap")
    dp = lax.axis_index("dp")
    core = lax.rem(dp, 2)
    cx = lax.rem(dp // 2, 2)
    cy = dp // 4
    peers = {
        "core": (dap, dp + 1 - 2 * core),
        "x": (dap, dp + 2 - 4 * cx),
        "y": (dap, dp + 4 - 8 * cy),
        "z": (1 - dap, dp),
    }
    place = {"coords": {"core": core, "x": cx, "y": cy, "z": dap}, "peers": peers}
    num_cplx, num_tok = mask_ref.shape
    half = num_tok // 2
    width = HEADS * HEAD_DIM

    loads = [(wkv_hbm, wkv), (wq_hbm, wq), (wg_hbm, wg), (wpa_hbm, wpa), (wpb_hbm, wpb), (wpo_hbm, wpo), (z_hbm, z_v),
             (wo_hbm, wo), (wsa_hbm, wsa), (wsb_hbm, wsb), (wso_hbm, wso), (dz_hbm, dz_v)]
    copies = [pltpu.make_async_copy(src, dst, in_sem.at[k]) for k, (src, dst) in enumerate(loads)]
    for item in copies:
        item.start()

    barrier = pltpu.get_barrier_semaphore()
    for peer in peers.values():
        pl.semaphore_signal(barrier, inc=1, device_id=peer, device_id_type=pl.DeviceIdType.MESH)

    red_a = Reducer(place, ROWS_A, ga_, (ga0, ga1, ga2, ga3), fa_ref, send_sem.at[0], recv_sem.at[0])
    red_p = Doubler(place, ROWS_P, gp, (gp0, gp1, gp2, gp3), fp_ref, send_sem.at[1], recv_sem.at[1])
    gat_ds = Gatherer(place, ds_all, send_sem.at[2], recv_sem.at[2])
    gat_c = Gatherer(place, c_all, send_sem.at[3], recv_sem.at[3])
    tiles = Tiles(place, fs0, fs1, send_sem.at[4], recv_sem.at[4])
    red_k = Reducer(place, ROWS_K, gk, (gk0, gk1, gk2, gk3), fk_ref, send_sem.at[5], recv_sem.at[5])

    def own_block(buf, value):
        for t in range(3):
            buf[t, core, cx, cy, dap] = value[:, t * LANES:(t + 1) * LANES]

    own_block(ds_all, ds_ref[...])

    s_f = s_ref[...].astype(F32)
    s_norm, s_inv = layer_norm(s_f)
    act = s_norm.astype(BF)
    act_v[...] = act
    copies[0].wait()
    kv_v[dap] = nn(act, wkv[...]).astype(BF)

    def kv_copy():
        return pltpu.make_async_remote_copy(
            src_ref=kv_v.at[dap], dst_ref=kv_v.at[dap], send_sem=kv_sem.at[0], recv_sem=kv_sem.at[1],
            device_id=peers["z"], device_id_type=pl.DeviceIdType.MESH)

    def gkv_copy():
        return pltpu.make_async_remote_copy(
            src_ref=gkv_v.at[1 - dap], dst_ref=gkvr_v, send_sem=kv_sem.at[2], recv_sem=kv_sem.at[3],
            device_id=peers["z"], device_id_type=pl.DeviceIdType.MESH)

    pl.semaphore_wait(barrier, 4)
    kv_copy().start()
    gat_ds.step(1)
    copies[1].wait()
    copies[2].wait()
    q_v[...] = (nn(act, wq[...]) + qb_ref[...].astype(F32).reshape(1, width)).astype(BF)
    gate_v[...] = sigmoid(nn(act, wg[...]))

    row_head = lax.broadcasted_iota(jnp.int32, (128, HEADS), 0)
    col_head = lax.broadcasted_iota(jnp.int32, (128, HEADS), 1)
    pick = jnp.where((row_head >= col_head * 8) & (row_head < col_head * 8 + 8), 1.0, 0.0).astype(BF)
    spread = nn(pick, wbias_ref[...])
    row8 = lax.rem(lax.broadcasted_iota(jnp.int32, (128, LANES), 0), 8)
    for k in range(8):
        w8[:, k * LANES:(k + 1) * LANES] = jnp.where(row8 == k, spread, 0.0).astype(BF)

    for k in range(3, 7):
        copies[k].wait()

    blk = 8 * num_tok
    per_cplx = half // 8
    num_blk = num_cplx * per_cplx

    def side_by_side(tokens):
        return jnp.concatenate([tokens[k * num_tok:(k + 1) * num_tok] for k in range(8)], axis=1)

    def rows_at(b):
        return pl.ds(pl.multiple_of(b * blk, blk), blk)

    def bias_at(b):
        return b // per_cplx, pl.ds(pl.multiple_of(lax.rem(b, per_cplx) * 8, 8), 8)

    def forward_norm(b, u_ref):
        normed, _ = layer_norm(z_v[rows_at(b), :].astype(F32))
        u_ref[...] = normed.astype(BF)

    def forward_main(b, u_ref):
        total = z_v[rows_at(b), :].astype(F32)
        for f in range(0, 512, 256):
            u = u_ref[...]
            ha = nn(u, wpa[:, f:f + 256])
            hb = nn(u, wpb[:, f:f + 256])
            hidden = (ha * sigmoid(ha) * hb).astype(BF)
            total = total + nn(hidden, wpo[f:f + 256, :])
        z1_v[rows_at(b), :] = total.astype(BF)

    def forward_bias(b):
        bias_norm, _ = layer_norm(z1_v[rows_at(b), :].astype(F32))
        c, at = bias_at(b)
        bias_v[c, :, at, :] = nt(w8[...], side_by_side(bias_norm.astype(BF))).reshape(HEADS, 8, num_tok)

    def forward_pair(p, carry):
        forward_bias(2 * p)
        forward_norm(2 * p + 2, u0)
        forward_main(2 * p + 1, u1)
        forward_bias(2 * p + 1)
        forward_norm(2 * p + 3, u1)
        forward_main(2 * p + 2, u0)
        for when, stage in ((1, 2), (4, 3)):
            @pl.when(p == when)
            def _():
                gat_ds.step(stage)
        return carry

    forward_norm(0, u0)
    forward_norm(1, u1)
    forward_main(0, u0)
    lax.fori_loop(0, num_blk // 2 - 1, forward_pair, 0)
    forward_bias(num_blk - 2)
    forward_main(num_blk - 1, u1)
    forward_bias(num_blk - 1)

    scale = HEAD_DIM ** -0.5
    grow = lax.broadcasted_iota(jnp.int32, (HEADS, 1, width), 0) * HEAD_DIM
    gcol = lax.broadcasted_iota(jnp.int32, (HEADS, 1, width), 2)
    head_mask = (gcol >= grow) & (gcol < grow + HEAD_DIM)

    def expand(rows):
        wide = jnp.where(head_mask, rows.astype(F32)[None], 0.0)
        return wide.reshape(HEADS * half, width).astype(BF)

    def gather_heads(wide):
        return jnp.sum(jnp.where(head_mask, wide.reshape(HEADS, half, width), 0.0), axis=0)

    def tokens_of(c, lo):
        rows = slice(c * half, (c + 1) * half)
        return jnp.concatenate([kv_v[0, rows, lo:lo + width], kv_v[1, rows, lo:lo + width]], axis=0)

    kv_copy().wait()
    for c in range(num_cplx):
        rows = slice(c * half, (c + 1) * half)
        key_mask = MASK_BIG * (mask_ref[c:c + 1, :].astype(F32) - 1.0)
        logits = nt(expand(q_v[rows, :]), tokens_of(c, 0)) * scale + bias_v[c].reshape(HEADS * half, num_tok) + key_mask
        ex = jnp.exp(logits - jnp.max(logits, axis=-1, keepdims=True))
        prob = ex / jnp.sum(ex, axis=-1, keepdims=True)
        prob_v[c] = prob
        att_v[rows, :] = gather_heads(nn(prob.astype(BF), tokens_of(c, width)))
    gated = (gate_v[...] * att_v[...]).astype(BF)
    gated_v[...] = gated
    copies[7].wait()
    s_mid = (s_ref[...].astype(F32) + nn(gated, wo[...])).astype(BF)
    mid_norm, mid_inv = layer_norm(s_mid.astype(F32))
    mid_act = mid_norm.astype(BF)
    own_block(c_all, mid_act)
    gat_c.step(1)

    for k in range(8, 11):
        copies[k].wait()
    ds_b = ds_ref[...]
    grad_mid_norm = None
    for t in range(3):
        cols = slice(t * 512, (t + 1) * 512)
        ta = nn(mid_act, wsa[:, cols])
        tb = nn(mid_act, wsb[:, cols])
        dh = nt(ds_b, wso[cols, :])
        _, grad_a, grad_b = swiglu_grad(ta, tb, dh)
        part = nt(grad_a, wsa[:, cols]) + nt(grad_b, wsb[:, cols])
        grad_mid_norm = part if grad_mid_norm is None else grad_mid_norm + part
    grad_mid = ds_b.astype(F32) + norm_grad(mid_norm, mid_inv, grad_mid_norm)
    gmid_v[...] = grad_mid
    grad_mid_bf = grad_mid.astype(BF)
    grad_gated = nt(grad_mid_bf, wo[...])
    gate = gate_v[...]
    gatt_v[...] = (grad_gated * gate).astype(BF)
    grad_gate_pre = (grad_gated * att_v[...] * gate * (1.0 - gate)).astype(BF)

    def put_attn(buf, name_row, value):
        val = value.astype(BF)
        per = val.shape[1] // width
        for k in range(val.shape[1] // LANES):
            lo = name_row + (k % per) * 384
            buf[k // per, lo:lo + 384, :] = val[:, k * LANES:(k + 1) * LANES]

    act_t = act_v[...].T
    put_attn(ga_, 384, nn(act_t, grad_gate_pre))
    put_attn(ga_, 768, tn(gated_v[...], grad_mid_bf))
    gat_c.step(2)
    gat_ds.step(4)

    grad_q_parts = []
    for c in range(num_cplx):
        rows = slice(c * half, (c + 1) * half)
        keys, vals = tokens_of(c, 0), tokens_of(c, width)
        gatt = expand(gatt_v[rows, :])
        prob = prob_v[c]
        grad_prob = nt(gatt, vals)
        grad_vals = tn(prob.astype(BF), gatt)
        grad_logits = prob * (grad_prob - jnp.sum(prob * grad_prob, axis=-1, keepdims=True))
        bias_v[c] = grad_logits.reshape(HEADS, half, num_tok)
        gl_b = grad_logits.astype(BF)
        grad_q_parts.append(gather_heads(nn(gl_b, keys)) * scale)
        grad_keys = tn(gl_b, expand(q_v[rows, :])) * scale
        for d in range(2):
            gkv_v[d, rows, 0:width] = grad_keys[d * half:(d + 1) * half].astype(BF)
            gkv_v[d, rows, width:2 * width] = grad_vals[d * half:(d + 1) * half].astype(BF)
    grad_q = jnp.concatenate(grad_q_parts, axis=0)
    grad_q_bf = grad_q.astype(BF)
    put_attn(ga_, 0, nn(act_t, grad_q_bf))
    row16 = lax.broadcasted_iota(jnp.int32, (16, width), 0)
    bias_tile = jnp.where(row16 == 0, jnp.sum(grad_q, axis=0, keepdims=True), 0.0).astype(BF)
    for t in range(3):
        ga_[t, 1152:1168, :] = bias_tile[:, t * LANES:(t + 1) * LANES]
        ga_[t, 1168:1280, :] = jnp.zeros((112, LANES), BF)
    red_a.start()
    gact_v[...] = nt(grad_q_bf, wq[...]) + nt(grad_gate_pre, wg[...])

    def finish_attention():
        gkv_copy().wait()
        grad_kv = (gkv_v[dap].astype(F32) + gkvr_v[...].astype(F32)).astype(BF)
        put_attn(gk, 0, tn(act_v[...], grad_kv))
        red_k.start()
        grad_act = gact_v[...] + nt(grad_kv, wkv[...])
        s_norm2, s_inv2 = layer_norm(s_ref[...].astype(F32))
        dsin_ref[...] = (gmid_v[...] + norm_grad(s_norm2, s_inv2, grad_act)).astype(BF)

    outs = [(dsin_ref, dsin_hbm), (fs0, fs0_hbm), (fs1, fs1_hbm), (fa_ref, fa_hbm), (fk_ref, fk_hbm), (fp_ref, fp_hbm)]
    out_copies = [pltpu.make_async_copy(src, dst, out_sem.at[k]) for k, (src, dst) in enumerate(outs)]

    def tile_grads():
        tile = jnp.where(core == 0, 3 * (2 * cx + cy) + 2 * dap, 3 * (2 * cx + cy) + 1)
        at = pl.ds(pl.multiple_of(tile * LANES, LANES), LANES)
        w_ab = jnp.concatenate([wsa[:, at], wsb[:, at]], axis=1)
        w_o_tile = wso[at, :]
        d_ab[...] = jnp.zeros(d_ab.shape, F32)
        d_so[...] = jnp.zeros(d_so.shape, F32)

        def quarter(k, carry):
            def rows_of(buf):
                return jnp.concatenate([buf[t, k // 2, lax.rem(k, 2)].reshape(4 * 96, LANES) for t in range(3)], axis=1)

            acts, cots = rows_of(c_all), rows_of(ds_all)
            both = nn(acts, w_ab)
            hidden, grad_a, grad_b = swiglu_grad(both[:, :LANES], both[:, LANES:], nt(cots, w_o_tile))
            d_ab[...] += tn(acts, jnp.concatenate([grad_a, grad_b], axis=1))
            d_so[...] += tn(hidden, cots)
            return carry

        lax.fori_loop(0, 4, quarter, 0)
        for k in range(2):
            @pl.when(core == k)
            def _():
                slot = (cx, cy, dap) if k == 0 else (cx, cy)
                buf = fs0 if k == 0 else fs1
                buf[(0,) + slot] = d_ab[:, :LANES].astype(BF)
                buf[(1,) + slot] = d_ab[:, LANES:].astype(BF)
                so_b = d_so[...].astype(BF)
                buf[(2,) + slot] = jnp.concatenate([so_b[:, t * LANES:(t + 1) * LANES] for t in range(3)], axis=0)

    copies[11].wait()
    for ref in (dwpa, dwpb, dwpo, m8):
        ref[...] = jnp.zeros(ref.shape, F32)

    def hook(*calls):
        def run():
            for call in calls:
                call()
        return run

    def dz_copy(k):
        at = pl.ds(pl.multiple_of(k * blk, blk), blk)
        return pltpu.make_async_copy(dzin_ref.at[at, :], dzin_hbm.at[at, :], dz_sem.at[k])

    hooks = {
        0: hook(lambda: gat_c.step(3), lambda: gkv_copy().start()),
        1: hook(lambda: red_a.step(1)),
        2: hook(lambda: gat_c.step(4)),
        3: hook(lambda: gat_c.step(5), lambda: gat_ds.step(5), tile_grads, lambda: tiles.step(1), lambda: red_a.step(2)),
        4: hook(finish_attention, lambda: red_a.step(3)),
        5: hook(lambda: tiles.step(2), lambda: red_a.step(4), lambda: red_k.step(1)),
    }
    tail_hooks = {
        2: hook(lambda: red_p.step(1)),
        4: hook(lambda: red_k.step(2), lambda: red_a.step(5)),
        7: hook(lambda: tiles.step(3)),
        9: hook(lambda: red_p.step(2)),
        11: hook(lambda: red_k.step(3), lambda: red_a.step(6)),
    }

    def backward_head(b, live, bufs):
        u_ref, ut_ref, gn_ref, gnt_ref = bufs
        at = rows_at(b)
        c, rows = bias_at(b)
        gl_f = bias_v[c, :, rows, :].reshape(8 * HEADS, num_tok)
        wide = tn(gl_f.astype(BF), w8[...])
        grad_norm = jnp.concatenate([wide[:, k * LANES:(k + 1) * LANES] for k in range(8)], axis=0)
        bias_norm, bias_inv = layer_norm(z1_v[at, :].astype(F32))
        m8[...] += nn((gl_f * live).astype(BF), side_by_side(bias_norm.astype(BF)))
        grad_new = dz_v[at, :].astype(F32) + norm_grad(bias_norm, bias_inv, grad_norm)
        gnew_v[at, :] = grad_new
        gnb = grad_new.astype(BF)
        gn_ref[...] = gnb
        gnt_ref[...] = gnb.T
        normed, _ = layer_norm(z_v[at, :].astype(F32))
        u = normed.astype(BF)
        u_ref[...] = u
        ut_ref[...] = u.T

    def backward_main(b, bufs):
        u_ref, ut_ref, gn_ref, gnt_ref = bufs
        at = rows_at(b)
        for f in range(0, 512, 256):
            cols = slice(f, f + 256)
            u, gnb = u_ref[...], gn_ref[...]
            hidden, grad_a, grad_b = swiglu_grad(nn(u, wpa[:, cols]), nn(u, wpb[:, cols]), nt(gnb, wpo[cols, :]))
            gab_v[at, cols] = grad_a
            gab_v[at, 512 + f:768 + f] = grad_b
            dwpo[:, cols] += nn(gnt_ref[...], hidden)
            dwpa[:, cols] += nn(ut_ref[...], grad_a)
            dwpb[:, cols] += nn(ut_ref[...], grad_b)

    def backward_tail(b, carry):
        at = rows_at(b)
        grad_normed = nt(gab_v[at, :], jnp.concatenate([wpa[...], wpb[...]], axis=1))
        normed, inv = layer_norm(z_v[at, :].astype(F32))
        dzin_ref[at, :] = (gnew_v[at, :] + norm_grad(normed, inv, grad_normed)).astype(BF)
        dz_copy(b).start()
        for when, todo in tail_hooks.items():
            pl.when(b == when)(todo)
        return carry

    bufs0, bufs1 = (u0, ut0, gn0, gnt0), (u1, ut1, gn1, gnt1)

    def backward_pair(p, carry):
        backward_head(2 * p + 1, 1.0, bufs1)
        backward_main(2 * p, bufs0)
        more = jnp.where(p < num_blk // 2 - 1, 1.0, 0.0)
        backward_head(jnp.minimum(2 * p + 2, num_blk - 1), more, bufs0)
        backward_main(2 * p + 1, bufs1)
        for when, todo in hooks.items():
            pl.when(p == when)(todo)
        return carry

    backward_head(0, 1.0, bufs0)
    lax.fori_loop(0, num_blk // 2, backward_pair, 0)
    out_copies[0].start()

    for t, ref in enumerate((dwpa, dwpb, dwpo)):
        for k in range(4):
            gp[t, k * 128:(k + 1) * 128, :] = ref[:, k * LANES:(k + 1) * LANES].astype(BF)
        gp[t, 528:544, :] = jnp.zeros((16, LANES), BF)
    diag = jnp.zeros((128, LANES), F32)
    for k in range(8):
        diag = diag + jnp.where(row8 == k, m8[:, k * LANES:(k + 1) * LANES], 0.0)
    gp[0, 512:528, :] = jnp.sum(diag.reshape(HEADS, 8, LANES), axis=1).astype(BF)
    for t in range(1, 3):
        gp[t, 512:528, :] = jnp.zeros((16, LANES), BF)
    red_p.start()
    lax.fori_loop(0, num_blk, backward_tail, 0)
    red_p.step(3)
    red_k.step(4)
    red_a.step(7)
    red_k.step(5)
    red_p.step(4)
    tiles.step(4)
    red_a.step(8)
    out_copies[3].start()
    red_k.step(6)
    red_p.step(5)
    out_copies[5].start()
    red_k.step(7)
    tiles.step(5)
    out_copies[1].start()
    out_copies[2].start()
    red_k.step(8)
    out_copies[4].start()

    def drain(k, carry):
        dz_copy(k).wait()
        return carry

    lax.fori_loop(0, num_blk, drain, 0)
    for item in out_copies:
        item.wait()


def unpack_kernel(dz_i, ds_i, fs0_i, fs1_i, fa_i, fk_i, fp_i,
                  dz_o, ds_o, pa_o, pb_o, po_o, bias_o, q_o, qb_o, kv_o, g_o, o_o, sa_o, sb_o, so_o,
                  dz, ds, fs0, fs1, fa, fk, fp, pa, pb, po, bias, q, qb, kv, g, o, sa, sb, so, in_sem, sem):
    ins = [(fs0_i, fs0), (fs1_i, fs1), (fa_i, fa), (fp_i, fp), (dz_i, dz), (ds_i, ds), (fk_i, fk)]
    reads = [pltpu.make_async_copy(src, dst, in_sem.at[k]) for k, (src, dst) in enumerate(ins)]
    for item in reads:
        item.start()
    outs = [(sa, sa_o), (sb, sb_o), (so, so_o), (q, q_o), (kv, kv_o), (g, g_o), (o, o_o), (qb, qb_o), (pa, pa_o), (pb, pb_o),
            (po, po_o), (bias, bias_o), (dz, dz_o), (ds, ds_o)]
    copies = [pltpu.make_async_copy(src, dst, sem.at[k]) for k, (src, dst) in enumerate(outs)]

    reads[0].wait()
    reads[1].wait()
    for kind in range(3):
        for pair in range(4):
            cx, cy = pair // 2, pair % 2
            for j in range(3):
                lo = (3 * pair + j) * LANES
                tile = fs1[kind, cx, cy] if j == 1 else fs0[kind, cx, cy, j // 2]
                wide = tile.astype(F32)
                if kind < 2:
                    (sa, sb)[kind][:, lo:lo + LANES] = wide
                else:
                    for k in range(3):
                        so[lo:lo + LANES, k * LANES:(k + 1) * LANES] = wide[k * LANES:(k + 1) * LANES]
        copies[kind].start()
    reads[2].wait()
    reads[6].wait()
    for index, (ref, buf, row) in enumerate(((q, fa, 0), (kv, fk, 0), (g, fa, 384), (o, fa, 768))):
        per = ref.shape[1] // 384
        for k in range(3 * per):
            lo = row + (k % per) * 384
            ref[:, k * LANES:(k + 1) * LANES] = buf[k // per, lo:lo + 384, :].astype(F32)
        copies[3 + index].start()
    for t in range(3):
        qb[t * LANES:(t + 1) * LANES] = fa[t, 1152:1168, :].astype(F32)[0]
    copies[7].start()
    reads[3].wait()
    for t, ref in enumerate((pa, pb)):
        for k in range(4):
            ref[:, k * LANES:(k + 1) * LANES] = fp[t, k * 128:(k + 1) * 128, :].astype(F32)
        copies[8 + t].start()
    for k in range(4):
        po[k * 128:(k + 1) * 128, :] = fp[2, k * 128:(k + 1) * 128, :].astype(F32).T
    copies[10].start()
    bias[...] = fp[0, 512:528, :].astype(F32)
    copies[11].start()
    for k in range(2):
        reads[4 + k].wait()
        copies[12 + k].start()
    for item in copies:
        item.wait()


def solution(mesh):
    pair_spec = P('dp', 'dap', None, None)
    single_spec = P('dp', 'dap', None)
    hbm = pl.BlockSpec(memory_space=pl.ANY)
    vmem = pl.BlockSpec(memory_space=pltpu.VMEM)

    def body(pair_z, single_s, token_mask, dz_out, ds_out, w_pa, w_pb, w_po, w_bias, w_q, q_bias, w_kv, w_g, w_o, w_sa, w_sb, w_so):
        num_cplx, half, num_tok, dim = pair_z.shape
        toks = num_cplx * half * num_tok
        rows = num_cplx * half
        width = w_q.shape[1]
        big = (pair_z.reshape(toks, dim), dz_out.reshape(toks, dim), w_pa, w_pb, w_po, w_q, w_kv, w_g, w_o, w_sa, w_sb, w_so)
        small = (single_s.reshape(rows, width), ds_out.reshape(rows, width), token_mask, q_bias, w_bias.T)
        scratch = [pltpu.VMEM(a.shape, a.dtype) for a in big]
        finals = [(toks, dim), (rows, width), (3, 2, 2, 2, width, LANES), (3, 2, 2, width, LANES), (3, ROWS_A, LANES), (3, ROWS_K, LANES), (3, ROWS_P, LANES)]
        scratch += [
            pltpu.VMEM((toks, dim), BF), pltpu.VMEM((128, 1024), BF),
            pltpu.VMEM((num_cplx, HEADS, half, num_tok), F32), pltpu.VMEM((num_cplx, HEADS * half, num_tok), F32),
            pltpu.VMEM((rows, width), BF), pltpu.VMEM((rows, width), BF), pltpu.VMEM((rows, width), F32),
            pltpu.VMEM((rows, width), F32), pltpu.VMEM((rows, width), BF), pltpu.VMEM((rows, width), BF),
            pltpu.VMEM((rows, width), F32), pltpu.VMEM((rows, width), F32),
            pltpu.VMEM((2, rows, 2 * width), BF), pltpu.VMEM((2, rows, 2 * width), BF), pltpu.VMEM((rows, 2 * width), BF),
            pltpu.VMEM((128, 512), F32), pltpu.VMEM((128, 512), F32), pltpu.VMEM((128, 512), F32), pltpu.VMEM((128, 1024), F32),
            pltpu.VMEM(finals[0], BF), pltpu.VMEM(finals[1], BF),
            pltpu.VMEM((3, 2, 2, 2, 2, rows, LANES), BF), pltpu.VMEM((3, 2, 2, 2, 2, rows, LANES), BF),
            pltpu.VMEM((width, 2 * LANES), F32), pltpu.VMEM((LANES, width), F32),
            pltpu.VMEM((toks, dim), F32), pltpu.VMEM((toks, 1024), BF),
        ]
        for _ in range(2):
            scratch += [pltpu.VMEM((512, dim), BF)] * 2 + [pltpu.VMEM((dim, 512), BF)] * 2
        scratch += [pltpu.VMEM(shape, BF) for shape in finals[2:]]
        for total in (ROWS_A, ROWS_K):
            scratch += [pltpu.VMEM((3, total >> k, LANES), BF) for k in range(5)]
        scratch += [pltpu.VMEM((3, ROWS_P, LANES), BF)] + [pltpu.VMEM((3, ROWS_P // 2, LANES), BF) for _ in range(4)]
        scratch += [pltpu.SemaphoreType.DMA((12,)), pltpu.SemaphoreType.DMA((6,)), pltpu.SemaphoreType.DMA((toks // (8 * num_tok),)),
                    pltpu.SemaphoreType.DMA((4,)), pltpu.SemaphoreType.DMA((6, 8, 3)), pltpu.SemaphoreType.DMA((6, 8, 3))]
        packed = pl.pallas_call(
            body_kernel,
            out_shape=[jax.ShapeDtypeStruct(shape, BF) for shape in finals],
            in_specs=[hbm] * 12 + [vmem] * 5,
            out_specs=[hbm] * 7,
            scratch_shapes=scratch,
            compiler_params=pltpu.CompilerParams(collective_id=0, has_side_effects=True, vmem_limit_bytes=60 * 2 ** 20),
            name="block",
        )(*big, *small)
        shapes = [w_pa.shape, w_pb.shape, w_po.shape, (HEADS, dim), w_q.shape, (width,), w_kv.shape, w_g.shape, w_o.shape,
                  w_sa.shape, w_sb.shape, w_so.shape]
        done = pl.pallas_call(
            unpack_kernel,
            out_shape=[jax.ShapeDtypeStruct(shape, BF) for shape in finals[:2]] + [jax.ShapeDtypeStruct(shape, F32) for shape in shapes],
            in_specs=[hbm] * 7,
            out_specs=[hbm] * 14,
            scratch_shapes=[pltpu.VMEM(shape, BF) for shape in finals] + [pltpu.VMEM(shape, F32) for shape in shapes] + [
                pltpu.SemaphoreType.DMA((7,)), pltpu.SemaphoreType.DMA((14,))],
            compiler_params=pltpu.CompilerParams(vmem_limit_bytes=56 * 2 ** 20),
            name="unpack",
        )(*packed)
        grads = list(done[2:])
        grads[3] = grads[3].T
        return (done[0].reshape(pair_z.shape), done[1].reshape(single_s.shape)) + tuple(grads)

    in_specs = (pair_spec, single_spec, P('dp', None), pair_spec, single_spec) + (P(),) * 12
    out_specs = (pair_spec, single_spec) + (P(),) * 12
    return jax.shard_map(body, mesh=mesh, in_specs=in_specs, out_specs=out_specs, check_vma=False)
```

```python
import jax
import jax.numpy as jnp
from jax import lax
from jax.experimental import pallas as pl
from jax.experimental.pallas import tpu as pltpu
from jax.sharding import PartitionSpec as P

HEADS = 16
HEAD_DIM = 24
EPSILON = 1e-5
MASK_BIG = 1e9
BF = jnp.bfloat16
F32 = jnp.float32
ROWS_A, ROWS_P = 2048, 544
LANES = 128


def nn(a, b):
    return lax.dot_general(a, b, (((1,), (0,)), ((), ())), preferred_element_type=F32)


def nt(a, b):
    return lax.dot_general(a, b, (((1,), (1,)), ((), ())), preferred_element_type=F32)


def tn(a, b):
    return lax.dot_general(a, b, (((0,), (0,)), ((), ())), preferred_element_type=F32)


def sigmoid(x):
    return 0.5 * jnp.tanh(0.5 * x) + 0.5


def layer_norm(vals):
    centred = vals - jnp.mean(vals, axis=-1, keepdims=True)
    inv = lax.rsqrt(jnp.mean(centred * centred, axis=-1, keepdims=True) + EPSILON)
    return centred * inv, inv


def norm_grad(normed, inv, grad):
    mean_grad = jnp.mean(grad, axis=-1, keepdims=True)
    mean_proj = jnp.mean(grad * normed, axis=-1, keepdims=True)
    return inv * (grad - mean_grad - normed * mean_proj)


def swiglu_grad(ha, hb, dh):
    sig = sigmoid(ha)
    silu = ha * sig
    hidden = silu * hb
    grad_a = dh * hb * (sig * (1.0 + (ha - silu)))
    return hidden.astype(BF), grad_a.astype(BF), (dh * silu).astype(BF)


AXES = ("x", "y", "z")
ORDER = (("x", "y", "z"), ("y", "z", "x"), ("z", "x", "y"))
ORDER_XY = (("x", "y"), ("y", "x"), ("x", "y"))


def remote(place, src, dst, send_sem, recv_sem, axis):
    return pltpu.make_async_remote_copy(
        src_ref=src, dst_ref=dst, send_sem=send_sem, recv_sem=recv_sem,
        device_id=place["peers"][axis], device_id_type=pl.DeviceIdType.MESH)


class Reducer:
    last = 8

    def __init__(self, place, rows, grads, recvs, final, send_sem, recv_sem):
        self.place, self.rows, self.grads, self.recvs, self.final = place, rows, grads, recvs, final
        self.send_sem, self.recv_sem = send_sem, recv_sem
        coords = place["coords"]
        self.base = []
        for third in range(3):
            base = [coords["core"] * (rows // 2)]
            for depth, axis in enumerate(ORDER[third]):
                base.append(base[-1] + coords[axis] * (rows >> (depth + 2)))
            self.base.append(base)

    def copy(self, stage, third):
        rows, base, order = self.rows, self.base[third], ORDER[third]
        coords = self.place["coords"]
        step = rows // 16
        if stage < 4:
            size = rows >> (stage + 1)
            axis = "core" if stage == 0 else order[stage - 1]
            low = 0 if stage == 0 else base[stage - 1]
            start = pl.multiple_of(low + (1 - coords[axis]) * size, step)
            src = self.grads.at[third, pl.ds(start, size)]
            dst = self.recvs[stage].at[third]
        else:
            size = rows >> (8 - stage)
            axis = "core" if stage == 7 else order[6 - stage]
            start = pl.multiple_of(base[7 - stage], step)
            src = self.final.at[third, pl.ds(start, size)]
            dst = src
        return remote(self.place, src, dst, self.send_sem.at[stage, third], self.recv_sem.at[stage, third], axis)

    def add(self, third, low, size, chunk, recv, dest):
        def run(k, carry):
            at = pl.ds(pl.multiple_of(low + k * chunk, chunk), chunk)
            off = pl.ds(pl.multiple_of(k * chunk, chunk), chunk)
            dest[third, at, :] = (self.grads[third, at, :].astype(F32) + recv[third, off, :].astype(F32)).astype(BF)
            return carry

        lax.fori_loop(0, size // chunk, run, 0)

    def start(self):
        for third in range(3):
            self.copy(0, third).start()

    def step(self, stage):
        with jax.named_scope(self.tag + str(stage)):
            self.step_(stage)

    def step_(self, stage):
        for third in range(3):
            done = stage - 1
            self.copy(done, third).wait()
            if done < 4:
                self.add(third, self.base[third][done], self.rows >> (done + 1), self.rows // 16, self.recvs[done],
                         self.final if done == 3 else self.grads)
            if stage < self.last:
                self.copy(stage, third).start()


class Doubler(Reducer):
    last = 5

    def copy(self, stage, third):
        half = self.rows // 2
        core = self.place["coords"]["core"]
        mine = pl.ds(pl.multiple_of(core * half, 16), half)
        if stage == 0:
            src = self.grads.at[third, pl.ds(pl.multiple_of((1 - core) * half, 16), half)]
            dst, axis = self.recvs[0].at[third], "core"
        elif stage < 4:
            src, dst, axis = self.grads.at[third, mine], self.recvs[stage].at[third], ORDER[third][stage - 1]
        else:
            src, dst, axis = self.final.at[third, mine], self.final.at[third, mine], "core"
        return remote(self.place, src, dst, self.send_sem.at[stage, third], self.recv_sem.at[stage, third], axis)

    def step(self, stage):
        with jax.named_scope(self.tag + str(stage)):
            self.step_(stage)

    def step_(self, stage):
        half = self.rows // 2
        for third in range(3):
            done = stage - 1
            self.copy(done, third).wait()
            if done < 4:
                self.add(third, self.base[third][0], half, half, self.recvs[done], self.final if done == 3 else self.grads)
            if stage < self.last:
                self.copy(stage, third).start()


class Gatherer:
    def __init__(self, place, buf, send_sem, recv_sem):
        self.place, self.buf, self.send_sem, self.recv_sem = place, buf, send_sem, recv_sem

    def copy(self, stage, third):
        coords, order = self.place["coords"], ORDER[third]
        got = order[:stage - 1]
        index = [third, coords["core"]] + [slice(None) if axis in got else coords[axis] for axis in AXES]
        ref = self.buf.at[tuple(index)]
        axis = order[stage - 1] if stage < 4 else "core"
        return remote(self.place, ref, ref, self.send_sem.at[stage, third], self.recv_sem.at[stage, third], axis)

    def step(self, stage):
        with jax.named_scope(self.tag + str(stage)):
            self.step_(stage)

    def step_(self, stage):
        for third in range(3):
            if stage > 1:
                self.copy(stage - 1, third).wait()
            if stage < 5:
                self.copy(stage, third).start()


class Tiles:
    def __init__(self, place, buf0, buf1, send_sem, recv_sem):
        self.place, self.bufs, self.send_sem, self.recv_sem = place, (buf0, buf1), send_sem, recv_sem

    def copy(self, core, stage, third):
        coords = self.place["coords"]
        order = ORDER[third] if core == 0 else ORDER_XY[third]
        axes = AXES if core == 0 else AXES[:2]
        if stage > len(order):
            ref, axis, slot = self.bufs[core].at[third], "core", 4 + core
        else:
            got = order[:stage - 1]
            ref = self.bufs[core].at[tuple([third] + [slice(None) if axis in got else coords[axis] for axis in axes])]
            axis, slot = order[stage - 1], stage
        return remote(self.place, ref, ref, self.send_sem.at[slot, third], self.recv_sem.at[slot, third], axis)

    def step(self, stage):
        with jax.named_scope(self.tag + str(stage)):
            self.step_(stage)

    def step_(self, stage):
        for core in range(2):
            last = 4 - core

            @pl.when(self.place["coords"]["core"] == core)
            def _():
                for third in range(3):
                    if 1 < stage <= last:
                        self.copy(core, stage - 1, third).wait()
                    if stage <= last:
                        self.copy(core, stage, third).start()
                    if stage == 5:
                        self.copy(core, last, third).wait_send()
                        self.copy(1 - core, 3 + core, third).wait_recv()


def body_kernel(
        z_hbm, dz_hbm, wpa_hbm, wpb_hbm, wpo_hbm, wq_hbm, wkv_hbm, wg_hbm, wo_hbm, wsa_hbm, wsb_hbm, wso_hbm,
        s_ref, ds_ref, mask_ref, qb_ref, wbias_ref,
        dzin_hbm, dsin_hbm, fs0_hbm, fs1_hbm, fa_hbm, fp_hbm,
        z_v, dz_v, wpa, wpb, wpo, wq, wkv, wg, wo, wsa, wsb, wso,
        z1_v, w8, bias_v, prob_v, act_v, q_v, gate_v, att_v, gated_v, gatt_v, gmid_v, gact_v, kv_v, gkv_v, gkvr_v,
        dwpa, dwpb, dwpo, m8, dsin_ref, c_all, ds_all, d_ab, d_so, gnew_v, gab_v,
        u0, u1, ut0, ut1, gn0, gn1, gnt0, gnt1, fs0, fs1, fa_ref, fp_ref,
        ga_, ga0, ga1, ga2, ga3, gp, gp0, gp1, gp2, gp3,
        in_sem, out_sem, dz_sem, kv_sem, send_sem, recv_sem):
    dap = lax.axis_index("dap")
    dp = lax.axis_index("dp")
    core = lax.rem(dp, 2)
    cx = lax.rem(dp // 2, 2)
    cy = dp // 4
    peers = {
        "core": (dap, dp + 1 - 2 * core),
        "x": (dap, dp + 2 - 4 * cx),
        "y": (dap, dp + 4 - 8 * cy),
        "z": (1 - dap, dp),
    }
    place = {"coords": {"core": core, "x": cx, "y": cy, "z": dap}, "peers": peers}
    num_cplx, num_tok = mask_ref.shape
    half = num_tok // 2
    width = HEADS * HEAD_DIM

    loads = [(wkv_hbm, wkv), (wq_hbm, wq), (wg_hbm, wg), (wpa_hbm, wpa), (wpb_hbm, wpb), (wpo_hbm, wpo), (z_hbm, z_v),
             (wo_hbm, wo), (wsa_hbm, wsa), (wsb_hbm, wsb), (wso_hbm, wso), (dz_hbm, dz_v)]
    copies = [pltpu.make_async_copy(src, dst, in_sem.at[k]) for k, (src, dst) in enumerate(loads)]
    for item in copies:
        item.start()

    barrier = pltpu.get_barrier_semaphore()
    for peer in peers.values():
        pl.semaphore_signal(barrier, inc=1, device_id=peer, device_id_type=pl.DeviceIdType.MESH)

    red_a = Reducer(place, ROWS_A, ga_, (ga0, ga1, ga2, ga3), fa_ref, send_sem.at[0], recv_sem.at[0])
    red_a.tag = 'A'
    red_p = Doubler(place, ROWS_P, gp, (gp0, gp1, gp2, gp3), fp_ref, send_sem.at[1], recv_sem.at[1])
    red_p.tag = 'P'
    gat_ds = Gatherer(place, ds_all, send_sem.at[2], recv_sem.at[2])
    gat_ds.tag = 'D'
    gat_c = Gatherer(place, c_all, send_sem.at[3], recv_sem.at[3])
    gat_c.tag = 'C'
    tiles = Tiles(place, fs0, fs1, send_sem.at[4], recv_sem.at[4])
    tiles.tag = 'T'

    def own_block(buf, value):
        for t in range(3):
            buf[t, core, cx, cy, dap] = value[:, t * LANES:(t + 1) * LANES]

    own_block(ds_all, ds_ref[...])

    s_f = s_ref[...].astype(F32)
    s_norm, s_inv = layer_norm(s_f)
    act = s_norm.astype(BF)
    act_v[...] = act
    copies[0].wait()
    kv_v[dap, :, 0:2 * width] = nn(act, wkv[...]).astype(BF)
    kv_v[dap, :, 2 * width:3 * width] = act

    def kv_copy():
        return pltpu.make_async_remote_copy(
            src_ref=kv_v.at[dap], dst_ref=kv_v.at[dap], send_sem=kv_sem.at[0], recv_sem=kv_sem.at[1],
            device_id=peers["z"], device_id_type=pl.DeviceIdType.MESH)

    def gkv_copy():
        return pltpu.make_async_remote_copy(
            src_ref=gkv_v.at[1 - dap], dst_ref=gkvr_v, send_sem=kv_sem.at[2], recv_sem=kv_sem.at[3],
            device_id=peers["z"], device_id_type=pl.DeviceIdType.MESH)

    with jax.named_scope('barrier'):
        pl.semaphore_wait(barrier, 4)
    kv_copy().start()
    gat_ds.step(1)
    copies[1].wait()
    copies[2].wait()
    q_v[...] = (nn(act, wq[...]) + qb_ref[...].astype(F32).reshape(1, width)).astype(BF)
    gate_v[...] = sigmoid(nn(act, wg[...]))

    row_head = lax.broadcasted_iota(jnp.int32, (128, HEADS), 0)
    col_head = lax.broadcasted_iota(jnp.int32, (128, HEADS), 1)
    pick = jnp.where((row_head >= col_head * 8) & (row_head < col_head * 8 + 8), 1.0, 0.0).astype(BF)
    spread = nn(pick, wbias_ref[...])
    row8 = lax.rem(lax.broadcasted_iota(jnp.int32, (128, LANES), 0), 8)
    for k in range(8):
        w8[:, k * LANES:(k + 1) * LANES] = jnp.where(row8 == k, spread, 0.0).astype(BF)

    for k in range(3, 7):
        copies[k].wait()

    blk = 8 * num_tok
    per_cplx = half // 8
    num_blk = num_cplx * per_cplx

    def side_by_side(tokens):
        return jnp.concatenate([tokens[k * num_tok:(k + 1) * num_tok] for k in range(8)], axis=1)

    def rows_at(b):
        return pl.ds(pl.multiple_of(b * blk, blk), blk)

    def bias_at(b):
        return b // per_cplx, pl.ds(pl.multiple_of(lax.rem(b, per_cplx) * 8, 8), 8)

    def forward_norm(b, u_ref):
        normed, _ = layer_norm(z_v[rows_at(b), :].astype(F32))
        u_ref[...] = normed.astype(BF)

    def forward_main(b, u_ref):
        total = z_v[rows_at(b), :].astype(F32)
        for f in range(0, 512, 256):
            u = u_ref[...]
            ha = nn(u, wpa[:, f:f + 256])
            hb = nn(u, wpb[:, f:f + 256])
            hidden = (ha * sigmoid(ha) * hb).astype(BF)
            total = total + nn(hidden, wpo[f:f + 256, :])
        z1_v[rows_at(b), :] = total.astype(BF)

    def forward_bias(b):
        bias_norm, _ = layer_norm(z1_v[rows_at(b), :].astype(F32))
        c, at = bias_at(b)
        bias_v[c, :, at, :] = nt(w8[...], side_by_side(bias_norm.astype(BF))).reshape(HEADS, 8, num_tok)

    def forward_pair(p, carry):
        forward_bias(2 * p)
        forward_norm(2 * p + 2, u0)
        forward_main(2 * p + 1, u1)
        forward_bias(2 * p + 1)
        forward_norm(2 * p + 3, u1)
        forward_main(2 * p + 2, u0)
        for when, stage in ((1, 2), (4, 3)):
            @pl.when(p == when)
            def _():
                gat_ds.step(stage)
        return carry

    forward_norm(0, u0)
    forward_norm(1, u1)
    forward_main(0, u0)
    with jax.named_scope('fwdloop'):
        lax.fori_loop(0, num_blk // 2 - 1, forward_pair, 0)
    forward_bias(num_blk - 2)
    forward_main(num_blk - 1, u1)
    forward_bias(num_blk - 1)

    scale = HEAD_DIM ** -0.5
    grow = lax.broadcasted_iota(jnp.int32, (HEADS, 1, width), 0) * HEAD_DIM
    gcol = lax.broadcasted_iota(jnp.int32, (HEADS, 1, width), 2)
    head_mask = (gcol >= grow) & (gcol < grow + HEAD_DIM)

    def expand(rows):
        wide = jnp.where(head_mask, rows.astype(F32)[None], 0.0)
        return wide.reshape(HEADS * half, width).astype(BF)

    def gather_heads(wide):
        return jnp.sum(jnp.where(head_mask, wide.reshape(HEADS, half, width), 0.0), axis=0)

    def tokens_of(c, lo):
        rows = slice(c * half, (c + 1) * half)
        return jnp.concatenate([kv_v[0, rows, lo:lo + width], kv_v[1, rows, lo:lo + width]], axis=0)

    kv_copy().wait()
    for c in range(num_cplx):
        rows = slice(c * half, (c + 1) * half)
        key_mask = MASK_BIG * (mask_ref[c:c + 1, :].astype(F32) - 1.0)
        logits = nt(expand(q_v[rows, :]), tokens_of(c, 0)) * scale + bias_v[c].reshape(HEADS * half, num_tok) + key_mask
        ex = jnp.exp(logits - jnp.max(logits, axis=-1, keepdims=True))
        prob = ex / jnp.sum(ex, axis=-1, keepdims=True)
        prob_v[c] = prob
        att_v[rows, :] = gather_heads(nn(prob.astype(BF), tokens_of(c, width)))
    gated = (gate_v[...] * att_v[...]).astype(BF)
    gated_v[...] = gated
    copies[7].wait()
    s_mid = (s_ref[...].astype(F32) + nn(gated, wo[...])).astype(BF)
    mid_norm, mid_inv = layer_norm(s_mid.astype(F32))
    mid_act = mid_norm.astype(BF)
    own_block(c_all, mid_act)
    gat_c.step(1)

    for k in range(8, 11):
        copies[k].wait()
    ds_b = ds_ref[...]
    grad_mid_norm = None
    for t in range(3):
        cols = slice(t * 512, (t + 1) * 512)
        ta = nn(mid_act, wsa[:, cols])
        tb = nn(mid_act, wsb[:, cols])
        dh = nt(ds_b, wso[cols, :])
        _, grad_a, grad_b = swiglu_grad(ta, tb, dh)
        part = nt(grad_a, wsa[:, cols]) + nt(grad_b, wsb[:, cols])
        grad_mid_norm = part if grad_mid_norm is None else grad_mid_norm + part
    grad_mid = ds_b.astype(F32) + norm_grad(mid_norm, mid_inv, grad_mid_norm)
    gmid_v[...] = grad_mid
    grad_mid_bf = grad_mid.astype(BF)
    grad_gated = nt(grad_mid_bf, wo[...])
    gate = gate_v[...]
    gatt_v[...] = (grad_gated * gate).astype(BF)
    grad_gate_pre = (grad_gated * att_v[...] * gate * (1.0 - gate)).astype(BF)

    def put_attn(buf, name_row, value):
        val = value.astype(BF)
        per = val.shape[1] // width
        for k in range(val.shape[1] // LANES):
            lo = name_row + (k % per) * 384
            buf[k // per, lo:lo + 384, :] = val[:, k * LANES:(k + 1) * LANES]

    act_t = act_v[...].T
    put_attn(ga_, 1152, nn(act_t, grad_gate_pre))
    put_attn(ga_, 1536, tn(gated_v[...], grad_mid_bf))
    gat_c.step(2)
    gat_ds.step(4)

    grad_q_parts = []
    for c in range(num_cplx):
        rows = slice(c * half, (c + 1) * half)
        keys, vals = tokens_of(c, 0), tokens_of(c, width)
        gatt = expand(gatt_v[rows, :])
        prob = prob_v[c]
        grad_prob = nt(gatt, vals)
        grad_vals = tn(prob.astype(BF), gatt)
        grad_logits = prob * (grad_prob - jnp.sum(prob * grad_prob, axis=-1, keepdims=True))
        bias_v[c] = grad_logits.reshape(HEADS, half, num_tok)
        gl_b = grad_logits.astype(BF)
        grad_q_parts.append(gather_heads(nn(gl_b, keys)) * scale)
        grad_keys = tn(gl_b, expand(q_v[rows, :])) * scale
        for d in range(2):
            gkv_v[d, rows, 0:width] = grad_keys[d * half:(d + 1) * half].astype(BF)
            gkv_v[d, rows, width:2 * width] = grad_vals[d * half:(d + 1) * half].astype(BF)
    grad_q = jnp.concatenate(grad_q_parts, axis=0)
    grad_q_bf = grad_q.astype(BF)
    put_attn(ga_, 0, nn(act_t, grad_q_bf))
    row16 = lax.broadcasted_iota(jnp.int32, (16, width), 0)
    bias_tile = jnp.where(row16 == 0, jnp.sum(grad_q, axis=0, keepdims=True), 0.0).astype(BF)
    for t in range(3):
        ga_[t, 1920:1936, :] = bias_tile[:, t * LANES:(t + 1) * LANES]
        ga_[t, 1936:2048, :] = jnp.zeros((112, LANES), BF)
    act_both = kv_v[:, :, 2 * width:3 * width].reshape(2 * s_ref.shape[0], width)
    put_attn(ga_, 384, tn(act_both, gkv_v[...].reshape(2 * s_ref.shape[0], 2 * width)))
    red_a.start()
    gact_v[...] = nt(grad_q_bf, wq[...]) + nt(grad_gate_pre, wg[...])

    def finish_attention():
        with jax.named_scope('gkvwait'):
            gkv_copy().wait()
        grad_kv = (gkv_v[dap].astype(F32) + gkvr_v[...].astype(F32)).astype(BF)
        grad_act = gact_v[...] + nt(grad_kv, wkv[...])
        s_norm2, s_inv2 = layer_norm(s_ref[...].astype(F32))
        dsin_ref[...] = (gmid_v[...] + norm_grad(s_norm2, s_inv2, grad_act)).astype(BF)
        out_copies[0].start()

    outs = [(dsin_ref, dsin_hbm), (fs0, fs0_hbm), (fs1, fs1_hbm), (fa_ref, fa_hbm), (fp_ref, fp_hbm)]
    out_copies = [pltpu.make_async_copy(src, dst, out_sem.at[k]) for k, (src, dst) in enumerate(outs)]

    def tile_grads():
        tile = jnp.where(core == 0, 3 * (2 * cx + cy) + 2 * dap, 3 * (2 * cx + cy) + 1)
        at = pl.ds(pl.multiple_of(tile * LANES, LANES), LANES)
        w_ab = jnp.concatenate([wsa[:, at], wsb[:, at]], axis=1)
        w_o_tile = wso[at, :]
        d_ab[...] = jnp.zeros(d_ab.shape, F32)
        d_so[...] = jnp.zeros(d_so.shape, F32)

        def quarter(k, carry):
            def rows_of(buf):
                return jnp.concatenate([buf[t, k // 2, lax.rem(k, 2)].reshape(4 * 96, LANES) for t in range(3)], axis=1)

            acts, cots = rows_of(c_all), rows_of(ds_all)
            both = nn(acts, w_ab)
            hidden, grad_a, grad_b = swiglu_grad(both[:, :LANES], both[:, LANES:], nt(cots, w_o_tile))
            d_ab[...] += tn(acts, jnp.concatenate([grad_a, grad_b], axis=1))
            d_so[...] += tn(hidden, cots)
            return carry

        with jax.named_scope('TP'):
            lax.fori_loop(0, 4, quarter, 0)
        for k in range(2):
            @pl.when(core == k)
            def _():
                slot = (cx, cy, dap) if k == 0 else (cx, cy)
                buf = fs0 if k == 0 else fs1
                buf[(0,) + slot] = d_ab[:, :LANES].astype(BF)
                buf[(1,) + slot] = d_ab[:, LANES:].astype(BF)
                so_b = d_so[...].astype(BF)
                buf[(2,) + slot] = jnp.concatenate([so_b[:, t * LANES:(t + 1) * LANES] for t in range(3)], axis=0)

    copies[11].wait()
    for ref in (dwpa, dwpb, dwpo, m8):
        ref[...] = jnp.zeros(ref.shape, F32)

    def hook(*calls):
        def run():
            for call in calls:
                call()
        return run

    def dz_copy(k):
        at = pl.ds(pl.multiple_of(k * blk, blk), blk)
        return pltpu.make_async_copy(dz_v.at[at, :], dzin_hbm.at[at, :], dz_sem.at[k])

    hooks = {
        0: hook(lambda: gat_c.step(3)),
        1: hook(lambda: red_a.step(1)),
        3: hook(lambda: gat_c.step(4)),
        4: hook(lambda: gat_c.step(5), lambda: gat_ds.step(5), tile_grads, lambda: tiles.step(1)),
        5: hook(lambda: red_a.step(2)),
        8: hook(lambda: red_a.step(3), lambda: tiles.step(2)),
        9: hook(lambda: gkv_copy().start()),
        11: hook(lambda: red_a.step(4)),
    }
    tail_hooks = {
        2: hook(lambda: red_p.step(1)),
        3: hook(lambda: tiles.step(3)),
        4: hook(lambda: red_a.step(5)),
        8: hook(finish_attention),
        10: hook(lambda: red_p.step(2)),
        11: hook(lambda: red_a.step(6)),
    }

    def run_hooks(table, k):
        for when, todo in table.items():
            pl.when(k == when)(todo)

    def backward_head(b, live, bufs):
        u_ref, ut_ref, gn_ref, gnt_ref = bufs
        at = rows_at(b)
        c, rows = bias_at(b)
        gl_f = bias_v[c, :, rows, :].reshape(8 * HEADS, num_tok)
        wide = tn(gl_f.astype(BF), w8[...])
        grad_norm = jnp.concatenate([wide[:, k * LANES:(k + 1) * LANES] for k in range(8)], axis=0)
        bias_norm, bias_inv = layer_norm(z1_v[at, :].astype(F32))
        m8[...] += nn((gl_f * live).astype(BF), side_by_side(bias_norm.astype(BF)))
        grad_new = dz_v[at, :].astype(F32) + norm_grad(bias_norm, bias_inv, grad_norm)
        gnew_v[at, :] = grad_new
        gnb = grad_new.astype(BF)
        gn_ref[...] = gnb
        gnt_ref[...] = gnb.T
        normed, _ = layer_norm(z_v[at, :].astype(F32))
        u = normed.astype(BF)
        u_ref[...] = u
        ut_ref[...] = u.T

    def backward_main(b, bufs):
        u_ref, ut_ref, gn_ref, gnt_ref = bufs
        at = rows_at(b)
        for f in range(0, 512, 256):
            cols = slice(f, f + 256)
            u, gnb = u_ref[...], gn_ref[...]
            hidden, grad_a, grad_b = swiglu_grad(nn(u, wpa[:, cols]), nn(u, wpb[:, cols]), nt(gnb, wpo[cols, :]))
            gab_v[at, cols] = grad_a
            gab_v[at, 512 + f:768 + f] = grad_b
            dwpo[:, cols] += nn(gnt_ref[...], hidden)
            dwpa[:, cols] += nn(ut_ref[...], grad_a)
            dwpb[:, cols] += nn(ut_ref[...], grad_b)

    def backward_tail(b, carry):
        at = rows_at(b)
        grad_normed = nt(gab_v[at, :], jnp.concatenate([wpa[...], wpb[...]], axis=1))
        normed, inv = layer_norm(z_v[at, :].astype(F32))
        dz_v[at, :] = (gnew_v[at, :] + norm_grad(normed, inv, grad_normed)).astype(BF)
        dz_copy(b).start()
        run_hooks(tail_hooks, b)
        return carry

    bufs0, bufs1 = (u0, ut0, gn0, gnt0), (u1, ut1, gn1, gnt1)

    def backward_pair(p, carry):
        backward_head(2 * p + 1, 1.0, bufs1)
        backward_main(2 * p, bufs0)
        run_hooks({k // 2: v for k, v in hooks.items() if k % 2 == 0}, p)
        more = jnp.where(p < num_blk // 2 - 1, 1.0, 0.0)
        backward_head(jnp.minimum(2 * p + 2, num_blk - 1), more, bufs0)
        backward_main(2 * p + 1, bufs1)
        run_hooks({k // 2: v for k, v in hooks.items() if k % 2}, p)
        return carry

    backward_head(0, 1.0, bufs0)
    with jax.named_scope('bwdloop'):
        lax.fori_loop(0, num_blk // 2, backward_pair, 0)

    for t, ref in enumerate((dwpa, dwpb, dwpo)):
        for k in range(4):
            gp[t, k * 128:(k + 1) * 128, :] = ref[:, k * LANES:(k + 1) * LANES].astype(BF)
        gp[t, 528:544, :] = jnp.zeros((16, LANES), BF)
    diag = jnp.zeros((128, LANES), F32)
    for k in range(8):
        diag = diag + jnp.where(row8 == k, m8[:, k * LANES:(k + 1) * LANES], 0.0)
    gp[0, 512:528, :] = jnp.sum(diag.reshape(HEADS, 8, LANES), axis=1).astype(BF)
    for t in range(1, 3):
        gp[t, 512:528, :] = jnp.zeros((16, LANES), BF)
    red_p.start()
    with jax.named_scope('tailloop'):
        lax.fori_loop(0, num_blk, backward_tail, 0)
    red_p.step(3)
    tiles.step(4)
    red_a.step(7)
    red_p.step(4)
    red_a.step(8)
    out_copies[3].start()
    tiles.step(5)
    out_copies[1].start()
    out_copies[2].start()
    red_p.step(5)
    out_copies[4].start()

    def drain(k, carry):
        dz_copy(k).wait()
        return carry

    with jax.named_scope('drain'):
        lax.fori_loop(0, num_blk, drain, 0)
    for item in out_copies:
        item.wait()


def unpack_kernel(dz_i, ds_i, fs0_i, fs1_i, fa_i, fp_i,
                  dz_o, ds_o, pa_o, pb_o, po_o, bias_o, q_o, qb_o, kv_o, g_o, o_o, sa_o, sb_o, so_o,
                  dz, ds, fs0, fs1, fa, fp, pa, pb, po, bias, q, qb, kv, g, o, sa, sb, so, in_sem, sem):
    ins = [(fs0_i, fs0), (fs1_i, fs1), (fa_i, fa), (fp_i, fp), (dz_i, dz), (ds_i, ds)]
    reads = [pltpu.make_async_copy(src, dst, in_sem.at[k]) for k, (src, dst) in enumerate(ins)]
    for item in reads:
        item.start()
    outs = [(sa, sa_o), (sb, sb_o), (so, so_o), (q, q_o), (kv, kv_o), (g, g_o), (o, o_o), (qb, qb_o), (pa, pa_o), (pb, pb_o),
            (po, po_o), (bias, bias_o), (dz, dz_o), (ds, ds_o)]
    copies = [pltpu.make_async_copy(src, dst, sem.at[k]) for k, (src, dst) in enumerate(outs)]

    reads[0].wait()
    reads[1].wait()
    for kind in range(3):
        for pair in range(4):
            cx, cy = pair // 2, pair % 2
            for j in range(3):
                lo = (3 * pair + j) * LANES
                tile = fs1[kind, cx, cy] if j == 1 else fs0[kind, cx, cy, j // 2]
                wide = tile.astype(F32)
                if kind < 2:
                    (sa, sb)[kind][:, lo:lo + LANES] = wide
                else:
                    for k in range(3):
                        so[lo:lo + LANES, k * LANES:(k + 1) * LANES] = wide[k * LANES:(k + 1) * LANES]
        copies[kind].start()
    reads[2].wait()
    for index, (ref, buf, row) in enumerate(((q, fa, 0), (kv, fa, 384), (g, fa, 1152), (o, fa, 1536))):
        per = ref.shape[1] // 384
        for k in range(3 * per):
            lo = row + (k % per) * 384
            ref[:, k * LANES:(k + 1) * LANES] = buf[k // per, lo:lo + 384, :].astype(F32)
        copies[3 + index].start()
    for t in range(3):
        qb[t * LANES:(t + 1) * LANES] = fa[t, 1920:1936, :].astype(F32)[0]
    copies[7].start()
    reads[3].wait()
    for t, ref in enumerate((pa, pb)):
        for k in range(4):
            ref[:, k * LANES:(k + 1) * LANES] = fp[t, k * 128:(k + 1) * 128, :].astype(F32)
        copies[8 + t].start()
    for k in range(4):
        po[k * 128:(k + 1) * 128, :] = fp[2, k * 128:(k + 1) * 128, :].astype(F32).T
    copies[10].start()
    bias[...] = fp[0, 512:528, :].astype(F32)
    copies[11].start()
    for k in range(2):
        reads[4 + k].wait()
        copies[12 + k].start()
    for item in copies:
        item.wait()


def solution(mesh):
    pair_spec = P('dp', 'dap', None, None)
    single_spec = P('dp', 'dap', None)
    hbm = pl.BlockSpec(memory_space=pl.ANY)
    vmem = pl.BlockSpec(memory_space=pltpu.VMEM)

    def body(pair_z, single_s, token_mask, dz_out, ds_out, w_pa, w_pb, w_po, w_bias, w_q, q_bias, w_kv, w_g, w_o, w_sa, w_sb, w_so):
        num_cplx, half, num_tok, dim = pair_z.shape
        toks = num_cplx * half * num_tok
        rows = num_cplx * half
        width = w_q.shape[1]
        big = (pair_z.reshape(toks, dim), dz_out.reshape(toks, dim), w_pa, w_pb, w_po, w_q, w_kv, w_g, w_o, w_sa, w_sb, w_so)
        small = (single_s.reshape(rows, width), ds_out.reshape(rows, width), token_mask, q_bias, w_bias.T)
        scratch = [pltpu.VMEM(a.shape, a.dtype) for a in big]
        finals = [(toks, dim), (rows, width), (3, 2, 2, 2, width, LANES), (3, 2, 2, width, LANES), (3, ROWS_A, LANES), (3, ROWS_P, LANES)]
        scratch += [
            pltpu.VMEM((toks, dim), BF), pltpu.VMEM((128, 1024), BF),
            pltpu.VMEM((num_cplx, HEADS, half, num_tok), F32), pltpu.VMEM((num_cplx, HEADS * half, num_tok), F32),
            pltpu.VMEM((rows, width), BF), pltpu.VMEM((rows, width), BF), pltpu.VMEM((rows, width), F32),
            pltpu.VMEM((rows, width), F32), pltpu.VMEM((rows, width), BF), pltpu.VMEM((rows, width), BF),
            pltpu.VMEM((rows, width), F32), pltpu.VMEM((rows, width), F32),
            pltpu.VMEM((2, rows, 3 * width), BF), pltpu.VMEM((2, rows, 2 * width), BF), pltpu.VMEM((rows, 2 * width), BF),
            pltpu.VMEM((128, 512), F32), pltpu.VMEM((128, 512), F32), pltpu.VMEM((128, 512), F32), pltpu.VMEM((128, 1024), F32),
            pltpu.VMEM(finals[1], BF),
            pltpu.VMEM((3, 2, 2, 2, 2, rows, LANES), BF), pltpu.VMEM((3, 2, 2, 2, 2, rows, LANES), BF),
            pltpu.VMEM((width, 2 * LANES), F32), pltpu.VMEM((LANES, width), F32),
            pltpu.VMEM((toks, dim), F32), pltpu.VMEM((toks, 1024), BF),
        ]
        for _ in range(2):
            scratch += [pltpu.VMEM((512, dim), BF)] * 2 + [pltpu.VMEM((dim, 512), BF)] * 2
        scratch += [pltpu.VMEM(shape, BF) for shape in finals[2:]]
        scratch += [pltpu.VMEM((3, ROWS_A >> k, LANES), BF) for k in range(5)]
        scratch += [pltpu.VMEM((3, ROWS_P, LANES), BF)] + [pltpu.VMEM((3, ROWS_P // 2, LANES), BF) for _ in range(4)]
        scratch += [pltpu.SemaphoreType.DMA((12,)), pltpu.SemaphoreType.DMA((5,)), pltpu.SemaphoreType.DMA((toks // (8 * num_tok),)),
                    pltpu.SemaphoreType.DMA((4,)), pltpu.SemaphoreType.DMA((5, 8, 3)), pltpu.SemaphoreType.DMA((5, 8, 3))]
        packed = pl.pallas_call(
            body_kernel,
            out_shape=[jax.ShapeDtypeStruct(shape, BF) for shape in finals],
            in_specs=[hbm] * 12 + [vmem] * 5,
            out_specs=[hbm] * 6,
            scratch_shapes=scratch,
            compiler_params=pltpu.CompilerParams(collective_id=0, has_side_effects=True, vmem_limit_bytes=60 * 2 ** 20),
            name="block",
        )(*big, *small)
        shapes = [w_pa.shape, w_pb.shape, w_po.shape, (HEADS, dim), w_q.shape, (width,), w_kv.shape, w_g.shape, w_o.shape,
                  w_sa.shape, w_sb.shape, w_so.shape]
        done = pl.pallas_call(
            unpack_kernel,
            out_shape=[jax.ShapeDtypeStruct(shape, BF) for shape in finals[:2]] + [jax.ShapeDtypeStruct(shape, F32) for shape in shapes],
            in_specs=[hbm] * 6,
            out_specs=[hbm] * 14,
            scratch_shapes=[pltpu.VMEM(shape, BF) for shape in finals] + [pltpu.VMEM(shape, F32) for shape in shapes] + [
                pltpu.SemaphoreType.DMA((6,)), pltpu.SemaphoreType.DMA((14,))],
            compiler_params=pltpu.CompilerParams(vmem_limit_bytes=56 * 2 ** 20),
            name="unpack",
        )(*packed)
        grads = list(done[2:])
        grads[3] = grads[3].T
        return (done[0].reshape(pair_z.shape), done[1].reshape(single_s.shape)) + tuple(grads)

    in_specs = (pair_spec, single_spec, P('dp', None), pair_spec, single_spec) + (P(),) * 12
    out_specs = (pair_spec, single_spec) + (P(),) * 12
    return jax.shard_map(body, mesh=mesh, in_specs=in_specs, out_specs=out_specs, check_vma=False)
```

```python
import jax
import jax.numpy as jnp
from jax import lax
from jax.experimental import pallas as pl
from jax.experimental.pallas import tpu as pltpu
from jax.sharding import PartitionSpec as P

HEADS = 16
HEAD_DIM = 24
EPSILON = 1e-5
MASK_BIG = 1e9
BF = jnp.bfloat16
F32 = jnp.float32
ROWS_A, ROWS_P = 2048, 544
LANES = 128


def nn(a, b):
    return lax.dot_general(a, b, (((1,), (0,)), ((), ())), preferred_element_type=F32)


def nt(a, b):
    return lax.dot_general(a, b, (((1,), (1,)), ((), ())), preferred_element_type=F32)


def tn(a, b):
    return lax.dot_general(a, b, (((0,), (0,)), ((), ())), preferred_element_type=F32)


def sigmoid(x):
    return 0.5 * jnp.tanh(0.5 * x) + 0.5


def layer_norm(vals):
    centred = vals - jnp.mean(vals, axis=-1, keepdims=True)
    inv = lax.rsqrt(jnp.mean(centred * centred, axis=-1, keepdims=True) + EPSILON)
    return centred * inv, inv


def norm_grad(normed, inv, grad):
    mean_grad = jnp.mean(grad, axis=-1, keepdims=True)
    mean_proj = jnp.mean(grad * normed, axis=-1, keepdims=True)
    return inv * (grad - mean_grad - normed * mean_proj)


def swiglu_grad(ha, hb, dh):
    sig = sigmoid(ha)
    silu = ha * sig
    hidden = silu * hb
    grad_a = dh * hb * (sig * (1.0 + (ha - silu)))
    return hidden.astype(BF), grad_a.astype(BF), (dh * silu).astype(BF)


AXES = ("x", "y", "z")
ORDER = (("x", "y", "z"), ("y", "z", "x"), ("z", "x", "y"))
ORDER_XY = (("x", "y"), ("y", "x"), ("x", "y"))


def remote(place, src, dst, send_sem, recv_sem, axis):
    return pltpu.make_async_remote_copy(
        src_ref=src, dst_ref=dst, send_sem=send_sem, recv_sem=recv_sem,
        device_id=place["peers"][axis], device_id_type=pl.DeviceIdType.MESH)


class Reducer:
    last = 8

    def __init__(self, place, rows, grads, recvs, final, send_sem, recv_sem):
        self.place, self.rows, self.grads, self.recvs, self.final = place, rows, grads, recvs, final
        self.send_sem, self.recv_sem = send_sem, recv_sem
        coords = place["coords"]
        self.base = []
        for third in range(3):
            base = [coords["core"] * (rows // 2)]
            for depth, axis in enumerate(ORDER[third]):
                base.append(base[-1] + coords[axis] * (rows >> (depth + 2)))
            self.base.append(base)

    def copy(self, stage, third):
        rows, base, order = self.rows, self.base[third], ORDER[third]
        coords = self.place["coords"]
        step = rows // 16
        if stage < 4:
            size = rows >> (stage + 1)
            axis = "core" if stage == 0 else order[stage - 1]
            low = 0 if stage == 0 else base[stage - 1]
            start = pl.multiple_of(low + (1 - coords[axis]) * size, step)
            src = self.grads.at[third, pl.ds(start, size)]
            dst = self.recvs[stage].at[third]
        else:
            size = rows >> (8 - stage)
            axis = "core" if stage == 7 else order[6 - stage]
            start = pl.multiple_of(base[7 - stage], step)
            src = self.final.at[third, pl.ds(start, size)]
            dst = src
        return remote(self.place, src, dst, self.send_sem.at[third], self.recv_sem.at[stage, third], axis)

    def add(self, third, low, size, chunk, recv, dest):
        def run(k, carry):
            at = pl.ds(pl.multiple_of(low + k * chunk, chunk), chunk)
            off = pl.ds(pl.multiple_of(k * chunk, chunk), chunk)
            dest[third, at, :] = (self.grads[third, at, :].astype(F32) + recv[third, off, :].astype(F32)).astype(BF)
            return carry

        lax.fori_loop(0, size // chunk, run, 0)

    def start(self):
        for third in range(3):
            self.copy(0, third).start()

    def step(self, stage):
        with jax.named_scope(self.tag + str(stage)):
            self.step_(stage)

    def step_(self, stage):
        for third in range(3):
            done = stage - 1
            self.copy(done, third).wait()
            if done < 4:
                self.add(third, self.base[third][done], self.rows >> (done + 1), self.rows // 16, self.recvs[done],
                         self.final if done == 3 else self.grads)
            if stage < self.last:
                self.copy(stage, third).start()


class Doubler(Reducer):
    last = 5

    def copy(self, stage, third):
        half = self.rows // 2
        core = self.place["coords"]["core"]
        mine = pl.ds(pl.multiple_of(core * half, 16), half)
        if stage == 0:
            src = self.grads.at[third, pl.ds(pl.multiple_of((1 - core) * half, 16), half)]
            dst, axis = self.recvs[0].at[third], "core"
        elif stage < 4:
            src, dst, axis = self.grads.at[third, mine], self.recvs[stage].at[third], ORDER[third][stage - 1]
        else:
            src, dst, axis = self.final.at[third, mine], self.final.at[third, mine], "core"
        return remote(self.place, src, dst, self.send_sem.at[third], self.recv_sem.at[stage, third], axis)

    def step(self, stage):
        with jax.named_scope(self.tag + str(stage)):
            self.step_(stage)

    def step_(self, stage):
        half = self.rows // 2
        for third in range(3):
            done = stage - 1
            self.copy(done, third).wait()
            if done < 4:
                self.add(third, self.base[third][0], half, half, self.recvs[done], self.final if done == 3 else self.grads)
            if stage < self.last:
                self.copy(stage, third).start()


class Gatherer:
    def __init__(self, place, buf, send_sem, recv_sem):
        self.place, self.buf, self.send_sem, self.recv_sem = place, buf, send_sem, recv_sem

    def copy(self, stage, third):
        coords, order = self.place["coords"], ORDER[third]
        got = order[:stage - 1]
        index = [third, coords["core"]] + [slice(None) if axis in got else coords[axis] for axis in AXES]
        ref = self.buf.at[tuple(index)]
        axis = order[stage - 1] if stage < 4 else "core"
        return remote(self.place, ref, ref, self.send_sem.at[third], self.recv_sem.at[stage - 1, third], axis)

    def step(self, stage):
        with jax.named_scope(self.tag + str(stage)):
            self.step_(stage)

    def step_(self, stage):
        for third in range(3):
            if stage > 1:
                self.copy(stage - 1, third).wait()
            if stage < 5:
                self.copy(stage, third).start()


class Tiles:
    def __init__(self, place, buf0, buf1, send_sem, recv_sem):
        self.place, self.bufs, self.send_sem, self.recv_sem = place, (buf0, buf1), send_sem, recv_sem

    def copy(self, core, stage, third):
        coords = self.place["coords"]
        order = ORDER[third] if core == 0 else ORDER_XY[third]
        axes = AXES if core == 0 else AXES[:2]
        if stage > len(order):
            ref, axis, slot = self.bufs[core].at[third], "core", 4
        else:
            got = order[:stage - 1]
            ref = self.bufs[core].at[tuple([third] + [slice(None) if axis in got else coords[axis] for axis in axes])]
            axis, slot = order[stage - 1], stage
        return remote(self.place, ref, ref, self.send_sem.at[third], self.recv_sem.at[slot - 1, third], axis)

    def step(self, stage):
        with jax.named_scope(self.tag + str(stage)):
            self.step_(stage)

    def step_(self, stage):
        for core in range(2):
            last = 4 - core

            @pl.when(self.place["coords"]["core"] == core)
            def _():
                for third in range(3):
                    if 1 < stage <= last:
                        self.copy(core, stage - 1, third).wait()
                    if stage <= last:
                        self.copy(core, stage, third).start()
                    if stage == 5:
                        self.copy(core, last, third).wait_send()
                        self.copy(1 - core, 3 + core, third).wait_recv()


def body_kernel(
        z_hbm, dz_hbm, wpa_hbm, wpb_hbm, wpo_hbm, wq_hbm, wkv_hbm, wg_hbm, wo_hbm, wsa_hbm, wsb_hbm, wso_hbm,
        s_ref, ds_ref, mask_ref, qb_ref, wbias_ref,
        dzin_hbm, dsin_hbm, fs0_hbm, fs1_hbm, fa_hbm, fp_hbm,
        z_v, dz_v, wpa, wpb, wpo, wq, wkv, wg, wo, wsa, wsb, wso,
        z1_v, w8, bias_v, prob_v, act_v, q_v, gate_v, att_v, gated_v, gatt_v, gmid_v, gact_v, kv_v, gkv_v, gkvr_v,
        dwpa, dwpb, dwpo, m8, dsin_ref, c_all, ds_all, d_ab, d_so, gnew_v, gab_v,
        u0, u1, ut0, ut1, gn0, gn1, gnt0, gnt1, fs0, fs1, fa_ref, fp_ref,
        ga_, ga0, ga1, ga2, ga3, gp, gp0, gp1, gp2, gp3,
        in_sem, out_sem, kv_sem, send_sem, recv_a, recv_p, recv_d, recv_c, recv_t):
    dap = lax.axis_index("dap")
    dp = lax.axis_index("dp")
    core = lax.rem(dp, 2)
    cx = lax.rem(dp // 2, 2)
    cy = dp // 4
    peers = {
        "core": (dap, dp + 1 - 2 * core),
        "x": (dap, dp + 2 - 4 * cx),
        "y": (dap, dp + 4 - 8 * cy),
        "z": (1 - dap, dp),
    }
    place = {"coords": {"core": core, "x": cx, "y": cy, "z": dap}, "peers": peers}
    num_cplx, num_tok = mask_ref.shape
    half = num_tok // 2
    width = HEADS * HEAD_DIM

    loads = [(wkv_hbm, wkv), (wq_hbm, wq), (wg_hbm, wg), (wpa_hbm, wpa), (wpb_hbm, wpb), (wpo_hbm, wpo), (z_hbm, z_v),
             (wo_hbm, wo), (wsa_hbm, wsa), (wsb_hbm, wsb), (wso_hbm, wso), (dz_hbm, dz_v)]
    copies = [pltpu.make_async_copy(src, dst, in_sem.at[k]) for k, (src, dst) in enumerate(loads)]
    for item in copies:
        item.start()

    barrier = pltpu.get_barrier_semaphore()
    for peer in peers.values():
        pl.semaphore_signal(barrier, inc=1, device_id=peer, device_id_type=pl.DeviceIdType.MESH)

    red_a = Reducer(place, ROWS_A, ga_, (ga0, ga1, ga2, ga3), fa_ref, send_sem.at[0], recv_a)
    red_a.tag = 'A'
    red_p = Doubler(place, ROWS_P, gp, (gp0, gp1, gp2, gp3), fp_ref, send_sem.at[1], recv_p)
    red_p.tag = 'P'
    gat_ds = Gatherer(place, ds_all, send_sem.at[2], recv_d)
    gat_ds.tag = 'D'
    gat_c = Gatherer(place, c_all, send_sem.at[3], recv_c)
    gat_c.tag = 'C'
    tiles = Tiles(place, fs0, fs1, send_sem.at[4], recv_t)
    tiles.tag = 'T'

    def own_block(buf, value):
        for t in range(3):
            buf[t, core, cx, cy, dap] = value[:, t * LANES:(t + 1) * LANES]

    own_block(ds_all, ds_ref[...])

    s_f = s_ref[...].astype(F32)
    s_norm, s_inv = layer_norm(s_f)
    act = s_norm.astype(BF)
    act_v[...] = act
    copies[0].wait()
    kv_v[dap, :, 0:2 * width] = nn(act, wkv[...]).astype(BF)
    kv_v[dap, :, 2 * width:3 * width] = act

    def kv_copy():
        return pltpu.make_async_remote_copy(
            src_ref=kv_v.at[dap], dst_ref=kv_v.at[dap], send_sem=kv_sem.at[0], recv_sem=kv_sem.at[1],
            device_id=peers["z"], device_id_type=pl.DeviceIdType.MESH)

    def gkv_copy():
        return pltpu.make_async_remote_copy(
            src_ref=gkv_v.at[1 - dap], dst_ref=gkvr_v, send_sem=kv_sem.at[2], recv_sem=kv_sem.at[3],
            device_id=peers["z"], device_id_type=pl.DeviceIdType.MESH)

    with jax.named_scope('barrier'):
        pl.semaphore_wait(barrier, 4)
    kv_copy().start()
    gat_ds.step(1)
    copies[1].wait()
    copies[2].wait()
    q_v[...] = (nn(act, wq[...]) + qb_ref[...].astype(F32).reshape(1, width)).astype(BF)
    gate_v[...] = sigmoid(nn(act, wg[...]))

    row_head = lax.broadcasted_iota(jnp.int32, (128, HEADS), 0)
    col_head = lax.broadcasted_iota(jnp.int32, (128, HEADS), 1)
    pick = jnp.where((row_head >= col_head * 8) & (row_head < col_head * 8 + 8), 1.0, 0.0).astype(BF)
    spread = nn(pick, wbias_ref[...])
    row8 = lax.rem(lax.broadcasted_iota(jnp.int32, (128, LANES), 0), 8)
    for k in range(8):
        w8[:, k * LANES:(k + 1) * LANES] = jnp.where(row8 == k, spread, 0.0).astype(BF)

    for k in range(3, 7):
        copies[k].wait()

    blk = 8 * num_tok
    per_cplx = half // 8
    num_blk = num_cplx * per_cplx

    def side_by_side(tokens):
        return jnp.concatenate([tokens[k * num_tok:(k + 1) * num_tok] for k in range(8)], axis=1)

    def rows_at(b):
        return pl.ds(pl.multiple_of(b * blk, blk), blk)

    def bias_at(b):
        return b // per_cplx, pl.ds(pl.multiple_of(lax.rem(b, per_cplx) * 8, 8), 8)

    def forward_norm(b, u_ref):
        normed, _ = layer_norm(z_v[rows_at(b), :].astype(F32))
        u_ref[...] = normed.astype(BF)

    def forward_main(b, u_ref):
        total = z_v[rows_at(b), :].astype(F32)
        for f in range(0, 512, 256):
            u = u_ref[...]
            ha = nn(u, wpa[:, f:f + 256])
            hb = nn(u, wpb[:, f:f + 256])
            hidden = (ha * sigmoid(ha) * hb).astype(BF)
            total = total + nn(hidden, wpo[f:f + 256, :])
        z1_v[rows_at(b), :] = total.astype(BF)

    def forward_bias(b):
        bias_norm, _ = layer_norm(z1_v[rows_at(b), :].astype(F32))
        c, at = bias_at(b)
        bias_v[c, :, at, :] = nt(w8[...], side_by_side(bias_norm.astype(BF))).reshape(HEADS, 8, num_tok)

    def forward_pair(p, carry):
        forward_bias(2 * p)
        forward_norm(2 * p + 2, u0)
        forward_main(2 * p + 1, u1)
        forward_bias(2 * p + 1)
        forward_norm(2 * p + 3, u1)
        forward_main(2 * p + 2, u0)
        @pl.when(p == 3)
        def _():
            gat_ds.step(2)
        return carry

    forward_norm(0, u0)
    forward_norm(1, u1)
    forward_main(0, u0)
    with jax.named_scope('fwdloop'):
        lax.fori_loop(0, num_blk // 2 - 1, forward_pair, 0)
    forward_bias(num_blk - 2)
    forward_main(num_blk - 1, u1)
    forward_bias(num_blk - 1)
    gat_ds.step(3)

    scale = HEAD_DIM ** -0.5
    grow = lax.broadcasted_iota(jnp.int32, (HEADS, 1, width), 0) * HEAD_DIM
    gcol = lax.broadcasted_iota(jnp.int32, (HEADS, 1, width), 2)
    head_mask = (gcol >= grow) & (gcol < grow + HEAD_DIM)

    def expand(rows):
        wide = jnp.where(head_mask, rows.astype(F32)[None], 0.0)
        return wide.reshape(HEADS * half, width).astype(BF)

    def gather_heads(wide):
        return jnp.sum(jnp.where(head_mask, wide.reshape(HEADS, half, width), 0.0), axis=0)

    def tokens_of(c, lo):
        rows = slice(c * half, (c + 1) * half)
        return jnp.concatenate([kv_v[0, rows, lo:lo + width], kv_v[1, rows, lo:lo + width]], axis=0)

    kv_copy().wait()
    for c in range(num_cplx):
        rows = slice(c * half, (c + 1) * half)
        key_mask = MASK_BIG * (mask_ref[c:c + 1, :].astype(F32) - 1.0)
        logits = nt(expand(q_v[rows, :]), tokens_of(c, 0)) * scale + bias_v[c].reshape(HEADS * half, num_tok) + key_mask
        ex = jnp.exp(logits - jnp.max(logits, axis=-1, keepdims=True))
        prob = ex / jnp.sum(ex, axis=-1, keepdims=True)
        prob_v[c] = prob
        att_v[rows, :] = gather_heads(nn(prob.astype(BF), tokens_of(c, width)))
    gated = (gate_v[...] * att_v[...]).astype(BF)
    gated_v[...] = gated
    copies[7].wait()
    s_mid = (s_ref[...].astype(F32) + nn(gated, wo[...])).astype(BF)
    mid_norm, mid_inv = layer_norm(s_mid.astype(F32))
    mid_act = mid_norm.astype(BF)
    own_block(c_all, mid_act)
    gat_c.step(1)

    for k in range(8, 11):
        copies[k].wait()
    ds_b = ds_ref[...]
    grad_mid_norm = None
    for t in range(3):
        cols = slice(t * 512, (t + 1) * 512)
        ta = nn(mid_act, wsa[:, cols])
        tb = nn(mid_act, wsb[:, cols])
        dh = nt(ds_b, wso[cols, :])
        _, grad_a, grad_b = swiglu_grad(ta, tb, dh)
        part = nt(grad_a, wsa[:, cols]) + nt(grad_b, wsb[:, cols])
        grad_mid_norm = part if grad_mid_norm is None else grad_mid_norm + part
    grad_mid = ds_b.astype(F32) + norm_grad(mid_norm, mid_inv, grad_mid_norm)
    gmid_v[...] = grad_mid
    grad_mid_bf = grad_mid.astype(BF)
    grad_gated = nt(grad_mid_bf, wo[...])
    gate = gate_v[...]
    gatt_v[...] = (grad_gated * gate).astype(BF)
    grad_gate_pre = (grad_gated * att_v[...] * gate * (1.0 - gate)).astype(BF)

    def put_attn(buf, name_row, value):
        val = value.astype(BF)
        per = val.shape[1] // width
        for k in range(val.shape[1] // LANES):
            lo = name_row + (k % per) * 384
            buf[k // per, lo:lo + 384, :] = val[:, k * LANES:(k + 1) * LANES]

    act_t = act_v[...].T
    put_attn(ga_, 1152, nn(act_t, grad_gate_pre))
    put_attn(ga_, 1536, tn(gated_v[...], grad_mid_bf))
    gat_c.step(2)
    gat_ds.step(4)

    grad_q_parts = []
    for c in range(num_cplx):
        rows = slice(c * half, (c + 1) * half)
        keys, vals = tokens_of(c, 0), tokens_of(c, width)
        gatt = expand(gatt_v[rows, :])
        prob = prob_v[c]
        grad_prob = nt(gatt, vals)
        grad_vals = tn(prob.astype(BF), gatt)
        grad_logits = prob * (grad_prob - jnp.sum(prob * grad_prob, axis=-1, keepdims=True))
        bias_v[c] = grad_logits.reshape(HEADS, half, num_tok)
        gl_b = grad_logits.astype(BF)
        grad_q_parts.append(gather_heads(nn(gl_b, keys)) * scale)
        grad_keys = tn(gl_b, expand(q_v[rows, :])) * scale
        for d in range(2):
            gkv_v[d, rows, 0:width] = grad_keys[d * half:(d + 1) * half].astype(BF)
            gkv_v[d, rows, width:2 * width] = grad_vals[d * half:(d + 1) * half].astype(BF)
    grad_q = jnp.concatenate(grad_q_parts, axis=0)
    grad_q_bf = grad_q.astype(BF)
    put_attn(ga_, 0, nn(act_t, grad_q_bf))
    row16 = lax.broadcasted_iota(jnp.int32, (16, width), 0)
    bias_tile = jnp.where(row16 == 0, jnp.sum(grad_q, axis=0, keepdims=True), 0.0).astype(BF)
    for t in range(3):
        ga_[t, 1920:1936, :] = bias_tile[:, t * LANES:(t + 1) * LANES]
        ga_[t, 1936:2048, :] = jnp.zeros((112, LANES), BF)
    act_both = kv_v[:, :, 2 * width:3 * width].reshape(2 * s_ref.shape[0], width)
    put_attn(ga_, 384, tn(act_both, gkv_v[...].reshape(2 * s_ref.shape[0], 2 * width)))
    red_a.start()
    gact_v[...] = nt(grad_q_bf, wq[...]) + nt(grad_gate_pre, wg[...])

    def finish_attention():
        with jax.named_scope('gkvwait'):
            gkv_copy().wait()
        grad_kv = (gkv_v[dap].astype(F32) + gkvr_v[...].astype(F32)).astype(BF)
        grad_act = gact_v[...] + nt(grad_kv, wkv[...])
        s_norm2, s_inv2 = layer_norm(s_ref[...].astype(F32))
        dsin_ref[...] = (gmid_v[...] + norm_grad(s_norm2, s_inv2, grad_act)).astype(BF)
        out_copies[0].start()

    outs = [(dsin_ref, dsin_hbm), (fs0, fs0_hbm), (fs1, fs1_hbm), (fa_ref, fa_hbm), (fp_ref, fp_hbm), (dz_v, dzin_hbm)]
    out_copies = [pltpu.make_async_copy(src, dst, out_sem.at[k]) for k, (src, dst) in enumerate(outs)]

    def tile_grads():
        tile = jnp.where(core == 0, 3 * (2 * cx + cy) + 2 * dap, 3 * (2 * cx + cy) + 1)
        at = pl.ds(pl.multiple_of(tile * LANES, LANES), LANES)
        w_ab = jnp.concatenate([wsa[:, at], wsb[:, at]], axis=1)
        w_o_tile = wso[at, :]
        d_ab[...] = jnp.zeros(d_ab.shape, F32)
        d_so[...] = jnp.zeros(d_so.shape, F32)

        def quarter(k, carry):
            def rows_of(buf):
                return jnp.concatenate([buf[t, k // 2, lax.rem(k, 2)].reshape(4 * 96, LANES) for t in range(3)], axis=1)

            acts, cots = rows_of(c_all), rows_of(ds_all)
            both = nn(acts, w_ab)
            hidden, grad_a, grad_b = swiglu_grad(both[:, :LANES], both[:, LANES:], nt(cots, w_o_tile))
            d_ab[...] += tn(acts, jnp.concatenate([grad_a, grad_b], axis=1))
            d_so[...] += tn(hidden, cots)
            return carry

        with jax.named_scope('TP'):
            lax.fori_loop(0, 4, quarter, 0)
        for k in range(2):
            @pl.when(core == k)
            def _():
                slot = (cx, cy, dap) if k == 0 else (cx, cy)
                buf = fs0 if k == 0 else fs1
                buf[(0,) + slot] = d_ab[:, :LANES].astype(BF)
                buf[(1,) + slot] = d_ab[:, LANES:].astype(BF)
                so_b = d_so[...].astype(BF)
                buf[(2,) + slot] = jnp.concatenate([so_b[:, t * LANES:(t + 1) * LANES] for t in range(3)], axis=0)

    copies[11].wait()
    for ref in (dwpa, dwpb, dwpo, m8):
        ref[...] = jnp.zeros(ref.shape, F32)

    def hook(*calls):
        def run():
            for call in calls:
                call()
        return run

    hooks = {
        0: hook(lambda: gat_c.step(3)),
        1: hook(lambda: red_a.step(1)),
        3: hook(lambda: gat_c.step(4)),
        4: hook(lambda: red_a.step(2), lambda: gat_c.step(5), lambda: gat_ds.step(5), tile_grads, lambda: tiles.step(1)),
        5: hook(lambda: red_a.step(3)),
        7: hook(lambda: tiles.step(2)),
        8: hook(lambda: red_a.step(4)),
        9: hook(lambda: gkv_copy().start()),
    }
    tail_hooks = {
        1: hook(lambda: red_a.step(5)),
        2: hook(lambda: red_p.step(1)),
        3: hook(lambda: tiles.step(3)),
        7: hook(finish_attention),
        9: hook(lambda: red_p.step(2), lambda: red_a.step(6)),
    }

    def run_hooks(table, k):
        for when, todo in table.items():
            pl.when(k == when)(todo)

    def backward_head(b, live, bufs):
        u_ref, ut_ref, gn_ref, gnt_ref = bufs
        at = rows_at(b)
        c, rows = bias_at(b)
        gl_f = bias_v[c, :, rows, :].reshape(8 * HEADS, num_tok)
        wide = tn(gl_f.astype(BF), w8[...])
        grad_norm = jnp.concatenate([wide[:, k * LANES:(k + 1) * LANES] for k in range(8)], axis=0)
        bias_norm, bias_inv = layer_norm(z1_v[at, :].astype(F32))
        m8[...] += nn((gl_f * live).astype(BF), side_by_side(bias_norm.astype(BF)))
        grad_new = dz_v[at, :].astype(F32) + norm_grad(bias_norm, bias_inv, grad_norm)
        gnew_v[at, :] = grad_new
        gnb = grad_new.astype(BF)
        gn_ref[...] = gnb
        gnt_ref[...] = gnb.T
        normed, _ = layer_norm(z_v[at, :].astype(F32))
        u = normed.astype(BF)
        u_ref[...] = u
        ut_ref[...] = u.T

    def backward_main(b, bufs):
        u_ref, ut_ref, gn_ref, gnt_ref = bufs
        at = rows_at(b)
        for f in range(0, 512, 256):
            cols = slice(f, f + 256)
            u, gnb = u_ref[...], gn_ref[...]
            hidden, grad_a, grad_b = swiglu_grad(nn(u, wpa[:, cols]), nn(u, wpb[:, cols]), nt(gnb, wpo[cols, :]))
            gab_v[at, cols] = grad_a
            gab_v[at, 512 + f:768 + f] = grad_b
            dwpo[:, cols] += nn(gnt_ref[...], hidden)
            dwpa[:, cols] += nn(ut_ref[...], grad_a)
            dwpb[:, cols] += nn(ut_ref[...], grad_b)

    def backward_tail(b, carry):
        at = rows_at(b)
        grad_normed = nt(gab_v[at, :], jnp.concatenate([wpa[...], wpb[...]], axis=1))
        normed, inv = layer_norm(z_v[at, :].astype(F32))
        dz_v[at, :] = (gnew_v[at, :] + norm_grad(normed, inv, grad_normed)).astype(BF)
        run_hooks(tail_hooks, b)
        return carry

    bufs0, bufs1 = (u0, ut0, gn0, gnt0), (u1, ut1, gn1, gnt1)

    def backward_pair(p, carry):
        backward_head(2 * p + 1, 1.0, bufs1)
        backward_main(2 * p, bufs0)
        run_hooks({k // 2: v for k, v in hooks.items() if k % 2 == 0}, p)
        more = jnp.where(p < num_blk // 2 - 1, 1.0, 0.0)
        backward_head(jnp.minimum(2 * p + 2, num_blk - 1), more, bufs0)
        backward_main(2 * p + 1, bufs1)
        run_hooks({k // 2: v for k, v in hooks.items() if k % 2}, p)
        return carry

    backward_head(0, 1.0, bufs0)
    with jax.named_scope('bwdloop'):
        lax.fori_loop(0, num_blk // 2, backward_pair, 0)

    for t, ref in enumerate((dwpa, dwpb, dwpo)):
        for k in range(4):
            gp[t, k * 128:(k + 1) * 128, :] = ref[:, k * LANES:(k + 1) * LANES].astype(BF)
        gp[t, 528:544, :] = jnp.zeros((16, LANES), BF)
    diag = jnp.zeros((128, LANES), F32)
    for k in range(8):
        diag = diag + jnp.where(row8 == k, m8[:, k * LANES:(k + 1) * LANES], 0.0)
    gp[0, 512:528, :] = jnp.sum(diag.reshape(HEADS, 8, LANES), axis=1).astype(BF)
    for t in range(1, 3):
        gp[t, 512:528, :] = jnp.zeros((16, LANES), BF)
    red_p.start()
    with jax.named_scope('tailloop'):
        lax.fori_loop(0, num_blk, backward_tail, 0)
    out_copies[5].start()
    tiles.step(4)
    for k in range(2):
        @pl.when(core == k)
        def _():
            out_copies[1 + k].start()
    red_p.step(3)
    red_a.step(7)
    red_p.step(4)
    tiles.step(5)
    for k in range(2):
        @pl.when(core == k)
        def _():
            out_copies[2 - k].start()
    red_a.step(8)
    out_copies[3].start()
    red_p.step(5)
    out_copies[4].start()
    for item in out_copies:
        item.wait()


def unpack_kernel(dz_i, ds_i, fs0_i, fs1_i, fa_i, fp_i,
                  dz_o, ds_o, pa_o, pb_o, po_o, bias_o, q_o, qb_o, kv_o, g_o, o_o, sa_o, sb_o, so_o,
                  dz, ds, fs0, fs1, fa, fp, pa, pb, po, bias, q, qb, kv, g, o, sa, sb, so, in_sem, sem):
    ins = [(fs0_i, fs0), (fs1_i, fs1), (fa_i, fa), (fp_i, fp), (dz_i, dz), (ds_i, ds)]
    reads = [pltpu.make_async_copy(src, dst, in_sem.at[k]) for k, (src, dst) in enumerate(ins)]
    for item in reads:
        item.start()
    outs = [(sa, sa_o), (sb, sb_o), (so, so_o), (q, q_o), (kv, kv_o), (g, g_o), (o, o_o), (qb, qb_o), (pa, pa_o), (pb, pb_o),
            (po, po_o), (bias, bias_o), (dz, dz_o), (ds, ds_o)]
    copies = [pltpu.make_async_copy(src, dst, sem.at[k]) for k, (src, dst) in enumerate(outs)]

    reads[0].wait()
    reads[1].wait()
    for kind in range(3):
        for pair in range(4):
            cx, cy = pair // 2, pair % 2
            for j in range(3):
                lo = (3 * pair + j) * LANES
                tile = fs1[kind, cx, cy] if j == 1 else fs0[kind, cx, cy, j // 2]
                wide = tile.astype(F32)
                if kind < 2:
                    (sa, sb)[kind][:, lo:lo + LANES] = wide
                else:
                    for k in range(3):
                        so[lo:lo + LANES, k * LANES:(k + 1) * LANES] = wide[k * LANES:(k + 1) * LANES]
        copies[kind].start()
    reads[2].wait()
    for index, (ref, buf, row) in enumerate(((q, fa, 0), (kv, fa, 384), (g, fa, 1152), (o, fa, 1536))):
        per = ref.shape[1] // 384
        for k in range(3 * per):
            lo = row + (k % per) * 384
            ref[:, k * LANES:(k + 1) * LANES] = buf[k // per, lo:lo + 384, :].astype(F32)
        copies[3 + index].start()
    for t in range(3):
        qb[t * LANES:(t + 1) * LANES] = fa[t, 1920:1936, :].astype(F32)[0]
    copies[7].start()
    reads[3].wait()
    for t, ref in enumerate((pa, pb)):
        for k in range(4):
            ref[:, k * LANES:(k + 1) * LANES] = fp[t, k * 128:(k + 1) * 128, :].astype(F32)
        copies[8 + t].start()
    for k in range(4):
        po[k * 128:(k + 1) * 128, :] = fp[2, k * 128:(k + 1) * 128, :].astype(F32).T
    copies[10].start()
    bias[...] = fp[0, 512:528, :].astype(F32)
    copies[11].start()
    for k in range(2):
        reads[4 + k].wait()
        copies[12 + k].start()
    for item in copies:
        item.wait()


def solution(mesh):
    pair_spec = P('dp', 'dap', None, None)
    single_spec = P('dp', 'dap', None)
    hbm = pl.BlockSpec(memory_space=pl.ANY)
    vmem = pl.BlockSpec(memory_space=pltpu.VMEM)

    def body(pair_z, single_s, token_mask, dz_out, ds_out, w_pa, w_pb, w_po, w_bias, w_q, q_bias, w_kv, w_g, w_o, w_sa, w_sb, w_so):
        num_cplx, half, num_tok, dim = pair_z.shape
        toks = num_cplx * half * num_tok
        rows = num_cplx * half
        width = w_q.shape[1]
        big = (pair_z.reshape(toks, dim), dz_out.reshape(toks, dim), w_pa, w_pb, w_po, w_q, w_kv, w_g, w_o, w_sa, w_sb, w_so)
        small = (single_s.reshape(rows, width), ds_out.reshape(rows, width), token_mask, q_bias, w_bias.T)
        scratch = [pltpu.VMEM(a.shape, a.dtype) for a in big]
        finals = [(toks, dim), (rows, width), (3, 2, 2, 2, width, LANES), (3, 2, 2, width, LANES), (3, ROWS_A, LANES), (3, ROWS_P, LANES)]
        scratch += [
            pltpu.VMEM((toks, dim), BF), pltpu.VMEM((128, 1024), BF),
            pltpu.VMEM((num_cplx, HEADS, half, num_tok), F32), pltpu.VMEM((num_cplx, HEADS * half, num_tok), F32),
            pltpu.VMEM((rows, width), BF), pltpu.VMEM((rows, width), BF), pltpu.VMEM((rows, width), F32),
            pltpu.VMEM((rows, width), F32), pltpu.VMEM((rows, width), BF), pltpu.VMEM((rows, width), BF),
            pltpu.VMEM((rows, width), F32), pltpu.VMEM((rows, width), F32),
            pltpu.VMEM((2, rows, 3 * width), BF), pltpu.VMEM((2, rows, 2 * width), BF), pltpu.VMEM((rows, 2 * width), BF),
            pltpu.VMEM((128, 512), F32), pltpu.VMEM((128, 512), F32), pltpu.VMEM((128, 512), F32), pltpu.VMEM((128, 1024), F32),
            pltpu.VMEM(finals[1], BF),
            pltpu.VMEM((3, 2, 2, 2, 2, rows, LANES), BF), pltpu.VMEM((3, 2, 2, 2, 2, rows, LANES), BF),
            pltpu.VMEM((width, 2 * LANES), F32), pltpu.VMEM((LANES, width), F32),
            pltpu.VMEM((toks, dim), F32), pltpu.VMEM((toks, 1024), BF),
        ]
        for _ in range(2):
            scratch += [pltpu.VMEM((512, dim), BF)] * 2 + [pltpu.VMEM((dim, 512), BF)] * 2
        scratch += [pltpu.VMEM(shape, BF) for shape in finals[2:]]
        scratch += [pltpu.VMEM((3, ROWS_A >> k, LANES), BF) for k in range(5)]
        scratch += [pltpu.VMEM((3, ROWS_P, LANES), BF)] + [pltpu.VMEM((3, ROWS_P // 2, LANES), BF) for _ in range(4)]
        scratch += [pltpu.SemaphoreType.DMA((12,)), pltpu.SemaphoreType.DMA((6,)),
                    pltpu.SemaphoreType.DMA((4,)), pltpu.SemaphoreType.DMA((5, 3))]
        scratch += [pltpu.SemaphoreType.DMA((stages, 3)) for stages in (8, 5, 4, 4, 4)]
        packed = pl.pallas_call(
            body_kernel,
            out_shape=[jax.ShapeDtypeStruct(shape, BF) for shape in finals],
            in_specs=[hbm] * 12 + [vmem] * 5,
            out_specs=[hbm] * 6,
            scratch_shapes=scratch,
            compiler_params=pltpu.CompilerParams(collective_id=0, has_side_effects=True, vmem_limit_bytes=60 * 2 ** 20),
            name="block",
        )(*big, *small)
        shapes = [w_pa.shape, w_pb.shape, w_po.shape, (HEADS, dim), w_q.shape, (width,), w_kv.shape, w_g.shape, w_o.shape,
                  w_sa.shape, w_sb.shape, w_so.shape]
        done = pl.pallas_call(
            unpack_kernel,
            out_shape=[jax.ShapeDtypeStruct(shape, BF) for shape in finals[:2]] + [jax.ShapeDtypeStruct(shape, F32) for shape in shapes],
            in_specs=[hbm] * 6,
            out_specs=[hbm] * 14,
            scratch_shapes=[pltpu.VMEM(shape, BF) for shape in finals] + [pltpu.VMEM(shape, F32) for shape in shapes] + [
                pltpu.SemaphoreType.DMA((6,)), pltpu.SemaphoreType.DMA((14,))],
            compiler_params=pltpu.CompilerParams(vmem_limit_bytes=56 * 2 ** 20),
            name="unpack",
        )(*packed)
        grads = list(done[2:])
        grads[3] = grads[3].T
        return (done[0].reshape(pair_z.shape), done[1].reshape(single_s.shape)) + tuple(grads)

    in_specs = (pair_spec, single_spec, P('dp', None), pair_spec, single_spec) + (P(),) * 12
    out_specs = (pair_spec, single_spec) + (P(),) * 12
    return jax.shard_map(body, mesh=mesh, in_specs=in_specs, out_specs=out_specs, check_vma=False)
```

```python
import jax
import jax.numpy as jnp
from jax import lax
from jax.experimental import pallas as pl
from jax.experimental.pallas import tpu as pltpu
from jax.sharding import PartitionSpec as P

HEADS = 16
HEAD_DIM = 24
EPSILON = 1e-5
MASK_BIG = 1e9
BF = jnp.bfloat16
F32 = jnp.float32
ROWS_A, ROWS_P = 2048, 544
LANES = 128


def nn(a, b):
    return lax.dot_general(a, b, (((1,), (0,)), ((), ())), preferred_element_type=F32)


def nt(a, b):
    return lax.dot_general(a, b, (((1,), (1,)), ((), ())), preferred_element_type=F32)


def tn(a, b):
    return lax.dot_general(a, b, (((0,), (0,)), ((), ())), preferred_element_type=F32)


def sigmoid(x):
    return 0.5 * jnp.tanh(0.5 * x) + 0.5


def layer_norm(vals):
    centred = vals - jnp.mean(vals, axis=-1, keepdims=True)
    inv = lax.rsqrt(jnp.mean(centred * centred, axis=-1, keepdims=True) + EPSILON)
    return centred * inv, inv


def norm_grad(normed, inv, grad):
    mean_grad = jnp.mean(grad, axis=-1, keepdims=True)
    mean_proj = jnp.mean(grad * normed, axis=-1, keepdims=True)
    return inv * (grad - mean_grad - normed * mean_proj)


def swiglu_grad(ha, hb, dh):
    sig = sigmoid(ha)
    silu = ha * sig
    hidden = silu * hb
    grad_a = dh * hb * (sig * (1.0 + (ha - silu)))
    return hidden.astype(BF), grad_a.astype(BF), (dh * silu).astype(BF)


AXES = ("x", "y", "z")
ORDER = (("x", "y", "z"), ("y", "z", "x"), ("z", "x", "y"))
ORDER_XY = (("x", "y"), ("y", "x"), ("x", "y"))


def remote(place, src, dst, send_sem, recv_sem, axis):
    return pltpu.make_async_remote_copy(
        src_ref=src, dst_ref=dst, send_sem=send_sem, recv_sem=recv_sem,
        device_id=place["peers"][axis], device_id_type=pl.DeviceIdType.MESH)


class Reducer:
    last = 8

    def __init__(self, place, rows, grads, recvs, final, send_sem, recv_sem):
        self.place, self.rows, self.grads, self.recvs, self.final = place, rows, grads, recvs, final
        self.send_sem, self.recv_sem = send_sem, recv_sem
        coords = place["coords"]
        self.base = []
        for third in range(3):
            base = [coords["core"] * (rows // 2)]
            for depth, axis in enumerate(ORDER[third]):
                base.append(base[-1] + coords[axis] * (rows >> (depth + 2)))
            self.base.append(base)

    def copy(self, stage, third):
        rows, base, order = self.rows, self.base[third], ORDER[third]
        coords = self.place["coords"]
        step = rows // 16
        if stage < 4:
            size = rows >> (stage + 1)
            axis = "core" if stage == 0 else order[stage - 1]
            low = 0 if stage == 0 else base[stage - 1]
            start = pl.multiple_of(low + (1 - coords[axis]) * size, step)
            src = self.grads.at[third, pl.ds(start, size)]
            dst = self.recvs[stage].at[third]
        else:
            size = rows >> (8 - stage)
            axis = "core" if stage == 7 else order[6 - stage]
            start = pl.multiple_of(base[7 - stage], step)
            src = self.final.at[third, pl.ds(start, size)]
            dst = src
        return remote(self.place, src, dst, self.send_sem.at[third], self.recv_sem.at[stage, third], axis)

    def add(self, third, low, size, chunk, recv, dest):
        def run(k, carry):
            at = pl.ds(pl.multiple_of(low + k * chunk, chunk), chunk)
            off = pl.ds(pl.multiple_of(k * chunk, chunk), chunk)
            dest[third, at, :] = (self.grads[third, at, :].astype(F32) + recv[third, off, :].astype(F32)).astype(BF)
            return carry

        lax.fori_loop(0, size // chunk, run, 0)

    def start(self):
        for third in range(3):
            self.copy(0, third).start()

    def step(self, stage):
        for third in range(3):
            done = stage - 1
            self.copy(done, third).wait()
            if done < 4:
                self.add(third, self.base[third][done], self.rows >> (done + 1), self.rows // 16, self.recvs[done],
                         self.final if done == 3 else self.grads)
            if stage < self.last:
                self.copy(stage, third).start()


class Doubler(Reducer):
    last = 5

    def copy(self, stage, third):
        half = self.rows // 2
        core = self.place["coords"]["core"]
        mine = pl.ds(pl.multiple_of(core * half, 16), half)
        if stage == 0:
            src = self.grads.at[third, pl.ds(pl.multiple_of((1 - core) * half, 16), half)]
            dst, axis = self.recvs[0].at[third], "core"
        elif stage < 4:
            src, dst, axis = self.grads.at[third, mine], self.recvs[stage].at[third], ORDER[third][stage - 1]
        else:
            src, dst, axis = self.final.at[third, mine], self.final.at[third, mine], "core"
        return remote(self.place, src, dst, self.send_sem.at[third], self.recv_sem.at[stage, third], axis)

    def step(self, stage):
        half = self.rows // 2
        for third in range(3):
            done = stage - 1
            self.copy(done, third).wait()
            if done < 4:
                self.add(third, self.base[third][0], half, half, self.recvs[done], self.final if done == 3 else self.grads)
            if stage < self.last:
                self.copy(stage, third).start()


class Gatherer:
    def __init__(self, place, buf, send_sem, recv_sem):
        self.place, self.buf, self.send_sem, self.recv_sem = place, buf, send_sem, recv_sem

    def copy(self, stage, third):
        coords, order = self.place["coords"], ORDER[third]
        got = order[:stage - 1]
        index = [third, coords["core"]] + [slice(None) if axis in got else coords[axis] for axis in AXES]
        ref = self.buf.at[tuple(index)]
        axis = order[stage - 1] if stage < 4 else "core"
        return remote(self.place, ref, ref, self.send_sem.at[third], self.recv_sem.at[stage - 1, third], axis)

    def step(self, stage):
        for third in range(3):
            if stage > 1:
                self.copy(stage - 1, third).wait()
            if stage < 5:
                self.copy(stage, third).start()


class Tiles:
    def __init__(self, place, buf0, buf1, send_sem, recv_sem):
        self.place, self.bufs, self.send_sem, self.recv_sem = place, (buf0, buf1), send_sem, recv_sem

    def copy(self, core, stage, third):
        coords = self.place["coords"]
        order = ORDER[third] if core == 0 else ORDER_XY[third]
        axes = AXES if core == 0 else AXES[:2]
        if stage > len(order):
            ref, axis, slot = self.bufs[core].at[third], "core", 4
        else:
            got = order[:stage - 1]
            ref = self.bufs[core].at[tuple([third] + [slice(None) if axis in got else coords[axis] for axis in axes])]
            axis, slot = order[stage - 1], stage
        return remote(self.place, ref, ref, self.send_sem.at[third], self.recv_sem.at[slot - 1, third], axis)

    def step(self, stage):
        for core in range(2):
            last = 4 - core

            @pl.when(self.place["coords"]["core"] == core)
            def _():
                for third in range(3):
                    if 1 < stage <= last:
                        self.copy(core, stage - 1, third).wait()
                    if stage <= last:
                        self.copy(core, stage, third).start()
                    if stage == 5:
                        self.copy(core, last, third).wait_send()
                        self.copy(1 - core, 3 + core, third).wait_recv()


def body_kernel(
        z_hbm, dz_hbm, wpa_hbm, wpb_hbm, wpo_hbm, wq_hbm, wkv_hbm, wg_hbm, wo_hbm, wsa_hbm, wsb_hbm, wso_hbm,
        s_ref, ds_ref, mask_ref, qb_ref, wbias_ref,
        dzin_hbm, dsin_hbm, fs0_hbm, fs1_hbm, fa_hbm, fp_hbm,
        z_v, dz_v, wpa, wpb, wpo, wq, wkv, wg, wo, wsa, wsb, wso,
        z1_v, w8, bias_v, prob_v, act_v, q_v, gate_v, att_v, gated_v, gatt_v, gmid_v, gact_v, kv_v, gkv_v, gkvr_v,
        dwpa, dwpb, dwpo, m8, dsin_ref, c_all, ds_all, d_ab, d_so, gnew_v, gab_v,
        u0, u1, ut0, ut1, gn0, gn1, gnt0, gnt1, fs0, fs1, fa_ref, fp_ref,
        ga_, ga0, ga1, ga2, ga3, gp, gp0, gp1, gp2, gp3,
        in_sem, out_sem, kv_sem, send_sem, recv_a, recv_p, recv_d, recv_c, recv_t):
    dap = lax.axis_index("dap")
    dp = lax.axis_index("dp")
    core = lax.rem(dp, 2)
    cx = lax.rem(dp // 2, 2)
    cy = dp // 4
    peers = {
        "core": (dap, dp + 1 - 2 * core),
        "x": (dap, dp + 2 - 4 * cx),
        "y": (dap, dp + 4 - 8 * cy),
        "z": (1 - dap, dp),
    }
    place = {"coords": {"core": core, "x": cx, "y": cy, "z": dap}, "peers": peers}
    num_cplx, num_tok = mask_ref.shape
    half = num_tok // 2
    width = HEADS * HEAD_DIM

    loads = [(wkv_hbm, wkv), (wq_hbm, wq), (wg_hbm, wg), (wpa_hbm, wpa), (wpb_hbm, wpb), (wpo_hbm, wpo), (z_hbm, z_v),
             (wo_hbm, wo), (wsa_hbm, wsa), (wsb_hbm, wsb), (wso_hbm, wso), (dz_hbm, dz_v)]
    copies = [pltpu.make_async_copy(src, dst, in_sem.at[k]) for k, (src, dst) in enumerate(loads)]
    for item in copies:
        item.start()

    barrier = pltpu.get_barrier_semaphore()
    for peer in peers.values():
        pl.semaphore_signal(barrier, inc=1, device_id=peer, device_id_type=pl.DeviceIdType.MESH)

    red_a = Reducer(place, ROWS_A, ga_, (ga0, ga1, ga2, ga3), fa_ref, send_sem.at[0], recv_a)
    red_p = Doubler(place, ROWS_P, gp, (gp0, gp1, gp2, gp3), fp_ref, send_sem.at[1], recv_p)
    gat_ds = Gatherer(place, ds_all, send_sem.at[2], recv_d)
    gat_c = Gatherer(place, c_all, send_sem.at[3], recv_c)
    tiles = Tiles(place, fs0, fs1, send_sem.at[4], recv_t)

    def own_block(buf, value):
        for t in range(3):
            buf[t, core, cx, cy, dap] = value[:, t * LANES:(t + 1) * LANES]

    own_block(ds_all, ds_ref[...])

    s_f = s_ref[...].astype(F32)
    s_norm, s_inv = layer_norm(s_f)
    act = s_norm.astype(BF)
    act_v[...] = act
    copies[0].wait()
    kv_v[dap, :, 0:2 * width] = nn(act, wkv[...]).astype(BF)
    kv_v[dap, :, 2 * width:3 * width] = act

    def kv_copy():
        return pltpu.make_async_remote_copy(
            src_ref=kv_v.at[dap], dst_ref=kv_v.at[dap], send_sem=kv_sem.at[0], recv_sem=kv_sem.at[1],
            device_id=peers["z"], device_id_type=pl.DeviceIdType.MESH)

    def gkv_copy():
        return pltpu.make_async_remote_copy(
            src_ref=gkv_v.at[1 - dap], dst_ref=gkvr_v, send_sem=kv_sem.at[2], recv_sem=kv_sem.at[3],
            device_id=peers["z"], device_id_type=pl.DeviceIdType.MESH)

    pl.semaphore_wait(barrier, 4)
    kv_copy().start()
    gat_ds.step(1)
    copies[1].wait()
    copies[2].wait()
    q_v[...] = (nn(act, wq[...]) + qb_ref[...].astype(F32).reshape(1, width)).astype(BF)
    gate_v[...] = sigmoid(nn(act, wg[...]))

    row_head = lax.broadcasted_iota(jnp.int32, (128, HEADS), 0)
    col_head = lax.broadcasted_iota(jnp.int32, (128, HEADS), 1)
    pick = jnp.where((row_head >= col_head * 8) & (row_head < col_head * 8 + 8), 1.0, 0.0).astype(BF)
    spread = nn(pick, wbias_ref[...])
    row8 = lax.rem(lax.broadcasted_iota(jnp.int32, (128, LANES), 0), 8)
    for k in range(8):
        w8[:, k * LANES:(k + 1) * LANES] = jnp.where(row8 == k, spread, 0.0).astype(BF)

    for k in range(3, 7):
        copies[k].wait()

    blk = 8 * num_tok
    per_cplx = half // 8
    num_blk = num_cplx * per_cplx

    def side_by_side(tokens):
        return jnp.concatenate([tokens[k * num_tok:(k + 1) * num_tok] for k in range(8)], axis=1)

    def rows_at(b):
        return pl.ds(pl.multiple_of(b * blk, blk), blk)

    def bias_at(b):
        return b // per_cplx, pl.ds(pl.multiple_of(lax.rem(b, per_cplx) * 8, 8), 8)

    def forward_norm(b, u_ref):
        normed, _ = layer_norm(z_v[rows_at(b), :].astype(F32))
        u_ref[...] = normed.astype(BF)

    def forward_main(b, u_ref):
        total = z_v[rows_at(b), :].astype(F32)
        for f in range(0, 512, 256):
            u = u_ref[...]
            ha = nn(u, wpa[:, f:f + 256])
            hb = nn(u, wpb[:, f:f + 256])
            hidden = (ha * sigmoid(ha) * hb).astype(BF)
            total = total + nn(hidden, wpo[f:f + 256, :])
        z1_v[rows_at(b), :] = total.astype(BF)

    def forward_bias(b):
        bias_norm, _ = layer_norm(z1_v[rows_at(b), :].astype(F32))
        c, at = bias_at(b)
        bias_v[c, :, at, :] = nt(w8[...], side_by_side(bias_norm.astype(BF))).reshape(HEADS, 8, num_tok)

    def forward_pair(p, carry):
        forward_bias(2 * p)
        forward_norm(2 * p + 2, u0)
        forward_main(2 * p + 1, u1)
        forward_bias(2 * p + 1)
        forward_norm(2 * p + 3, u1)
        forward_main(2 * p + 2, u0)
        @pl.when(p == 3)
        def _():
            gat_ds.step(2)
        return carry

    forward_norm(0, u0)
    forward_norm(1, u1)
    forward_main(0, u0)
    lax.fori_loop(0, num_blk // 2 - 1, forward_pair, 0)
    forward_bias(num_blk - 2)
    forward_main(num_blk - 1, u1)
    forward_bias(num_blk - 1)
    gat_ds.step(3)

    scale = HEAD_DIM ** -0.5
    grow = lax.broadcasted_iota(jnp.int32, (HEADS, 1, width), 0) * HEAD_DIM
    gcol = lax.broadcasted_iota(jnp.int32, (HEADS, 1, width), 2)
    head_mask = (gcol >= grow) & (gcol < grow + HEAD_DIM)

    def expand(rows):
        wide = jnp.where(head_mask, rows.astype(F32)[None], 0.0)
        return wide.reshape(HEADS * half, width).astype(BF)

    def gather_heads(wide):
        return jnp.sum(jnp.where(head_mask, wide.reshape(HEADS, half, width), 0.0), axis=0)

    def tokens_of(c, lo):
        rows = slice(c * half, (c + 1) * half)
        return jnp.concatenate([kv_v[0, rows, lo:lo + width], kv_v[1, rows, lo:lo + width]], axis=0)

    kv_copy().wait()
    for c in range(num_cplx):
        rows = slice(c * half, (c + 1) * half)
        key_mask = MASK_BIG * (mask_ref[c:c + 1, :].astype(F32) - 1.0)
        logits = nt(expand(q_v[rows, :]), tokens_of(c, 0)) * scale + bias_v[c].reshape(HEADS * half, num_tok) + key_mask
        ex = jnp.exp(logits - jnp.max(logits, axis=-1, keepdims=True))
        prob = ex / jnp.sum(ex, axis=-1, keepdims=True)
        prob_v[c] = prob
        att_v[rows, :] = gather_heads(nn(prob.astype(BF), tokens_of(c, width)))
    gated = (gate_v[...] * att_v[...]).astype(BF)
    gated_v[...] = gated
    copies[7].wait()
    s_mid = (s_ref[...].astype(F32) + nn(gated, wo[...])).astype(BF)
    mid_norm, mid_inv = layer_norm(s_mid.astype(F32))
    mid_act = mid_norm.astype(BF)
    own_block(c_all, mid_act)
    gat_c.step(1)

    for k in range(8, 11):
        copies[k].wait()
    ds_b = ds_ref[...]
    grad_mid_norm = None
    for t in range(3):
        cols = slice(t * 512, (t + 1) * 512)
        ta = nn(mid_act, wsa[:, cols])
        tb = nn(mid_act, wsb[:, cols])
        dh = nt(ds_b, wso[cols, :])
        _, grad_a, grad_b = swiglu_grad(ta, tb, dh)
        part = nt(grad_a, wsa[:, cols]) + nt(grad_b, wsb[:, cols])
        grad_mid_norm = part if grad_mid_norm is None else grad_mid_norm + part
    grad_mid = ds_b.astype(F32) + norm_grad(mid_norm, mid_inv, grad_mid_norm)
    gmid_v[...] = grad_mid
    grad_mid_bf = grad_mid.astype(BF)
    grad_gated = nt(grad_mid_bf, wo[...])
    gate = gate_v[...]
    gatt_v[...] = (grad_gated * gate).astype(BF)
    grad_gate_pre = (grad_gated * att_v[...] * gate * (1.0 - gate)).astype(BF)

    def put_attn(buf, name_row, value):
        val = value.astype(BF)
        per = val.shape[1] // width
        for k in range(val.shape[1] // LANES):
            lo = name_row + (k % per) * 384
            buf[k // per, lo:lo + 384, :] = val[:, k * LANES:(k + 1) * LANES]

    act_t = act_v[...].T
    put_attn(ga_, 1152, nn(act_t, grad_gate_pre))
    put_attn(ga_, 1536, tn(gated_v[...], grad_mid_bf))
    gat_c.step(2)
    gat_ds.step(4)

    grad_q_parts = []
    for c in range(num_cplx):
        rows = slice(c * half, (c + 1) * half)
        keys, vals = tokens_of(c, 0), tokens_of(c, width)
        gatt = expand(gatt_v[rows, :])
        prob = prob_v[c]
        grad_prob = nt(gatt, vals)
        grad_vals = tn(prob.astype(BF), gatt)
        grad_logits = prob * (grad_prob - jnp.sum(prob * grad_prob, axis=-1, keepdims=True))
        bias_v[c] = grad_logits.reshape(HEADS, half, num_tok)
        gl_b = grad_logits.astype(BF)
        grad_q_parts.append(gather_heads(nn(gl_b, keys)) * scale)
        grad_keys = tn(gl_b, expand(q_v[rows, :])) * scale
        for d in range(2):
            gkv_v[d, rows, 0:width] = grad_keys[d * half:(d + 1) * half].astype(BF)
            gkv_v[d, rows, width:2 * width] = grad_vals[d * half:(d + 1) * half].astype(BF)
    grad_q = jnp.concatenate(grad_q_parts, axis=0)
    grad_q_bf = grad_q.astype(BF)
    put_attn(ga_, 0, nn(act_t, grad_q_bf))
    row16 = lax.broadcasted_iota(jnp.int32, (16, width), 0)
    bias_tile = jnp.where(row16 == 0, jnp.sum(grad_q, axis=0, keepdims=True), 0.0).astype(BF)
    for t in range(3):
        ga_[t, 1920:1936, :] = bias_tile[:, t * LANES:(t + 1) * LANES]
        ga_[t, 1936:2048, :] = jnp.zeros((112, LANES), BF)
    act_both = kv_v[:, :, 2 * width:3 * width].reshape(2 * s_ref.shape[0], width)
    put_attn(ga_, 384, tn(act_both, gkv_v[...].reshape(2 * s_ref.shape[0], 2 * width)))
    red_a.start()
    gact_v[...] = nt(grad_q_bf, wq[...]) + nt(grad_gate_pre, wg[...])

    def finish_attention():
        gkv_copy().wait()
        grad_kv = (gkv_v[dap].astype(F32) + gkvr_v[...].astype(F32)).astype(BF)
        grad_act = gact_v[...] + nt(grad_kv, wkv[...])
        s_norm2, s_inv2 = layer_norm(s_ref[...].astype(F32))
        dsin_ref[...] = (gmid_v[...] + norm_grad(s_norm2, s_inv2, grad_act)).astype(BF)
        out_copies[0].start()

    outs = [(dsin_ref, dsin_hbm), (fs0, fs0_hbm), (fs1, fs1_hbm), (fa_ref, fa_hbm), (fp_ref, fp_hbm), (dz_v, dzin_hbm)]
    out_copies = [pltpu.make_async_copy(src, dst, out_sem.at[k]) for k, (src, dst) in enumerate(outs)]

    def tile_grads():
        tile = jnp.where(core == 0, 3 * (2 * cx + cy) + 2 * dap, 3 * (2 * cx + cy) + 1)
        at = pl.ds(pl.multiple_of(tile * LANES, LANES), LANES)
        w_ab = jnp.concatenate([wsa[:, at], wsb[:, at]], axis=1)
        w_o_tile = wso[at, :]
        d_ab[...] = jnp.zeros(d_ab.shape, F32)
        d_so[...] = jnp.zeros(d_so.shape, F32)

        def quarter(k, carry):
            def rows_of(buf):
                return jnp.concatenate([buf[t, k // 2, lax.rem(k, 2)].reshape(4 * 96, LANES) for t in range(3)], axis=1)

            acts, cots = rows_of(c_all), rows_of(ds_all)
            both = nn(acts, w_ab)
            hidden, grad_a, grad_b = swiglu_grad(both[:, :LANES], both[:, LANES:], nt(cots, w_o_tile))
            d_ab[...] += tn(acts, jnp.concatenate([grad_a, grad_b], axis=1))
            d_so[...] += tn(hidden, cots)
            return carry

        lax.fori_loop(0, 4, quarter, 0)
        for k in range(2):
            @pl.when(core == k)
            def _():
                slot = (cx, cy, dap) if k == 0 else (cx, cy)
                buf = fs0 if k == 0 else fs1
                buf[(0,) + slot] = d_ab[:, :LANES].astype(BF)
                buf[(1,) + slot] = d_ab[:, LANES:].astype(BF)
                so_b = d_so[...].astype(BF)
                buf[(2,) + slot] = jnp.concatenate([so_b[:, t * LANES:(t + 1) * LANES] for t in range(3)], axis=0)

    copies[11].wait()
    for ref in (dwpa, dwpb, dwpo, m8):
        ref[...] = jnp.zeros(ref.shape, F32)

    def hook(*calls):
        def run():
            for call in calls:
                call()
        return run

    hooks = {
        0: hook(lambda: red_a.step(1)),
        1: hook(lambda: gat_c.step(4)),
        2: hook(lambda: red_a.step(2), lambda: gat_c.step(5), lambda: gat_ds.step(5), tile_grads, lambda: tiles.step(1)),
        3: hook(lambda: red_a.step(3)),
        4: hook(lambda: red_a.step(4), lambda: tiles.step(2), lambda: gkv_copy().start()),
    }
    tail_hooks = {
        0: hook(lambda: red_a.step(5)),
        2: hook(lambda: red_p.step(1)),
        6: hook(finish_attention),
        7: hook(lambda: tiles.step(3)),
        9: hook(lambda: red_p.step(2), lambda: red_a.step(6)),
    }

    def run_hooks(table, k):
        for when, todo in table.items():
            pl.when(k == when)(todo)

    def backward_head(b, live, bufs):
        u_ref, ut_ref, gn_ref, gnt_ref = bufs
        at = rows_at(b)
        c, rows = bias_at(b)
        gl_f = bias_v[c, :, rows, :].reshape(8 * HEADS, num_tok)
        wide = tn(gl_f.astype(BF), w8[...])
        grad_norm = jnp.concatenate([wide[:, k * LANES:(k + 1) * LANES] for k in range(8)], axis=0)
        bias_norm, bias_inv = layer_norm(z1_v[at, :].astype(F32))
        m8[...] += nn((gl_f * live).astype(BF), side_by_side(bias_norm.astype(BF)))
        grad_new = dz_v[at, :].astype(F32) + norm_grad(bias_norm, bias_inv, grad_norm)
        gnew_v[at, :] = grad_new
        gnb = grad_new.astype(BF)
        gn_ref[...] = gnb
        gnt_ref[...] = gnb.T
        normed, _ = layer_norm(z_v[at, :].astype(F32))
        u = normed.astype(BF)
        u_ref[...] = u
        ut_ref[...] = u.T

    def backward_main(b, bufs):
        u_ref, ut_ref, gn_ref, gnt_ref = bufs
        at = rows_at(b)
        for f in range(0, 512, 256):
            cols = slice(f, f + 256)
            u, gnb = u_ref[...], gn_ref[...]
            hidden, grad_a, grad_b = swiglu_grad(nn(u, wpa[:, cols]), nn(u, wpb[:, cols]), nt(gnb, wpo[cols, :]))
            gab_v[at, cols] = grad_a
            gab_v[at, 512 + f:768 + f] = grad_b
            dwpo[:, cols] += nn(gnt_ref[...], hidden)
            dwpa[:, cols] += nn(ut_ref[...], grad_a)
            dwpb[:, cols] += nn(ut_ref[...], grad_b)

    def backward_tail(b, carry):
        at = rows_at(b)
        grad_normed = nt(gab_v[at, :], jnp.concatenate([wpa[...], wpb[...]], axis=1))
        normed, inv = layer_norm(z_v[at, :].astype(F32))
        dz_v[at, :] = (gnew_v[at, :] + norm_grad(normed, inv, grad_normed)).astype(BF)
        run_hooks(tail_hooks, b)
        return carry

    bufs0, bufs1 = (u0, ut0, gn0, gnt0), (u1, ut1, gn1, gnt1)

    def backward_pair(p, carry):
        backward_head(2 * p + 1, 1.0, bufs1)
        backward_main(2 * p, bufs0)
        more = jnp.where(p < num_blk // 2 - 1, 1.0, 0.0)
        backward_head(jnp.minimum(2 * p + 2, num_blk - 1), more, bufs0)
        backward_main(2 * p + 1, bufs1)
        run_hooks(hooks, p)
        return carry

    backward_head(0, 1.0, bufs0)
    gat_c.step(3)
    lax.fori_loop(0, num_blk // 2, backward_pair, 0)

    for t, ref in enumerate((dwpa, dwpb, dwpo)):
        for k in range(4):
            gp[t, k * 128:(k + 1) * 128, :] = ref[:, k * LANES:(k + 1) * LANES].astype(BF)
        gp[t, 528:544, :] = jnp.zeros((16, LANES), BF)
    diag = jnp.zeros((128, LANES), F32)
    for k in range(8):
        diag = diag + jnp.where(row8 == k, m8[:, k * LANES:(k + 1) * LANES], 0.0)
    gp[0, 512:528, :] = jnp.sum(diag.reshape(HEADS, 8, LANES), axis=1).astype(BF)
    for t in range(1, 3):
        gp[t, 512:528, :] = jnp.zeros((16, LANES), BF)
    red_p.start()
    lax.fori_loop(0, num_blk, backward_tail, 0)
    out_copies[5].start()
    tiles.step(4)
    for k in range(2):
        @pl.when(core == k)
        def _():
            out_copies[1 + k].start()
    red_p.step(3)
    red_a.step(7)
    red_p.step(4)
    tiles.step(5)
    for k in range(2):
        @pl.when(core == k)
        def _():
            out_copies[2 - k].start()
    red_a.step(8)
    out_copies[3].start()
    red_p.step(5)
    out_copies[4].start()
    for item in out_copies:
        item.wait()


def unpack_kernel(dz_i, ds_i, fs0_i, fs1_i, fa_i, fp_i,
                  dz_o, ds_o, pa_o, pb_o, po_o, bias_o, q_o, qb_o, kv_o, g_o, o_o, sa_o, sb_o, so_o,
                  dz, ds, fs0, fs1, fa, fp, pa, pb, po, bias, q, qb, kv, g, o, sa, sb, so, in_sem, sem):
    ins = [(fs0_i, fs0), (fs1_i, fs1), (fa_i, fa), (fp_i, fp), (dz_i, dz), (ds_i, ds)]
    reads = [pltpu.make_async_copy(src, dst, in_sem.at[k]) for k, (src, dst) in enumerate(ins)]
    for item in reads:
        item.start()
    outs = [(sa, sa_o), (sb, sb_o), (so, so_o), (q, q_o), (kv, kv_o), (g, g_o), (o, o_o), (qb, qb_o), (pa, pa_o), (pb, pb_o),
            (po, po_o), (bias, bias_o), (dz, dz_o), (ds, ds_o)]
    copies = [pltpu.make_async_copy(src, dst, sem.at[k]) for k, (src, dst) in enumerate(outs)]

    reads[0].wait()
    reads[1].wait()
    for kind in range(3):
        for pair in range(4):
            cx, cy = pair // 2, pair % 2
            for j in range(3):
                lo = (3 * pair + j) * LANES
                tile = fs1[kind, cx, cy] if j == 1 else fs0[kind, cx, cy, j // 2]
                wide = tile.astype(F32)
                if kind < 2:
                    (sa, sb)[kind][:, lo:lo + LANES] = wide
                else:
                    for k in range(3):
                        so[lo:lo + LANES, k * LANES:(k + 1) * LANES] = wide[k * LANES:(k + 1) * LANES]
        copies[kind].start()
    reads[2].wait()
    for index, (ref, buf, row) in enumerate(((q, fa, 0), (kv, fa, 384), (g, fa, 1152), (o, fa, 1536))):
        per = ref.shape[1] // 384
        for k in range(3 * per):
            lo = row + (k % per) * 384
            ref[:, k * LANES:(k + 1) * LANES] = buf[k // per, lo:lo + 384, :].astype(F32)
        copies[3 + index].start()
    for t in range(3):
        qb[t * LANES:(t + 1) * LANES] = fa[t, 1920:1936, :].astype(F32)[0]
    copies[7].start()
    reads[3].wait()
    for t, ref in enumerate((pa, pb)):
        for k in range(4):
            ref[:, k * LANES:(k + 1) * LANES] = fp[t, k * 128:(k + 1) * 128, :].astype(F32)
        copies[8 + t].start()
    for k in range(4):
        po[k * 128:(k + 1) * 128, :] = fp[2, k * 128:(k + 1) * 128, :].astype(F32).T
    copies[10].start()
    bias[...] = fp[0, 512:528, :].astype(F32)
    copies[11].start()
    for k in range(2):
        reads[4 + k].wait()
        copies[12 + k].start()
    for item in copies:
        item.wait()


def solution(mesh):
    pair_spec = P('dp', 'dap', None, None)
    single_spec = P('dp', 'dap', None)
    hbm = pl.BlockSpec(memory_space=pl.ANY)
    vmem = pl.BlockSpec(memory_space=pltpu.VMEM)

    def body(pair_z, single_s, token_mask, dz_out, ds_out, w_pa, w_pb, w_po, w_bias, w_q, q_bias, w_kv, w_g, w_o, w_sa, w_sb, w_so):
        num_cplx, half, num_tok, dim = pair_z.shape
        toks = num_cplx * half * num_tok
        rows = num_cplx * half
        width = w_q.shape[1]
        big = (pair_z.reshape(toks, dim), dz_out.reshape(toks, dim), w_pa, w_pb, w_po, w_q, w_kv, w_g, w_o, w_sa, w_sb, w_so)
        small = (single_s.reshape(rows, width), ds_out.reshape(rows, width), token_mask, q_bias, w_bias.T)
        scratch = [pltpu.VMEM(a.shape, a.dtype) for a in big]
        finals = [(toks, dim), (rows, width), (3, 2, 2, 2, width, LANES), (3, 2, 2, width, LANES), (3, ROWS_A, LANES), (3, ROWS_P, LANES)]
        scratch += [
            pltpu.VMEM((toks, dim), BF), pltpu.VMEM((128, 1024), BF),
            pltpu.VMEM((num_cplx, HEADS, half, num_tok), F32), pltpu.VMEM((num_cplx, HEADS * half, num_tok), F32),
            pltpu.VMEM((rows, width), BF), pltpu.VMEM((rows, width), BF), pltpu.VMEM((rows, width), F32),
            pltpu.VMEM((rows, width), F32), pltpu.VMEM((rows, width), BF), pltpu.VMEM((rows, width), BF),
            pltpu.VMEM((rows, width), F32), pltpu.VMEM((rows, width), F32),
            pltpu.VMEM((2, rows, 3 * width), BF), pltpu.VMEM((2, rows, 2 * width), BF), pltpu.VMEM((rows, 2 * width), BF),
            pltpu.VMEM((128, 512), F32), pltpu.VMEM((128, 512), F32), pltpu.VMEM((128, 512), F32), pltpu.VMEM((128, 1024), F32),
            pltpu.VMEM(finals[1], BF),
            pltpu.VMEM((3, 2, 2, 2, 2, rows, LANES), BF), pltpu.VMEM((3, 2, 2, 2, 2, rows, LANES), BF),
            pltpu.VMEM((width, 2 * LANES), F32), pltpu.VMEM((LANES, width), F32),
            pltpu.VMEM((toks, dim), F32), pltpu.VMEM((toks, 1024), BF),
        ]
        for _ in range(2):
            scratch += [pltpu.VMEM((512, dim), BF)] * 2 + [pltpu.VMEM((dim, 512), BF)] * 2
        scratch += [pltpu.VMEM(shape, BF) for shape in finals[2:]]
        scratch += [pltpu.VMEM((3, ROWS_A >> k, LANES), BF) for k in range(5)]
        scratch += [pltpu.VMEM((3, ROWS_P, LANES), BF)] + [pltpu.VMEM((3, ROWS_P // 2, LANES), BF) for _ in range(4)]
        scratch += [pltpu.SemaphoreType.DMA((12,)), pltpu.SemaphoreType.DMA((6,)),
                    pltpu.SemaphoreType.DMA((4,)), pltpu.SemaphoreType.DMA((5, 3))]
        scratch += [pltpu.SemaphoreType.DMA((stages, 3)) for stages in (8, 5, 4, 4, 4)]
        packed = pl.pallas_call(
            body_kernel,
            out_shape=[jax.ShapeDtypeStruct(shape, BF) for shape in finals],
            in_specs=[hbm] * 12 + [vmem] * 5,
            out_specs=[hbm] * 6,
            scratch_shapes=scratch,
            compiler_params=pltpu.CompilerParams(collective_id=0, has_side_effects=True, vmem_limit_bytes=60 * 2 ** 20),
            name="block",
        )(*big, *small)
        shapes = [w_pa.shape, w_pb.shape, w_po.shape, (HEADS, dim), w_q.shape, (width,), w_kv.shape, w_g.shape, w_o.shape,
                  w_sa.shape, w_sb.shape, w_so.shape]
        done = pl.pallas_call(
            unpack_kernel,
            out_shape=[jax.ShapeDtypeStruct(shape, BF) for shape in finals[:2]] + [jax.ShapeDtypeStruct(shape, F32) for shape in shapes],
            in_specs=[hbm] * 6,
            out_specs=[hbm] * 14,
            scratch_shapes=[pltpu.VMEM(shape, BF) for shape in finals] + [pltpu.VMEM(shape, F32) for shape in shapes] + [
                pltpu.SemaphoreType.DMA((6,)), pltpu.SemaphoreType.DMA((14,))],
            compiler_params=pltpu.CompilerParams(vmem_limit_bytes=56 * 2 ** 20),
            name="unpack",
        )(*packed)
        grads = list(done[2:])
        grads[3] = grads[3].T
        return (done[0].reshape(pair_z.shape), done[1].reshape(single_s.shape)) + tuple(grads)

    in_specs = (pair_spec, single_spec, P('dp', None), pair_spec, single_spec) + (P(),) * 12
    out_specs = (pair_spec, single_spec) + (P(),) * 12
    return jax.shard_map(body, mesh=mesh, in_specs=in_specs, out_specs=out_specs, check_vma=False)
```
